256 devices in a mesh: parts: 256 (over x, y, z, core).
Axes of the slice: x: 4, y: 4, z: 8, core: 2. Of those that a mesh axis runs over, the one named last changes fastest.
Arguments:
- features: bfloat16 [524288, 256], P('parts'), may hold values from -32 to 32, as said below
- tile_values: bfloat16 [65536, 128, 128], P('parts'), may hold values from -0.0078125 to 0.009338379
- tile_blocks: int32 [65536, 2], P('parts'), may hold values from 0 to 23, as said below
- tile_count: int32 [256], P('parts'), may hold values from 24 to 256, as said below
- send_rows: int32 [256, 4, 256], P('parts'), may hold values from 0 to 2047, as said below
- recv_index: int32 [256, 1024], P('parts'), may hold values from 0 to 1023, as said below
- layer_weight: bfloat16 [2, 256, 256], replicated, may hold values from -0.375 to 0.375
- norm_gain: float32 [2, 256], replicated, may hold values from 0.1 to 1.9
- norm_shift: float32 [2, 256], replicated, may hold values from -3 to 3
Outputs:
- embedded: bfloat16 [524288, 256], P('parts')
The draws below stay inside these ranges and needn't reach their ends.
Inputs may be any that keep to these rules, and one draw needn't show every extreme that they name: `features`: every entry is finite. `tile_blocks`: column 0 is a row block (0 to 15), column 1 a column block of columns_l. A device's first 16 tiles are the diagonal blocks (t, t) in order; the next 8 tiles have the column blocks 2048 // 128, 17, ... in order; blocks may repeat. `tile_count`: the live tiles are the leading ones of a device's list; some device has all 256 live in every draw. `send_rows`: entry [q, n] lists 256 distinct local rows that device q sends to device q + o[n], o = (1, -1, 2, -2). `recv_index`: each device's row is a permutation.
All inputs are finite; a program needn't handle non-finite values.
Results may differ from the reference program's by a relative error of at most 0.0072.
Values may be sent and summed in bfloat16 or wider, within the bound.
No kernel may reach another device: no remote copies, remote signals or barrier semaphores. Data moves between devices by JAX's collectives and lax.ppermute only.
A program may use at most 64 MiB of HBM per device.

```python
import jax
import jax.numpy as jnp
from jax import lax

C = 256
B = 128
LAYERS = 2
NEIGHBOURS = 4
V_DEV = 2048
HALO_DEV = 256
NT_DEV = 256
V_TOT = 524288
TILES = 65536
N_PARTS = 256


def draw_features(key, part):
    key_noise, key_spread, key_mean = jax.random.split(key, 3)
    row_total = V_TOT
    position = jnp.arange(row_total, dtype=jnp.float32) / (row_total - 1)
    fluctuation = jnp.clip(jax.random.normal(key_noise, (row_total, C), jnp.float32), -5.0, 5.0)
    drift = jnp.exp(jnp.log(3.0) * (position - 0.5))
    centre = jax.random.uniform(key_mean, (C,), jnp.float32, -0.3, 0.3)
    spread = jnp.exp(jax.random.uniform(key_spread, (row_total,), jnp.float32, -1.15, 1.15))
    return ((fluctuation + centre[None, :]) * (drift * spread)[:, None]).astype(jnp.bfloat16)


def draw_tile_blocks(key, part):
    key_rows, key_cols = jax.random.split(jax.random.fold_in(key, 11), 2)
    row_count = V_DEV // B
    halo_count = NEIGHBOURS * HALO_DEV // B
    number = jnp.arange(TILES, dtype=jnp.int32) % NT_DEV
    random_rows = jax.random.randint(key_rows, (TILES,), 0, row_count, dtype=jnp.int32)
    random_cols = jax.random.randint(key_cols, (TILES,), 0, row_count + halo_count, dtype=jnp.int32)
    diagonal = number < row_count
    halo_part = (number >= row_count) & (number < row_count + halo_count)
    rows_out = jnp.where(diagonal, number, random_rows)
    cols_out = jnp.where(diagonal, number, jnp.where(halo_part, number, random_cols))
    return jnp.stack([rows_out, cols_out], axis=1).astype(jnp.int32)


def draw_tile_count(key, part):
    key_load, key_heavy = jax.random.split(jax.random.fold_in(key, 23), 2)
    device_total = TILES // NT_DEV
    fixed_part = V_DEV // B + NEIGHBOURS * HALO_DEV // B
    remainder = NT_DEV - fixed_part
    drawn = jax.random.randint(key_load, (device_total,), 0, remainder + 1, dtype=jnp.int32)
    skewed = drawn * drawn // remainder
    heaviest = jax.random.randint(key_heavy, (), 0, device_total, dtype=jnp.int32)
    skewed = jnp.where(jnp.arange(device_total, dtype=jnp.int32) == heaviest, remainder, skewed)
    return (fixed_part + skewed).astype(jnp.int32)


def draw_send_rows(key, part):
    device_total = V_TOT // V_DEV
    key_list = jax.random.split(jax.random.fold_in(key, 37), device_total * NEIGHBOURS)
    chosen = jax.vmap(lambda single: jax.random.permutation(single, V_DEV)[:HALO_DEV])(key_list)
    return chosen.reshape(device_total, NEIGHBOURS, HALO_DEV).astype(jnp.int32)


def draw_recv_index(key, part):
    device_total = V_TOT // V_DEV
    key_list = jax.random.split(jax.random.fold_in(key, 41), device_total)
    chosen = jax.vmap(lambda single: jax.random.permutation(single, NEIGHBOURS * HALO_DEV))(key_list)
    return chosen.astype(jnp.int32)


def shard_levels(stream_key, extent, cuts, smallest, high):
    def one(dim, blocks):
        steps = jax.random.uniform(jax.random.fold_in(jax.random.fold_in(stream_key, 6), dim), (blocks,), jnp.float32, smallest / len(cuts), high / len(cuts))
        return jnp.repeat(jnp.exp(steps), extent[dim] // blocks).reshape((-1,) + (1,) * (len(extent) - dim - 1))

    gain = one(*cuts[0])
    for cut in cuts[1:]:
        gain = gain * one(*cut)
    return gain


def centred(stream_key, dims, scale, reach, kind=jnp.bfloat16):
    result = jax.random.normal(stream_key, dims, jnp.float32) * scale
    return jnp.minimum(jnp.maximum(result, -reach), reach).astype(kind)


def setup_inputs(seed: int = 0) -> dict:
    streams_of = jax.random.split(jax.random.key(seed), 10)
    return {
        "features": draw_features(jax.random.fold_in(streams_of[9], 71), 0),
        "tile_values": jnp.clip(-0.0078125 + 0.017150879 * jax.random.uniform(streams_of[1], (TILES, B, B), jnp.float32) ** shard_levels(streams_of[1], (TILES, B, B), ((0, 256),), -0.2, 0.2), -0.0078125, 0.009338379).astype(jnp.bfloat16),
        "tile_blocks": draw_tile_blocks(jax.random.fold_in(streams_of[9], 71), 0),
        "tile_count": draw_tile_count(jax.random.fold_in(streams_of[9], 71), 0),
        "send_rows": draw_send_rows(jax.random.fold_in(streams_of[9], 71), 0),
        "recv_index": draw_recv_index(jax.random.fold_in(streams_of[9], 71), 0),
        "layer_weight": centred(streams_of[6], (LAYERS, C, C), C ** -0.5, 0.375),
        "norm_gain": jnp.clip(1.0 + 0.18 * jax.random.normal(streams_of[7], (LAYERS, C), jnp.float32), 0.1, 1.9),
        "norm_shift": centred(streams_of[8], (LAYERS, C), 0.5, 3.0, jnp.float32),
    }


neighbour_offsets = (1, -1, 2, -2)
norm_eps = 1e-05

def halo_rows(stacked, send_rows, recv_index, device):
    device_total = stacked.shape[0]
    pieces = []
    for position, offset in enumerate(neighbour_offsets):
        source = device - offset
        inside = (source >= 0) & (source < device_total)
        clipped = jnp.clip(source, 0, device_total - 1).astype(jnp.int32)
        source_rows = stacked[clipped]
        picked = jnp.take(source_rows, send_rows[clipped, position], axis=0)
        pieces.append(jnp.where(inside, picked, jnp.zeros_like(picked)))
    received = jnp.concatenate(pieces, axis=0)
    return jnp.take(received, recv_index[device], axis=0)

def aggregate(columns, values, blocks, live_count):
    tile_edge = values.shape[1]
    channels = columns.shape[1]
    column_blocks = columns.reshape(-1, tile_edge, channels)
    picked = jnp.take(column_blocks, blocks[:, 1], axis=0).astype(jnp.float32)
    partial_value = jnp.einsum('tij,tjc->tic', values.astype(jnp.float32), picked, precision=lax.Precision.HIGHEST)
    row_count = V_DEV // B
    owners = (blocks[:, 0][None, :] == jnp.arange(row_count, dtype=jnp.int32)[:, None]) & (jnp.arange(values.shape[0], dtype=jnp.int32) < live_count)[None, :]
    summed = jnp.einsum('rt,tic->ric', owners.astype(jnp.float32), partial_value, precision=lax.Precision.HIGHEST)
    return summed.reshape(row_count * tile_edge, channels)

def reference(features, tile_values, tile_blocks, tile_count, send_rows, recv_index, layer_weight, norm_gain, norm_shift):
    stacked = features.reshape(N_PARTS, V_DEV, C)
    values_all = tile_values.reshape(N_PARTS, NT_DEV, B, B)
    blocks_all = tile_blocks.reshape(N_PARTS, NT_DEV, 2)
    for layer_index in range(LAYERS):
        weight = layer_weight[layer_index]

        def one_device(device, stacked=stacked, weight=weight):
            halo_block = halo_rows(stacked, send_rows, recv_index, device)
            columns = jnp.concatenate([stacked[device], halo_block], axis=0)
            summed = aggregate(columns, values_all[device], blocks_all[device], tile_count[device])
            gathered = summed.astype(jnp.bfloat16)
            return jnp.dot(gathered, weight, preferred_element_type=jnp.float32).astype(jnp.bfloat16)
        mixed_rows = lax.map(one_device, jnp.arange(N_PARTS, dtype=jnp.int32))
        widened = mixed_rows.astype(jnp.float32)
        centre = lax.optimization_barrier(jnp.mean(widened, axis=(0, 1)))
        spread = lax.optimization_barrier(jnp.mean(jnp.square(widened - centre), axis=(0, 1)))
        scaled = (widened - centre) / jnp.sqrt(spread + norm_eps)
        stacked = jax.nn.relu(norm_gain[layer_index] * scaled + norm_shift[layer_index]).astype(jnp.bfloat16)
    return stacked.reshape(V_TOT, C)
```

```python
import functools

import jax
import jax.numpy as jnp
from jax import lax
from jax.experimental import pallas as pl
from jax.experimental.pallas import tpu as pltpu
from jax.sharding import Mesh
from jax.sharding import PartitionSpec as P

PARTS = ("parts_0", "parts_1", "parts_2", "parts_3")
PLANE = PARTS[:2]
COLUMN = PARTS[2:]
norm_eps = 1e-05
EDGE = 128
MIB = 1 << 20


def swap(value, first, stride, total):
    pairs = []
    for q in range(total - stride):
        if first(q):
            pairs += [(q, q + stride), (q + stride, q)]
    return lax.ppermute(value, PARTS, pairs)


def exchange(pieces):
    total = lax.axis_size(PARTS)
    a, b, c, d = pieces
    got_c = swap(c, lambda q: q % 4 < 2, 2, total)
    got_d = swap(d, lambda q: q % 4 >= 2, 2, total)
    got_b = swap(b, lambda q: q % 2 == 1, 1, total)
    got_a = swap(a, lambda q: q % 2 == 0, 1, total)
    return got_a, got_b, got_c, got_d


def fill_one_hot(index_ref, one_hot_ref):
    groups, columns = index_ref.shape[0], one_hot_ref.shape[1]
    lanes = lax.broadcasted_iota(jnp.int32, (EDGE, EDGE), 1)
    for group in range(groups):
        row = jnp.broadcast_to(index_ref[pl.ds(group, 1), :], (EDGE, EDGE))
        away = row.T - lanes
        for block in range(columns // EDGE):
            one_hot_ref[pl.ds(group * EDGE, EDGE), pl.ds(block * EDGE, EDGE)] = jnp.where(
                away == block * EDGE, 1.0, 0.0
            ).astype(jnp.bfloat16)


def pick_pieces(one_hot_ref, rows_ref, piece_refs):
    count = piece_refs[0].shape[0]
    for n, piece in enumerate(piece_refs):
        piece[...] = jnp.dot(
            one_hot_ref[pl.ds(n * count, count), :],
            rows_ref[...],
            preferred_element_type=jnp.float32,
        ).astype(jnp.bfloat16)


def gather_kernel(send_ref, rows_ref, a, b, c, d, one_hot_ref):
    fill_one_hot(send_ref, one_hot_ref)
    pick_pieces(one_hot_ref, rows_ref, (a, b, c, d))


def adjacency_block(dense_ref, first, last, start, size):
    return jnp.concatenate(
        [dense_ref[c, pl.ds(start, size), :] for c in range(first, last)], axis=1
    )


def build_kernel(order_ref, row_ref, column_ref, keep_ref, live_ref, tiles_ref, rows_ref,
                 dense_ref, own_ref):
    blocks, height = dense_ref.shape[0], dense_ref.shape[1]
    unroll = 8
    zeros = jnp.zeros((height // 8, EDGE), jnp.bfloat16)

    @pl.loop(0, blocks)
    def _(c):
        for part in range(8):
            dense_ref[c, pl.ds(part * (height // 8), height // 8), :] = zeros

    def step(turn, total):
        for u in range(unroll):
            k = turn * unroll + u
            tile = tiles_ref[order_ref[k]].astype(jnp.float32)
            total = total * keep_ref[k].astype(jnp.float32) + tile
            start = pl.multiple_of(row_ref[k] * EDGE, EDGE)
            dense_ref[column_ref[k], pl.ds(start, EDGE), :] = total.astype(jnp.bfloat16)
        return total

    lax.fori_loop(
        0, (live_ref[0] + unroll - 1) // unroll, step, jnp.zeros((EDGE, EDGE), jnp.float32)
    )
    own_blocks = height // EDGE
    size = 512

    @pl.loop(0, height // size)
    def _(m):
        start = pl.multiple_of(m * size, size)
        own_ref[pl.ds(start, size), :] = jnp.dot(
            adjacency_block(dense_ref, 0, own_blocks, start, size),
            rows_ref[...],
            preferred_element_type=jnp.float32,
        )


def add_moments(z, moment_ref):
    wide = z.astype(jnp.float32)
    moment_ref[0:8, :] += jnp.sum(wide.reshape(-1, 8, wide.shape[1]), axis=0)
    moment_ref[8:16, :] += jnp.sum(jnp.square(wide).reshape(-1, 8, wide.shape[1]), axis=0)


def put_moments(moment_ref, out_ref):
    both = jnp.concatenate(
        [
            jnp.sum(moment_ref[0:8, :], axis=0, keepdims=True),
            jnp.sum(moment_ref[8:16, :], axis=0, keepdims=True),
        ],
        axis=0,
    )
    for n in range(out_ref.shape[0]):
        out_ref[n] = both


def first_kernel(recv_ref, a, b, c, d, dense_ref, own_ref, weight_ref, send_hot_ref,
                 z_ref, stats_ref, oa, ob, oc, od, recv_hot_ref, halo_ref, got_ref, moment_ref):
    count = a.shape[0]
    for n, piece in enumerate((a, b, c, d)):
        got_ref[pl.ds(n * count, count), :] = piece[...]
    fill_one_hot(recv_ref, recv_hot_ref)
    halo_ref[...] = jnp.dot(
        recv_hot_ref[...], got_ref[...], preferred_element_type=jnp.float32
    ).astype(jnp.bfloat16)
    moment_ref[...] = jnp.zeros_like(moment_ref)
    height = z_ref.shape[0]
    own_blocks, halo_blocks = height // EDGE, halo_ref.shape[0] // EDGE
    size = 512

    @pl.loop(0, height // size)
    def _(m):
        start = pl.multiple_of(m * size, size)
        agg = own_ref[pl.ds(start, size), :] + jnp.dot(
            adjacency_block(dense_ref, own_blocks, own_blocks + halo_blocks, start, size),
            halo_ref[...],
            preferred_element_type=jnp.float32,
        )
        z = jnp.dot(
            agg.astype(jnp.bfloat16), weight_ref[...], preferred_element_type=jnp.float32
        ).astype(jnp.bfloat16)
        z_ref[pl.ds(start, size), :] = z
        add_moments(z, moment_ref)

    put_moments(moment_ref, stats_ref)
    pick_pieces(send_hot_ref, z_ref, (oa, ob, oc, od))


def scale_of(stats_ref, gain_ref, shift_ref, vertex_total):
    both = jnp.sum(stats_ref[...], axis=0) / vertex_total
    centre = both[0:1, :]
    spread = both[1:2, :] - jnp.square(centre)
    factor = gain_ref[...] / jnp.sqrt(spread + norm_eps)
    return centre, factor, shift_ref[...]


def normal(rows, terms):
    centre, factor, shift = terms
    return jnp.maximum((rows.astype(jnp.float32) - centre) * factor + shift, 0.0)


def second_kernel(vertex_total, present_ref, recv_ref, a, b, c, d, mixed_ref, stats_in_ref,
                  gain_ref, shift_ref, dense_ref, weight_ref, z_ref, stats_ref,
                  recv_hot_ref, got_ref, columns_ref, moment_ref):
    count = a.shape[0]
    height = z_ref.shape[0]
    halo = 4 * count
    terms = scale_of(stats_in_ref, gain_ref, shift_ref, vertex_total)
    for n, piece in enumerate((a, b, c, d)):
        got_ref[pl.ds(n * count, count), :] = (
            normal(piece[...], terms) * present_ref[n].astype(jnp.float32)
        ).astype(jnp.bfloat16)
    fill_one_hot(recv_ref, recv_hot_ref)
    columns_ref[pl.ds(height, halo), :] = jnp.dot(
        recv_hot_ref[...], got_ref[...], preferred_element_type=jnp.float32
    ).astype(jnp.bfloat16)
    for part in range(8):
        rows = pl.ds(part * (height // 8), height // 8)
        columns_ref[rows, :] = normal(mixed_ref[rows, :], terms).astype(jnp.bfloat16)
    moment_ref[...] = jnp.zeros_like(moment_ref)
    size = 512

    @pl.loop(0, height // size)
    def _(m):
        start = pl.multiple_of(m * size, size)
        agg = jnp.dot(
            adjacency_block(dense_ref, 0, (height + halo) // EDGE, start, size),
            columns_ref[...],
            preferred_element_type=jnp.float32,
        )
        z = jnp.dot(
            agg.astype(jnp.bfloat16), weight_ref[...], preferred_element_type=jnp.float32
        ).astype(jnp.bfloat16)
        z_ref[pl.ds(start, size), :] = z
        add_moments(z, moment_ref)

    put_moments(moment_ref, stats_ref)


def last_kernel(vertex_total, mixed_ref, stats_in_ref, gain_ref, shift_ref, out_ref):
    terms = scale_of(stats_in_ref, gain_ref, shift_ref, vertex_total)
    out_ref[...] = normal(mixed_ref[...], terms).astype(jnp.bfloat16)


def all_sums(stats):
    stats = lax.all_to_all(stats, COLUMN, 0, 0, tiled=True)
    peers = lax.axis_size(PLANE)
    stats = jnp.broadcast_to(jnp.sum(stats, axis=0)[None], (peers,) + stats.shape[1:])
    return lax.all_to_all(stats, PLANE, 0, 0, tiled=True)


def tile_order(tile_blocks, live_count, row_count, column_count):
    tiles = tile_blocks.shape[0]
    number = jnp.arange(tiles, dtype=jnp.int32)
    live = number < live_count
    row = jnp.where(live, tile_blocks[:, 0], 0)
    column = jnp.where(live, tile_blocks[:, 1], column_count)
    key = (column * row_count + row) * tiles + number
    rank = jnp.sum((key[None, :] < key[:, None]).astype(jnp.int32), axis=1)
    hit = rank[None, :] == number[:, None]

    def sorted_by_rank(values):
        return jnp.sum(jnp.where(hit, values[None, :], 0), axis=1)

    order = sorted_by_rank(number)
    row, column = sorted_by_rank(row), sorted_by_rank(column)
    cell = column * row_count + row
    before = jnp.concatenate([jnp.full((1,), -1, jnp.int32), cell[:-1]])
    return order, row, column, (cell == before).astype(jnp.int32)


VMEM = pl.BlockSpec(memory_space=pltpu.VMEM)
SMEM = pl.BlockSpec(memory_space=pltpu.SMEM)


def shards(features, tile_values, tile_blocks, tile_count, send_rows, recv_index,
           layer_weight, norm_gain, norm_shift):
    height, channels = features.shape
    neighbours, count = send_rows.shape[1:]
    halo = neighbours * count
    row_count = height // EDGE
    column_count = (height + halo) // EDGE
    device = lax.axis_index(PARTS)
    total = lax.axis_size(PARTS)
    vertex_total = height * total
    peers = lax.axis_size(COLUMN)
    bf16, f32 = jnp.bfloat16, jnp.float32
    struct = jax.ShapeDtypeStruct
    piece = struct((count, channels), bf16)
    stats_type = struct((peers, 2, channels), f32)
    mixed = struct((height, channels), bf16)

    near_swapped = device % 2 == 0
    far_swapped = device % 4 < 2
    n0, n1, n2, n3 = (send_rows[0, n] for n in range(4))
    send = jnp.stack([
        jnp.where(near_swapped, n0, n1),
        jnp.where(near_swapped, n1, n0),
        jnp.where(far_swapped, n2, n3),
        jnp.where(far_swapped, n3, n2),
    ]).reshape(halo // EDGE, EDGE)
    flip = jnp.where(recv_index[0] < 2 * count, near_swapped, far_swapped)
    recv = (recv_index[0] ^ jnp.where(flip, count, 0)).reshape(halo // EDGE, EDGE)
    present = jnp.stack([
        jnp.ones((), bool),
        (device > 0) & (device < total - 1),
        jnp.ones((), bool),
        (device > 1) & (device < total - 2),
    ]).astype(jnp.int32)

    *pieces, send_hot = pl.pallas_call(
        gather_kernel,
        out_shape=[piece] * 4 + [struct((halo, height), bf16)],
        in_specs=[VMEM, VMEM],
        out_specs=[VMEM] * 5,
        compiler_params=pltpu.CompilerParams(vmem_limit_bytes=24 * MIB),
        cost_estimate=pl.CostEstimate(
            flops=2 * halo * height * channels, bytes_accessed=2 * MIB, transcendentals=0),
    )(send, features)
    got = exchange(pieces)

    live_count = tile_count[0]
    order, row, column, keep = tile_order(tile_blocks, live_count, row_count, column_count)
    dense, own = pl.pallas_call(
        build_kernel,
        out_shape=[struct((column_count + 1, height, EDGE), bf16), struct((height, channels), f32)],
        in_specs=[SMEM] * 5 + [VMEM, VMEM],
        out_specs=[VMEM, VMEM],
        compiler_params=pltpu.CompilerParams(vmem_limit_bytes=40 * MIB),
        cost_estimate=pl.CostEstimate(
            flops=4 * height * height * channels, bytes_accessed=24 * MIB, transcendentals=0),
    )(order, row, column, keep, tile_count, tile_values, features)

    z, stats, *pieces = pl.pallas_call(
        first_kernel,
        out_shape=[mixed, stats_type] + [piece] * 4,
        in_specs=[VMEM] * 9,
        out_specs=[VMEM] * 6,
        scratch_shapes=[
            pltpu.VMEM((halo, halo), bf16),
            pltpu.VMEM((halo, channels), bf16),
            pltpu.VMEM((halo, channels), bf16),
            pltpu.VMEM((16, channels), f32),
        ],
        compiler_params=pltpu.CompilerParams(vmem_limit_bytes=40 * MIB),
        cost_estimate=pl.CostEstimate(
            flops=2 * height * halo * channels, bytes_accessed=16 * MIB, transcendentals=0),
    )(recv, *got, dense, own, layer_weight[0], send_hot)
    got = exchange(pieces)
    stats = all_sums(stats)

    z, stats = pl.pallas_call(
        functools.partial(second_kernel, vertex_total),
        out_shape=[mixed, stats_type],
        in_specs=[SMEM] + [VMEM] * 11,
        out_specs=[VMEM] * 2,
        scratch_shapes=[
            pltpu.VMEM((halo, halo), bf16),
            pltpu.VMEM((halo, channels), bf16),
            pltpu.VMEM((height + halo, channels), bf16),
            pltpu.VMEM((16, channels), f32),
        ],
        compiler_params=pltpu.CompilerParams(vmem_limit_bytes=40 * MIB),
        cost_estimate=pl.CostEstimate(
            flops=2 * height * (height + halo) * channels, bytes_accessed=16 * MIB,
            transcendentals=0),
    )(present, recv, *got, z, stats, norm_gain[0:1], norm_shift[0:1], dense, layer_weight[1])
    stats = all_sums(stats)

    return pl.pallas_call(
        functools.partial(last_kernel, vertex_total),
        out_shape=mixed,
        in_specs=[VMEM] * 4,
        out_specs=VMEM,
        compiler_params=pltpu.CompilerParams(vmem_limit_bytes=16 * MIB),
    )(z, stats, norm_gain[1:2], norm_shift[1:2])


def solution(mesh):
    finer = Mesh(mesh.devices.reshape(4, 4, 8, 2), PARTS)
    placed = (
        P(PARTS, None),
        P(PARTS, None, None),
        P(PARTS, None),
        P(PARTS),
        P(PARTS, None, None),
        P(PARTS, None),
        P(),
        P(),
        P(),
    )
    return jax.shard_map(
        shards, mesh=finer, in_specs=placed, out_specs=P(PARTS, None), check_vma=False
    )
```

```python
import functools

import jax
import jax.numpy as jnp
from jax import lax
from jax.experimental import pallas as pl
from jax.experimental.pallas import tpu as pltpu
from jax.sharding import Mesh
from jax.sharding import PartitionSpec as P

PARTS = ("parts_0", "parts_1", "parts_2", "parts_3")
PLANE = PARTS[:2]
COLUMN = PARTS[2:]
norm_eps = 1e-05
EDGE = 128
MIB = 1 << 20


def swap(value, first, stride, total):
    pairs = []
    for q in range(total - stride):
        if first(q):
            pairs += [(q, q + stride), (q + stride, q)]
    return lax.ppermute(value, PARTS, pairs)


def exchange(pieces):
    total = lax.axis_size(PARTS)
    a, b, c, d = pieces
    got_c = swap(c, lambda q: q % 4 < 2, 2, total)
    got_d = swap(d, lambda q: q % 4 >= 2, 2, total)
    got_b = swap(b, lambda q: q % 2 == 1, 1, total)
    got_a = swap(a, lambda q: q % 2 == 0, 1, total)
    return got_a, got_b, got_c, got_d


def fill_one_hot(index_ref, one_hot_ref):
    groups, columns = index_ref.shape[0], one_hot_ref.shape[1]
    lanes = lax.broadcasted_iota(jnp.int32, (EDGE, EDGE), 1)
    for group in range(groups):
        row = jnp.broadcast_to(index_ref[pl.ds(group, 1), :], (EDGE, EDGE))
        away = row.T - lanes
        for block in range(columns // EDGE):
            one_hot_ref[pl.ds(group * EDGE, EDGE), pl.ds(block * EDGE, EDGE)] = jnp.where(
                away == block * EDGE, 1.0, 0.0
            ).astype(jnp.bfloat16)


def pick_pieces(one_hot_ref, rows_ref, piece_refs):
    count = piece_refs[0].shape[0]
    for n, piece in enumerate(piece_refs):
        piece[...] = jnp.dot(
            one_hot_ref[pl.ds(n * count, count), :],
            rows_ref[...],
            preferred_element_type=jnp.float32,
        ).astype(jnp.bfloat16)


def spread(row):
    n = row.shape[1]
    return jnp.broadcast_to(row, (n, n)).T


def put_tile_order(blocks_ref, live_count, row_count, column_count, order_ref):
    tiles = blocks_ref.shape[1]
    number = lax.broadcasted_iota(jnp.int32, (1, tiles), 1)
    live = number < live_count
    row = jnp.where(live, blocks_ref[0:1, :], 0)
    column = jnp.where(live, blocks_ref[1:2, :], column_count)
    cell = column * row_count + row
    key = cell * tiles + number
    down = lax.broadcasted_iota(jnp.int32, (tiles, tiles), 0)
    cells_down = spread(cell)
    keys_down = cells_down * tiles + down
    rank = jnp.sum((keys_down < key).astype(jnp.int32), axis=0, keepdims=True)
    same = (cells_down == cell) & (down < number)
    keep = jnp.sum(same.astype(jnp.int32), axis=0, keepdims=True) > 0
    packed = (cell * 2 + keep.astype(jnp.int32)) * tiles + number
    hit = spread(rank) == number
    packed = jnp.sum(jnp.where(hit, spread(packed), 0), axis=0, keepdims=True)
    cell = packed // (2 * tiles)
    order_ref[0:1, :] = packed % tiles
    order_ref[1:2, :] = cell % row_count
    order_ref[2:3, :] = cell // row_count
    order_ref[3:4, :] = (packed // tiles) % 2


def gather_kernel(row_count, column_count, device_ref, live_ref, send_in, blocks_in, features_ref,
                  a, b, c, d, one_hot_ref, order_ref, rows_ref,
                  send_ref, blocks_ref, index_ref, arrived):
    load_send = pltpu.make_async_copy(send_in, send_ref, arrived.at[0])
    load_blocks = pltpu.make_async_copy(blocks_in, blocks_ref, arrived.at[1])
    load = pltpu.make_async_copy(features_ref, rows_ref, arrived.at[2])
    load_send.start()
    load_blocks.start()
    load.start()
    load_send.wait()
    near = device_ref[0] % 2 == 0
    far = device_ref[0] % 4 < 2
    count = send_ref.shape[1]
    for part in range(count // EDGE):
        n0, n1, n2, n3 = (send_ref[n:n + 1, part * EDGE:(part + 1) * EDGE] for n in range(4))
        lists = (
            jnp.where(near, n0, n1),
            jnp.where(near, n1, n0),
            jnp.where(far, n2, n3),
            jnp.where(far, n3, n2),
        )
        for n, chosen in enumerate(lists):
            at = n * (count // EDGE) + part
            index_ref[at:at + 1, :] = chosen
    fill_one_hot(index_ref, one_hot_ref)
    load_blocks.wait()
    put_tile_order(blocks_ref, live_ref[0], row_count, column_count, order_ref)
    load.wait()
    pick_pieces(one_hot_ref, rows_ref, (a, b, c, d))


def adjacency_block(dense_ref, first, last, start, size):
    return jnp.concatenate(
        [dense_ref[c, pl.ds(start, size), :] for c in range(first, last)], axis=1
    )


def build_kernel(count, device_ref, order_ref, live_ref, recv_in, tiles_ref, rows_ref,
                 dense_ref, own_ref, recv_hot_ref, held_ref, recv_ref, index_ref, arrived):
    load_recv = pltpu.make_async_copy(recv_in, recv_ref, arrived.at[0])
    load = pltpu.make_async_copy(tiles_ref, held_ref, arrived.at[1])
    load_recv.start()
    load.start()
    blocks, height = dense_ref.shape[0], dense_ref.shape[1]
    unroll = 8
    zeros = jnp.zeros((height // 8, EDGE), jnp.bfloat16)

    @pl.loop(0, blocks)
    def _(c):
        for part in range(8):
            dense_ref[c, pl.ds(part * (height // 8), height // 8), :] = zeros

    near = jnp.where(device_ref[0] % 2 == 0, count, 0)
    far = jnp.where(device_ref[0] % 4 < 2, count, 0)
    load_recv.wait()
    for group in range(index_ref.shape[0]):
        rows = recv_ref[0:1, group * EDGE:(group + 1) * EDGE]
        index_ref[group:group + 1, :] = rows ^ jnp.where(rows < 2 * count, near, far)
    fill_one_hot(index_ref, recv_hot_ref)
    load.wait()

    def step(turn, total):
        for u in range(unroll):
            k = turn * unroll + u
            tile = held_ref[order_ref[0, k]].astype(jnp.float32)
            total = total * order_ref[3, k].astype(jnp.float32) + tile
            start = pl.multiple_of(order_ref[1, k] * EDGE, EDGE)
            dense_ref[order_ref[2, k], pl.ds(start, EDGE), :] = total.astype(jnp.bfloat16)
        return total

    lax.fori_loop(
        0, (live_ref[0] + unroll - 1) // unroll, step, jnp.zeros((EDGE, EDGE), jnp.float32)
    )
    own_blocks = height // EDGE
    size = 512

    @pl.loop(0, height // size)
    def _(m):
        start = pl.multiple_of(m * size, size)
        own_ref[pl.ds(start, size), :] = jnp.dot(
            adjacency_block(dense_ref, 0, own_blocks, start, size),
            rows_ref[...],
            preferred_element_type=jnp.float32,
        )


def add_moments(z, moment_ref):
    wide = z.astype(jnp.float32)
    moment_ref[0:8, :] += jnp.sum(wide.reshape(-1, 8, wide.shape[1]), axis=0)
    moment_ref[8:16, :] += jnp.sum(jnp.square(wide).reshape(-1, 8, wide.shape[1]), axis=0)


def put_moments(moment_ref, out_ref):
    both = jnp.concatenate(
        [
            jnp.sum(moment_ref[0:8, :], axis=0, keepdims=True),
            jnp.sum(moment_ref[8:16, :], axis=0, keepdims=True),
        ],
        axis=0,
    )
    for n in range(out_ref.shape[0]):
        out_ref[n] = both


def first_kernel(recv_hot_ref, a, b, c, d, dense_ref, own_ref, weight_ref, send_hot_ref,
                 z_ref, stats_ref, oa, ob, oc, od, halo_ref, got_ref, moment_ref):
    layer = 0
    count = a.shape[0]
    for n, piece in enumerate((a, b, c, d)):
        got_ref[pl.ds(n * count, count), :] = piece[...]
    halo_ref[...] = jnp.dot(
        recv_hot_ref[...], got_ref[...], preferred_element_type=jnp.float32
    ).astype(jnp.bfloat16)
    moment_ref[...] = jnp.zeros_like(moment_ref)
    height = z_ref.shape[0]
    own_blocks, halo_blocks = height // EDGE, halo_ref.shape[0] // EDGE
    size = 512

    @pl.loop(0, height // size)
    def _(m):
        start = pl.multiple_of(m * size, size)
        agg = own_ref[pl.ds(start, size), :] + jnp.dot(
            adjacency_block(dense_ref, own_blocks, own_blocks + halo_blocks, start, size),
            halo_ref[...],
            preferred_element_type=jnp.float32,
        )
        z = jnp.dot(
            agg.astype(jnp.bfloat16), weight_ref[layer], preferred_element_type=jnp.float32
        ).astype(jnp.bfloat16)
        z_ref[pl.ds(start, size), :] = z
        add_moments(z, moment_ref)

    put_moments(moment_ref, stats_ref)
    pick_pieces(send_hot_ref, z_ref, (oa, ob, oc, od))


def scale_of(stats_ref, gain_ref, shift_ref, layer, vertex_total):
    both = jnp.sum(stats_ref[...], axis=0) / vertex_total
    centre = both[0:1, :]
    spread = both[1:2, :] - jnp.square(centre)
    factor = gain_ref[layer:layer + 1, :] / jnp.sqrt(spread + norm_eps)
    return centre, factor, shift_ref[layer:layer + 1, :]


def normal(rows, terms):
    centre, factor, shift = terms
    return jnp.maximum((rows.astype(jnp.float32) - centre) * factor + shift, 0.0)


def second_kernel(device_total, device_ref, recv_hot_ref, a, b, c, d, mixed_ref, stats_in_ref,
                  gain_ref, shift_ref, dense_ref, weight_ref, z_ref, stats_ref,
                  got_ref, columns_ref, moment_ref):
    layer = 1
    count = a.shape[0]
    height = z_ref.shape[0]
    halo = 4 * count
    terms = scale_of(stats_in_ref, gain_ref, shift_ref, 0, device_total * height)
    device = device_ref[0]
    near_side = (device > 0) & (device < device_total - 1)
    far_side = (device > 1) & (device < device_total - 2)
    present = (1.0, near_side.astype(jnp.float32), 1.0, far_side.astype(jnp.float32))
    for n, piece in enumerate((a, b, c, d)):
        got_ref[pl.ds(n * count, count), :] = (
            normal(piece[...], terms) * present[n]
        ).astype(jnp.bfloat16)
    columns_ref[pl.ds(height, halo), :] = jnp.dot(
        recv_hot_ref[...], got_ref[...], preferred_element_type=jnp.float32
    ).astype(jnp.bfloat16)
    for part in range(8):
        rows = pl.ds(part * (height // 8), height // 8)
        columns_ref[rows, :] = normal(mixed_ref[rows, :], terms).astype(jnp.bfloat16)
    moment_ref[...] = jnp.zeros_like(moment_ref)
    size = 512

    @pl.loop(0, height // size)
    def _(m):
        start = pl.multiple_of(m * size, size)
        agg = jnp.dot(
            adjacency_block(dense_ref, 0, (height + halo) // EDGE, start, size),
            columns_ref[...],
            preferred_element_type=jnp.float32,
        )
        z = jnp.dot(
            agg.astype(jnp.bfloat16), weight_ref[layer], preferred_element_type=jnp.float32
        ).astype(jnp.bfloat16)
        z_ref[pl.ds(start, size), :] = z
        add_moments(z, moment_ref)

    put_moments(moment_ref, stats_ref)


def last_kernel(vertex_total, mixed_ref, stats_in_ref, gain_ref, shift_ref, out_ref):
    terms = scale_of(stats_in_ref, gain_ref, shift_ref, 1, vertex_total)
    out_ref[...] = normal(mixed_ref[...], terms).astype(jnp.bfloat16)


def total_kernel(parts_ref, out_ref):
    both = jnp.sum(parts_ref[...], axis=0)
    for n in range(out_ref.shape[0]):
        out_ref[n] = both


VMEM = pl.BlockSpec(memory_space=pltpu.VMEM)
SMEM = pl.BlockSpec(memory_space=pltpu.SMEM)
HBM = pl.BlockSpec(memory_space=pltpu.HBM)


def all_sums(stats):
    stats = lax.all_to_all(stats, COLUMN, 0, 0, tiled=True)
    stats = pl.pallas_call(
        total_kernel,
        out_shape=jax.ShapeDtypeStruct((lax.axis_size(PLANE),) + stats.shape[1:], stats.dtype),
        in_specs=[VMEM],
        out_specs=VMEM,
        compiler_params=pltpu.CompilerParams(vmem_limit_bytes=MIB),
    )(stats)
    return lax.all_to_all(stats, PLANE, 0, 0, tiled=True)


def shards(features, tile_values, tile_blocks, tile_count, send_rows, recv_index,
           layer_weight, norm_gain, norm_shift):
    height, channels = features.shape
    neighbours, count = send_rows.shape[1:]
    halo = neighbours * count
    row_count = height // EDGE
    column_count = (height + halo) // EDGE
    device = lax.axis_index(PARTS)
    total = lax.axis_size(PARTS)
    vertex_total = height * total
    peers = lax.axis_size(COLUMN)
    bf16, f32 = jnp.bfloat16, jnp.float32
    struct = jax.ShapeDtypeStruct
    piece = struct((count, channels), bf16)
    stats_type = struct((peers, 2, channels), f32)
    mixed = struct((height, channels), bf16)

    place = device.reshape(1)

    def on_chip(value):
        return pltpu.with_memory_space_constraint(value, pltpu.VMEM)

    def in_hbm(value):
        return pltpu.with_memory_space_constraint(value, pltpu.HBM)

    *pieces, send_hot, order, rows = pl.pallas_call(
        functools.partial(gather_kernel, row_count, column_count),
        out_shape=[piece] * 4 + [
            pltpu.VMEM((halo, height), bf16),
            struct((4, tile_blocks.shape[0]), jnp.int32),
            pltpu.VMEM((height, channels), bf16),
        ],
        in_specs=[SMEM, SMEM, HBM, HBM, HBM],
        out_specs=[VMEM] * 7,
        scratch_shapes=[
            pltpu.VMEM((neighbours, count), jnp.int32),
            pltpu.VMEM((2, tile_blocks.shape[0]), jnp.int32),
            pltpu.VMEM((halo // EDGE, EDGE), jnp.int32),
            pltpu.SemaphoreType.DMA((3,)),
        ],
        compiler_params=pltpu.CompilerParams(vmem_limit_bytes=16 * MIB),
        cost_estimate=pl.CostEstimate(
            flops=2 * halo * height * channels, bytes_accessed=2 * MIB, transcendentals=0),
    )(place, tile_count, in_hbm(send_rows[0]), in_hbm(tile_blocks.T), in_hbm(features))
    got = exchange(pieces)

    dense, own, recv_hot = pl.pallas_call(
        functools.partial(build_kernel, count),
        out_shape=[
            pltpu.VMEM((column_count + 1, height, EDGE), bf16),
            pltpu.VMEM((height, channels), f32),
            pltpu.VMEM((halo, halo), bf16),
        ],
        in_specs=[SMEM, SMEM, SMEM, HBM, HBM, VMEM],
        out_specs=[VMEM] * 3,
        scratch_shapes=[
            pltpu.VMEM(tile_values.shape, bf16),
            pltpu.VMEM(recv_index.shape, jnp.int32),
            pltpu.VMEM((halo // EDGE, EDGE), jnp.int32),
            pltpu.SemaphoreType.DMA((2,)),
        ],
        compiler_params=pltpu.CompilerParams(vmem_limit_bytes=16 * MIB),
        cost_estimate=pl.CostEstimate(
            flops=4 * height * height * channels, bytes_accessed=24 * MIB, transcendentals=0),
    )(place, order, tile_count, in_hbm(recv_index), in_hbm(tile_values), on_chip(rows))
    dense, recv_hot = on_chip(dense), on_chip(recv_hot)

    z, stats, *pieces = pl.pallas_call(
        first_kernel,
        out_shape=[pltpu.VMEM(mixed.shape, bf16), stats_type] + [piece] * 4,
        in_specs=[VMEM] * 9,
        out_specs=[VMEM] * 6,
        scratch_shapes=[
            pltpu.VMEM((halo, channels), bf16),
            pltpu.VMEM((halo, channels), bf16),
            pltpu.VMEM((16, channels), f32),
        ],
        compiler_params=pltpu.CompilerParams(vmem_limit_bytes=12 * MIB),
        cost_estimate=pl.CostEstimate(
            flops=2 * height * halo * channels, bytes_accessed=16 * MIB, transcendentals=0),
    )(recv_hot, *got, dense, on_chip(own), layer_weight, on_chip(send_hot))
    got = exchange(pieces)
    stats = all_sums(stats)

    z, stats = pl.pallas_call(
        functools.partial(second_kernel, total),
        out_shape=[pltpu.VMEM(mixed.shape, bf16), stats_type],
        in_specs=[SMEM] + [VMEM] * 11,
        out_specs=[VMEM] * 2,
        scratch_shapes=[
            pltpu.VMEM((halo, channels), bf16),
            pltpu.VMEM((height + halo, channels), bf16),
            pltpu.VMEM((16, channels), f32),
        ],
        compiler_params=pltpu.CompilerParams(vmem_limit_bytes=12 * MIB),
        cost_estimate=pl.CostEstimate(
            flops=2 * height * (height + halo) * channels, bytes_accessed=16 * MIB,
            transcendentals=0),
    )(place, recv_hot, *got, on_chip(z), stats, norm_gain, norm_shift, dense, layer_weight)
    stats = all_sums(stats)

    return pl.pallas_call(
        functools.partial(last_kernel, vertex_total),
        out_shape=mixed,
        in_specs=[VMEM] * 4,
        out_specs=VMEM,
        compiler_params=pltpu.CompilerParams(vmem_limit_bytes=16 * MIB),
    )(on_chip(z), stats, norm_gain, norm_shift)


def solution(mesh):
    finer = Mesh(mesh.devices.reshape(4, 4, 8, 2), PARTS)
    placed = (
        P(PARTS, None),
        P(PARTS, None, None),
        P(PARTS, None),
        P(PARTS),
        P(PARTS, None, None),
        P(PARTS, None),
        P(),
        P(),
        P(),
    )
    return jax.shard_map(
        shards, mesh=finer, in_specs=placed, out_specs=P(PARTS, None), check_vma=False
    )
```

```python
import functools

import jax
import jax.numpy as jnp
from jax import lax
from jax.experimental import pallas as pl
from jax.experimental.pallas import tpu as pltpu
from jax.sharding import Mesh
from jax.sharding import PartitionSpec as P

PARTS = ("parts_0", "parts_1", "parts_2", "parts_3")
PLANE = PARTS[:2]
COLUMN = PARTS[2:]
norm_eps = 1e-05
EDGE = 128
MIB = 1 << 20


def swap(value, first, stride, total):
    pairs = []
    for q in range(total - stride):
        if first(q):
            pairs += [(q, q + stride), (q + stride, q)]
    return lax.ppermute(value, PARTS, pairs)


def chip_swaps(to_c, to_d):
    total = lax.axis_size(PARTS)
    return (
        swap(to_c, lambda q: q % 4 < 2, 2, total),
        swap(to_d, lambda q: q % 4 >= 2, 2, total),
    )


def core_swap(value):
    return swap(value, lambda q: q % 2 == 0, 1, lax.axis_size(PARTS))


def fill_one_hot(index_ref, one_hot_ref, groups):
    columns = one_hot_ref.shape[1]
    lanes = lax.broadcasted_iota(jnp.int32, (EDGE, EDGE), 1)
    for group in groups:
        row = jnp.broadcast_to(index_ref[pl.ds(group, 1), :], (EDGE, EDGE))
        away = row.T - lanes
        for block in range(columns // EDGE):
            one_hot_ref[pl.ds(group * EDGE, EDGE), pl.ds(block * EDGE, EDGE)] = jnp.where(
                away == block * EDGE, 1.0, 0.0
            ).astype(jnp.bfloat16)


def pick_piece(one_hot_ref, rows_ref, piece_ref, first, at, count):
    piece_ref[pl.ds(at, count), :] = jnp.dot(
        one_hot_ref[pl.ds(first, count), :], rows_ref[...], preferred_element_type=jnp.float32
    ).astype(jnp.bfloat16)


def pick_payloads(one_hot_ref, rows_ref, to_c, to_d):
    size = to_c.shape[0]
    pick_piece(one_hot_ref, rows_ref, to_c, 0, 0, size)
    pick_piece(one_hot_ref, rows_ref, to_d, size, 0, size)


def spread(row):
    n = row.shape[1]
    return jnp.broadcast_to(row, (n, n)).T


def put_tile_order(blocks_ref, live_count, row_count, column_count, order_ref):
    tiles = blocks_ref.shape[1]
    number = lax.broadcasted_iota(jnp.int32, (1, tiles), 1)
    live = number < live_count
    row = jnp.where(live, blocks_ref[0:1, :], 0)
    column = jnp.where(live, blocks_ref[1:2, :], column_count)
    cell = column * row_count + row
    key = cell * tiles + number
    down = lax.broadcasted_iota(jnp.int32, (tiles, tiles), 0)
    cells_down = spread(cell)
    keys_down = cells_down * tiles + down
    rank = jnp.sum((keys_down < key).astype(jnp.int32), axis=0, keepdims=True)
    same = (cells_down == cell) & (down < number)
    keep = jnp.sum(same.astype(jnp.int32), axis=0, keepdims=True) > 0
    packed = (cell * 2 + keep.astype(jnp.int32)) * tiles + number
    hit = spread(rank) == number
    packed = jnp.sum(jnp.where(hit, spread(packed), 0), axis=0, keepdims=True)
    cell = packed // (2 * tiles)
    order_ref[0:1, :] = packed % tiles
    order_ref[1:2, :] = cell % row_count
    order_ref[2:3, :] = cell // row_count
    order_ref[3:4, :] = (packed // tiles) % 2


def gather_kernel(row_count, column_count, device_ref, live_ref, send_in, blocks_in, features_ref,
                  to_c, to_d, one_hot_ref, order_ref, rows_ref,
                  send_ref, blocks_ref, index_ref, arrived):
    load_send = pltpu.make_async_copy(send_in, send_ref, arrived.at[0])
    load_blocks = pltpu.make_async_copy(blocks_in, blocks_ref, arrived.at[1])
    load = pltpu.make_async_copy(features_ref, rows_ref, arrived.at[2])
    load_send.start()
    load_blocks.start()
    load.start()
    load_send.wait()
    even_chip = device_ref[0] % 4 < 2
    count = send_ref.shape[1]
    per_piece = count // EDGE
    for part in range(per_piece):
        n0, n1, n2, n3 = (send_ref[n:n + 1, part * EDGE:(part + 1) * EDGE] for n in range(4))
        lists = (
            jnp.where(even_chip, n2, n3),
            jnp.where(even_chip, n0, n1),
            jnp.where(even_chip, n3, n2),
            jnp.where(even_chip, n1, n0),
        )
        for n, chosen in enumerate(lists):
            at = n * per_piece + part
            index_ref[at:at + 1, :] = chosen
    fill_one_hot(index_ref, one_hot_ref, range(2 * per_piece))
    load_blocks.wait()
    put_tile_order(blocks_ref, live_ref[0], row_count, column_count, order_ref)
    load.wait()
    pick_piece(one_hot_ref, rows_ref, to_c, 0, 0, count)
    fill_one_hot(index_ref, one_hot_ref, range(2 * per_piece, 3 * per_piece))
    pick_piece(one_hot_ref, rows_ref, to_c, count, count, count)
    fill_one_hot(index_ref, one_hot_ref, range(3 * per_piece, 4 * per_piece))
    pick_piece(one_hot_ref, rows_ref, to_d, 2 * count, 0, count)
    pick_piece(one_hot_ref, rows_ref, to_d, 3 * count, count, count)


def put_relay(device_ref, sent_c, sent_d, got_c, got_d, out_ref):
    count = out_ref.shape[0] // 2
    first = (device_ref[0] % 4 < 2) == (device_ref[0] % 2 == 0)

    @pl.when(first)
    def _():
        out_ref[0:count, :] = sent_c[count:2 * count, :]
        out_ref[count:2 * count, :] = got_c[count:2 * count, :]

    @pl.when(jnp.logical_not(first))
    def _():
        out_ref[0:count, :] = sent_d[count:2 * count, :]
        out_ref[count:2 * count, :] = got_d[count:2 * count, :]


def relay_kernel(after_ref, device_ref, sent_c, sent_d, got_c, got_d, out_ref):
    del after_ref
    put_relay(device_ref, sent_c, sent_d, got_c, got_d, out_ref)


def put_total(parts_ref, out_ref):
    both = jnp.sum(parts_ref[...], axis=0)
    for n in range(out_ref.shape[0]):
        out_ref[n] = both


def relay_total_kernel(device_ref, sent_c, sent_d, got_c, got_d, parts_ref, out_ref, total_ref):
    put_total(parts_ref, total_ref)
    put_relay(device_ref, sent_c, sent_d, got_c, got_d, out_ref)


def adjacency_block(dense_ref, first, last, start, size):
    return jnp.concatenate(
        [dense_ref[c, pl.ds(start, size), :] for c in range(first, last)], axis=1
    )


def build_kernel(count, device_ref, order_ref, live_ref, recv_in, tiles_ref,
                 dense_ref, recv_hot_ref, held_ref, recv_ref, index_ref, arrived):
    load_recv = pltpu.make_async_copy(recv_in, recv_ref, arrived.at[0])
    load = pltpu.make_async_copy(tiles_ref, held_ref, arrived.at[1])
    load_recv.start()
    load.start()
    blocks, height = dense_ref.shape[0], dense_ref.shape[1]
    unroll = 8
    zeros = jnp.zeros((height // 8, EDGE), jnp.bfloat16)

    @pl.loop(0, blocks)
    def _(c):
        for part in range(8):
            dense_ref[c, pl.ds(part * (height // 8), height // 8), :] = zeros

    near = jnp.where(device_ref[0] % 2 == 0, count, 0)
    far = jnp.where(device_ref[0] % 4 < 2, count, 0)
    load_recv.wait()
    for group in range(index_ref.shape[0]):
        rows = recv_ref[0:1, group * EDGE:(group + 1) * EDGE]
        index_ref[group:group + 1, :] = rows ^ jnp.where(rows < 2 * count, near, far)
    fill_one_hot(index_ref, recv_hot_ref, range(index_ref.shape[0]))
    load.wait()

    def step(turn, total):
        for u in range(unroll):
            k = turn * unroll + u
            tile = held_ref[order_ref[0, k]].astype(jnp.float32)
            total = total * order_ref[3, k].astype(jnp.float32) + tile
            start = pl.multiple_of(order_ref[1, k] * EDGE, EDGE)
            dense_ref[order_ref[2, k], pl.ds(start, EDGE), :] = total.astype(jnp.bfloat16)
        return total

    lax.fori_loop(
        0, (live_ref[0] + unroll - 1) // unroll, step, jnp.zeros((EDGE, EDGE), jnp.float32)
    )


def own_kernel(after_ref, dense_ref, rows_ref, own_ref):
    del after_ref
    height = own_ref.shape[0]
    own_blocks = height // EDGE
    size = 512

    @pl.loop(0, height // size)
    def _(m):
        start = pl.multiple_of(m * size, size)
        own_ref[pl.ds(start, size), :] = jnp.dot(
            adjacency_block(dense_ref, 0, own_blocks, start, size),
            rows_ref[...],
            preferred_element_type=jnp.float32,
        )


def add_moments(z, moment_ref):
    wide = z.astype(jnp.float32)
    moment_ref[0:8, :] += jnp.sum(wide.reshape(-1, 8, wide.shape[1]), axis=0)
    moment_ref[8:16, :] += jnp.sum(jnp.square(wide).reshape(-1, 8, wide.shape[1]), axis=0)


def put_moments(moment_ref, out_ref):
    both = jnp.concatenate(
        [
            jnp.sum(moment_ref[0:8, :], axis=0, keepdims=True),
            jnp.sum(moment_ref[8:16, :], axis=0, keepdims=True),
        ],
        axis=0,
    )
    for n in range(out_ref.shape[0]):
        out_ref[n] = both


def received(a, c, d):
    count = a.shape[0] // 2
    return a[0:count, :], a[count:2 * count, :], c[0:count, :], d[0:count, :]


def first_kernel(recv_hot_ref, a, c, d, dense_ref, own_ref, weight_ref, send_hot_ref,
                 z_ref, stats_ref, to_c, to_d, halo_ref, got_ref, moment_ref):
    layer = 0
    count = a.shape[0] // 2
    for n, piece in enumerate(received(a, c, d)):
        got_ref[pl.ds(n * count, count), :] = piece
    halo_ref[...] = jnp.dot(
        recv_hot_ref[...], got_ref[...], preferred_element_type=jnp.float32
    ).astype(jnp.bfloat16)
    moment_ref[...] = jnp.zeros_like(moment_ref)
    height = z_ref.shape[0]
    own_blocks, halo_blocks = height // EDGE, halo_ref.shape[0] // EDGE
    size = 512

    @pl.loop(0, height // size)
    def _(m):
        start = pl.multiple_of(m * size, size)
        agg = own_ref[pl.ds(start, size), :] + jnp.dot(
            adjacency_block(dense_ref, own_blocks, own_blocks + halo_blocks, start, size),
            halo_ref[...],
            preferred_element_type=jnp.float32,
        )
        z = jnp.dot(
            agg.astype(jnp.bfloat16), weight_ref[layer], preferred_element_type=jnp.float32
        ).astype(jnp.bfloat16)
        z_ref[pl.ds(start, size), :] = z
        add_moments(z, moment_ref)

    put_moments(moment_ref, stats_ref)
    pick_payloads(send_hot_ref, z_ref, to_c, to_d)


def scale_of(stats_ref, gain_ref, shift_ref, layer, vertex_total):
    both = jnp.sum(stats_ref[...], axis=0) / vertex_total
    centre = both[0:1, :]
    spread = both[1:2, :] - jnp.square(centre)
    factor = gain_ref[layer:layer + 1, :] / jnp.sqrt(spread + norm_eps)
    return centre, factor, shift_ref[layer:layer + 1, :]


def normal(rows, terms):
    centre, factor, shift = terms
    return jnp.maximum((rows.astype(jnp.float32) - centre) * factor + shift, 0.0)


def second_kernel(device_total, device_ref, recv_hot_ref, a, c, d, mixed_ref, stats_in_ref,
                  gain_ref, shift_ref, dense_ref, weight_ref, z_ref, stats_ref,
                  got_ref, columns_ref, moment_ref):
    layer = 1
    count = a.shape[0] // 2
    height = z_ref.shape[0]
    halo = 4 * count
    terms = scale_of(stats_in_ref, gain_ref, shift_ref, 0, device_total * height)
    device = device_ref[0]
    near_side = (device > 0) & (device < device_total - 1)
    far_side = (device > 1) & (device < device_total - 2)
    present = (1.0, near_side.astype(jnp.float32), 1.0, far_side.astype(jnp.float32))
    for n, piece in enumerate(received(a, c, d)):
        got_ref[pl.ds(n * count, count), :] = (
            normal(piece, terms) * present[n]
        ).astype(jnp.bfloat16)
    columns_ref[pl.ds(height, halo), :] = jnp.dot(
        recv_hot_ref[...], got_ref[...], preferred_element_type=jnp.float32
    ).astype(jnp.bfloat16)
    for part in range(8):
        rows = pl.ds(part * (height // 8), height // 8)
        columns_ref[rows, :] = normal(mixed_ref[rows, :], terms).astype(jnp.bfloat16)
    moment_ref[...] = jnp.zeros_like(moment_ref)
    size = 512

    @pl.loop(0, height // size)
    def _(m):
        start = pl.multiple_of(m * size, size)
        agg = jnp.dot(
            adjacency_block(dense_ref, 0, (height + halo) // EDGE, start, size),
            columns_ref[...],
            preferred_element_type=jnp.float32,
        )
        z = jnp.dot(
            agg.astype(jnp.bfloat16), weight_ref[layer], preferred_element_type=jnp.float32
        ).astype(jnp.bfloat16)
        z_ref[pl.ds(start, size), :] = z
        add_moments(z, moment_ref)

    put_moments(moment_ref, stats_ref)


def last_kernel(vertex_total, mixed_ref, stats_in_ref, gain_ref, shift_ref, out_ref):
    terms = scale_of(stats_in_ref, gain_ref, shift_ref, 1, vertex_total)
    out_ref[...] = normal(mixed_ref[...], terms).astype(jnp.bfloat16)


VMEM = pl.BlockSpec(memory_space=pltpu.VMEM)
SMEM = pl.BlockSpec(memory_space=pltpu.SMEM)
HBM = pl.BlockSpec(memory_space=pltpu.HBM)


def from_peers(stats, axes):
    return lax.all_to_all(stats, axes, 0, 0, tiled=True)


def shards(features, tile_values, tile_blocks, tile_count, send_rows, recv_index,
           layer_weight, norm_gain, norm_shift):
    height, channels = features.shape
    neighbours, count = send_rows.shape[1:]
    halo = neighbours * count
    row_count = height // EDGE
    column_count = (height + halo) // EDGE
    device = lax.axis_index(PARTS)
    total = lax.axis_size(PARTS)
    vertex_total = height * total
    peers = lax.axis_size(PLANE)
    bf16, f32 = jnp.bfloat16, jnp.float32
    struct = jax.ShapeDtypeStruct
    payload = struct((2 * count, channels), bf16)
    stats_type = struct((peers, 2, channels), f32)
    mixed = struct((height, channels), bf16)

    place = device.reshape(1)

    def on_chip(value):
        return pltpu.with_memory_space_constraint(value, pltpu.VMEM)

    def in_hbm(value):
        return pltpu.with_memory_space_constraint(value, pltpu.HBM)

    *sent, send_hot, order, rows = pl.pallas_call(
        functools.partial(gather_kernel, row_count, column_count),
        out_shape=[payload] * 2 + [
            pltpu.VMEM((halo, height), bf16),
            struct((4, tile_blocks.shape[0]), jnp.int32),
            pltpu.VMEM((height, channels), bf16),
        ],
        in_specs=[SMEM, SMEM, HBM, HBM, HBM],
        out_specs=[VMEM] * 5,
        scratch_shapes=[
            pltpu.VMEM((neighbours, count), jnp.int32),
            pltpu.VMEM((2, tile_blocks.shape[0]), jnp.int32),
            pltpu.VMEM((halo // EDGE, EDGE), jnp.int32),
            pltpu.SemaphoreType.DMA((3,)),
        ],
        compiler_params=pltpu.CompilerParams(vmem_limit_bytes=16 * MIB),
        cost_estimate=pl.CostEstimate(
            flops=2 * halo * height * channels, bytes_accessed=2 * MIB, transcendentals=0),
    )(place, tile_count, in_hbm(send_rows[0]), in_hbm(tile_blocks.T), in_hbm(features))
    got = chip_swaps(*sent)

    dense, recv_hot = pl.pallas_call(
        functools.partial(build_kernel, count),
        out_shape=[
            pltpu.VMEM((column_count + 1, height, EDGE), bf16),
            pltpu.VMEM((halo, halo), bf16),
        ],
        in_specs=[SMEM, SMEM, SMEM, HBM, HBM],
        out_specs=[VMEM] * 2,
        scratch_shapes=[
            pltpu.VMEM(tile_values.shape, bf16),
            pltpu.VMEM(recv_index.shape, jnp.int32),
            pltpu.VMEM((halo // EDGE, EDGE), jnp.int32),
            pltpu.SemaphoreType.DMA((2,)),
        ],
        compiler_params=pltpu.CompilerParams(vmem_limit_bytes=16 * MIB),
        cost_estimate=pl.CostEstimate(
            flops=4 * height * height * channels, bytes_accessed=24 * MIB, transcendentals=0),
    )(place, order, tile_count, in_hbm(recv_index), in_hbm(tile_values))
    dense, recv_hot = on_chip(dense), on_chip(recv_hot)

    relay = pl.pallas_call(
        relay_kernel,
        out_shape=payload,
        in_specs=[VMEM, SMEM] + [VMEM] * 4,
        out_specs=VMEM,
        compiler_params=pltpu.CompilerParams(vmem_limit_bytes=4 * MIB),
    )(recv_hot, place, *sent, *got)
    got_core = core_swap(relay)

    own = pl.pallas_call(
        own_kernel,
        out_shape=pltpu.VMEM((height, channels), f32),
        in_specs=[VMEM] * 3,
        out_specs=VMEM,
        compiler_params=pltpu.CompilerParams(vmem_limit_bytes=8 * MIB),
        cost_estimate=pl.CostEstimate(
            flops=2 * height * height * channels, bytes_accessed=8 * MIB, transcendentals=0),
    )(relay, dense, on_chip(rows))

    z, stats, *sent = pl.pallas_call(
        first_kernel,
        out_shape=[pltpu.VMEM(mixed.shape, bf16), stats_type] + [payload] * 2,
        in_specs=[VMEM] * 8,
        out_specs=[VMEM] * 4,
        scratch_shapes=[
            pltpu.VMEM((halo, channels), bf16),
            pltpu.VMEM((halo, channels), bf16),
            pltpu.VMEM((16, channels), f32),
        ],
        compiler_params=pltpu.CompilerParams(vmem_limit_bytes=12 * MIB),
        cost_estimate=pl.CostEstimate(
            flops=2 * height * halo * channels, bytes_accessed=16 * MIB, transcendentals=0),
    )(recv_hot, got_core, *got, dense, on_chip(own), layer_weight, on_chip(send_hot))
    got = chip_swaps(*sent)
    stats = from_peers(stats, PLANE)
    column_stats = struct((lax.axis_size(COLUMN), 2, channels), f32)
    relay, stats = pl.pallas_call(
        relay_total_kernel,
        out_shape=[payload, column_stats],
        in_specs=[SMEM] + [VMEM] * 5,
        out_specs=[VMEM] * 2,
        compiler_params=pltpu.CompilerParams(vmem_limit_bytes=4 * MIB),
    )(place, *sent, *got, stats)
    got_core = core_swap(relay)
    stats = from_peers(stats, COLUMN)

    z, stats = pl.pallas_call(
        functools.partial(second_kernel, total),
        out_shape=[pltpu.VMEM(mixed.shape, bf16), stats_type],
        in_specs=[SMEM] + [VMEM] * 10,
        out_specs=[VMEM] * 2,
        scratch_shapes=[
            pltpu.VMEM((halo, channels), bf16),
            pltpu.VMEM((height + halo, channels), bf16),
            pltpu.VMEM((16, channels), f32),
        ],
        compiler_params=pltpu.CompilerParams(vmem_limit_bytes=12 * MIB),
        cost_estimate=pl.CostEstimate(
            flops=2 * height * (height + halo) * channels, bytes_accessed=16 * MIB,
            transcendentals=0),
    )(place, recv_hot, got_core, *got, on_chip(z), stats, norm_gain, norm_shift, dense, layer_weight)
    stats = from_peers(stats, PLANE)
    stats = pl.pallas_call(
        put_total,
        out_shape=column_stats,
        in_specs=[VMEM],
        out_specs=VMEM,
        compiler_params=pltpu.CompilerParams(vmem_limit_bytes=MIB),
    )(stats)
    stats = from_peers(stats, COLUMN)

    return pl.pallas_call(
        functools.partial(last_kernel, vertex_total),
        out_shape=mixed,
        in_specs=[VMEM] * 4,
        out_specs=VMEM,
        compiler_params=pltpu.CompilerParams(vmem_limit_bytes=16 * MIB),
    )(on_chip(z), stats, norm_gain, norm_shift)


def solution(mesh):
    finer = Mesh(mesh.devices.reshape(4, 4, 8, 2), PARTS)
    placed = (
        P(PARTS, None),
        P(PARTS, None, None),
        P(PARTS, None),
        P(PARTS),
        P(PARTS, None, None),
        P(PARTS, None),
        P(),
        P(),
        P(),
    )
    return jax.shard_map(
        shards, mesh=finer, in_specs=placed, out_specs=P(PARTS, None), check_vma=False
    )
```

```python
import functools

import jax
import jax.numpy as jnp
from jax import lax
from jax.experimental import pallas as pl
from jax.experimental.pallas import tpu as pltpu
from jax.sharding import Mesh
from jax.sharding import PartitionSpec as P


PARTS = ("parts_0", "parts_1", "parts_2", "parts_3")
PLANE = PARTS[:2]
COLUMN = PARTS[2:]
norm_eps = 1e-05
EDGE = 128
MIB = 1 << 20


def swap(value, first, stride, total):
    pairs = []
    for q in range(total - stride):
        if first(q):
            pairs += [(q, q + stride), (q + stride, q)]
    return lax.ppermute(value, PARTS, pairs)


def chip_swaps(to_c, to_d):
    total = lax.axis_size(PARTS)
    return (
        swap(to_c, lambda q: q % 4 < 2, 2, total),
        swap(to_d, lambda q: q % 4 >= 2, 2, total),
    )


def core_swap(value):
    return swap(value, lambda q: q % 2 == 0, 1, lax.axis_size(PARTS))


def fill_one_hot(index_ref, one_hot_ref, groups):
    columns = one_hot_ref.shape[1]
    lanes = lax.broadcasted_iota(jnp.int32, (EDGE, EDGE), 1)
    for group in groups:
        row = jnp.broadcast_to(index_ref[pl.ds(group, 1), :], (EDGE, EDGE))
        away = row.T - lanes
        for block in range(columns // EDGE):
            one_hot_ref[pl.ds(group * EDGE, EDGE), pl.ds(block * EDGE, EDGE)] = jnp.where(
                away == block * EDGE, 1.0, 0.0
            ).astype(jnp.bfloat16)


def pick_piece(one_hot_ref, rows_ref, piece_ref, first, at, count):
    piece_ref[pl.ds(at, count), :] = jnp.dot(
        one_hot_ref[pl.ds(first, count), :], rows_ref[...], preferred_element_type=jnp.float32
    ).astype(jnp.bfloat16)


def pick_payloads(one_hot_ref, rows_ref, to_c, to_d):
    size = to_c.shape[0]
    pick_piece(one_hot_ref, rows_ref, to_c, 0, 0, size)
    pick_piece(one_hot_ref, rows_ref, to_d, size, 0, size)


def spread(row):
    n = row.shape[1]
    return jnp.broadcast_to(row, (n, n)).T


def put_tile_order(blocks_ref, live_count, row_count, column_count, order_ref):
    tiles = blocks_ref.shape[1]
    number = lax.broadcasted_iota(jnp.int32, (1, tiles), 1)
    live = number < live_count
    row = jnp.where(live, blocks_ref[0:1, :], 0)
    column = jnp.where(live, blocks_ref[1:2, :], column_count)
    cell = column * row_count + row
    key = cell * tiles + number
    down = lax.broadcasted_iota(jnp.int32, (tiles, tiles), 0)
    cells_down = spread(cell)
    keys_down = cells_down * tiles + down
    rank = jnp.sum((keys_down < key).astype(jnp.int32), axis=0, keepdims=True)
    same = (cells_down == cell) & (down < number)
    keep = jnp.sum(same.astype(jnp.int32), axis=0, keepdims=True) > 0
    packed = (cell * 2 + keep.astype(jnp.int32)) * tiles + number
    hit = spread(rank) == number
    packed = jnp.sum(jnp.where(hit, spread(packed), 0), axis=0, keepdims=True)
    cell = packed // (2 * tiles)
    order_ref[0:1, :] = packed % tiles
    order_ref[1:2, :] = cell % row_count
    order_ref[2:3, :] = cell // row_count
    order_ref[3:4, :] = (packed // tiles) % 2


def gather_kernel(row_count, column_count, device_ref, live_ref, send_in, blocks_in, features_ref,
                  to_c, to_d, near_ref, one_hot_ref, order_ref, rows_ref,
                  send_ref, blocks_ref, index_ref, arrived):
    load_send = pltpu.make_async_copy(send_in, send_ref, arrived.at[0])
    load_blocks = pltpu.make_async_copy(blocks_in, blocks_ref, arrived.at[1])
    load = pltpu.make_async_copy(features_ref, rows_ref, arrived.at[2])
    load_send.start()
    load_blocks.start()
    load.start()
    load_send.wait()
    even_chip = device_ref[0] % 4 < 2
    count = send_ref.shape[1]
    per_piece = count // EDGE
    for part in range(per_piece):
        n0, n1, n2, n3 = (send_ref[n:n + 1, part * EDGE:(part + 1) * EDGE] for n in range(4))
        lists = (
            jnp.where(even_chip, n2, n3),
            jnp.where(even_chip, n0, n1),
            jnp.where(even_chip, n3, n2),
            jnp.where(even_chip, n1, n0),
        )
        for n, chosen in enumerate(lists):
            at = n * per_piece + part
            index_ref[at:at + 1, :] = chosen
    fill_one_hot(index_ref, one_hot_ref, range(2 * per_piece))
    load_blocks.wait()
    put_tile_order(blocks_ref, live_ref[0], row_count, column_count, order_ref)
    load.wait()
    pick_piece(one_hot_ref, rows_ref, to_c, 0, 0, count)
    fill_one_hot(index_ref, one_hot_ref, range(2 * per_piece, 3 * per_piece))
    pick_piece(one_hot_ref, rows_ref, to_c, count, count, count)
    fill_one_hot(index_ref, one_hot_ref, range(3 * per_piece, 4 * per_piece))
    pick_piece(one_hot_ref, rows_ref, to_d, 2 * count, 0, count)
    pick_piece(one_hot_ref, rows_ref, to_d, 3 * count, count, count)
    put_near(device_ref, to_c, to_d, near_ref, 0)


def put_near(device_ref, from_c, from_d, out_ref, at):
    count = from_c.shape[0] // 2
    first = (device_ref[0] % 4 < 2) == (device_ref[0] % 2 == 0)

    @pl.when(first)
    def _():
        out_ref[at:at + count, :] = from_c[count:2 * count, :]

    @pl.when(jnp.logical_not(first))
    def _():
        out_ref[at:at + count, :] = from_d[count:2 * count, :]


def relay_kernel(after_ref, device_ref, near_ref, got_c, got_d, out_ref):
    del after_ref
    count = near_ref.shape[0]
    out_ref[0:count, :] = near_ref[...]
    put_near(device_ref, got_c, got_d, out_ref, count)


def put_total(parts_ref, out_ref):
    both = jnp.sum(parts_ref[...], axis=0)
    for n in range(out_ref.shape[0]):
        out_ref[n] = both


def adjacency_block(dense_ref, first, last, start, size):
    return jnp.concatenate(
        [dense_ref[c, pl.ds(start, size), :] for c in range(first, last)], axis=1
    )


def build_kernel(count, device_ref, order_ref, live_ref, recv_in, tiles_ref,
                 dense_ref, recv_hot_ref, index_ref, held_ref, recv_ref, arrived):
    load_recv = pltpu.make_async_copy(recv_in, recv_ref, arrived.at[0])
    load = pltpu.make_async_copy(tiles_ref, held_ref, arrived.at[1])
    load_recv.start()
    load.start()
    blocks, height = dense_ref.shape[0], dense_ref.shape[1]
    unroll = 8
    zeros = jnp.zeros((height // 8, EDGE), jnp.bfloat16)

    @pl.loop(0, blocks)
    def _(c):
        for part in range(8):
            dense_ref[c, pl.ds(part * (height // 8), height // 8), :] = zeros

    near = jnp.where(device_ref[0] % 2 == 0, count, 0)
    far = jnp.where(device_ref[0] % 4 < 2, count, 0)
    load_recv.wait()
    for group in range(index_ref.shape[0]):
        rows = recv_ref[0:1, group * EDGE:(group + 1) * EDGE]
        index_ref[group:group + 1, :] = rows ^ jnp.where(rows < 2 * count, near, far)
    fill_one_hot(index_ref, recv_hot_ref, range(index_ref.shape[0]))
    load.wait()

    def step(turn, total):
        for u in range(unroll):
            k = turn * unroll + u
            tile = held_ref[order_ref[0, k]].astype(jnp.float32)
            total = total * order_ref[3, k].astype(jnp.float32) + tile
            start = pl.multiple_of(order_ref[1, k] * EDGE, EDGE)
            dense_ref[order_ref[2, k], pl.ds(start, EDGE), :] = total.astype(jnp.bfloat16)
        return total

    lax.fori_loop(
        0, (live_ref[0] + unroll - 1) // unroll, step, jnp.zeros((EDGE, EDGE), jnp.float32)
    )


def own_kernel(after_ref, dense_ref, rows_ref, own_ref):
    del after_ref
    height = own_ref.shape[0]
    own_blocks = height // EDGE
    size = 512

    @pl.loop(0, height // size)
    def _(m):
        start = pl.multiple_of(m * size, size)
        own_ref[pl.ds(start, size), :] = jnp.dot(
            adjacency_block(dense_ref, 0, own_blocks, start, size),
            rows_ref[...],
            preferred_element_type=jnp.float32,
        )


def add_moments(z, moment_ref):
    wide = z.astype(jnp.float32)
    moment_ref[0:8, :] += jnp.sum(wide.reshape(-1, 8, wide.shape[1]), axis=0)
    moment_ref[8:16, :] += jnp.sum(jnp.square(wide).reshape(-1, 8, wide.shape[1]), axis=0)


def put_moments(moment_ref, out_ref):
    both = jnp.concatenate(
        [
            jnp.sum(moment_ref[0:8, :], axis=0, keepdims=True),
            jnp.sum(moment_ref[8:16, :], axis=0, keepdims=True),
        ],
        axis=0,
    )
    for n in range(out_ref.shape[0]):
        out_ref[n] = both


def received(a, c, d):
    count = a.shape[0] // 2
    return a[0:count, :], a[count:2 * count, :], c[0:count, :], d[0:count, :]


def first_kernel(device_ref, recv_hot_ref, a, c, d, dense_ref, own_ref, weight_ref, send_hot_ref,
                 z_ref, stats_ref, to_c, to_d, near_ref, halo_ref, got_ref, moment_ref):
    layer = 0
    count = a.shape[0] // 2
    for n, piece in enumerate(received(a, c, d)):
        got_ref[pl.ds(n * count, count), :] = piece
    halo_ref[...] = jnp.dot(
        recv_hot_ref[...], got_ref[...], preferred_element_type=jnp.float32
    ).astype(jnp.bfloat16)
    moment_ref[...] = jnp.zeros_like(moment_ref)
    height = z_ref.shape[0]
    own_blocks, halo_blocks = height // EDGE, halo_ref.shape[0] // EDGE
    size = 512

    @pl.loop(0, height // size)
    def _(m):
        start = pl.multiple_of(m * size, size)
        agg = own_ref[pl.ds(start, size), :] + jnp.dot(
            adjacency_block(dense_ref, own_blocks, own_blocks + halo_blocks, start, size),
            halo_ref[...],
            preferred_element_type=jnp.float32,
        )
        z = jnp.dot(
            agg.astype(jnp.bfloat16), weight_ref[layer], preferred_element_type=jnp.float32
        ).astype(jnp.bfloat16)
        z_ref[pl.ds(start, size), :] = z
        add_moments(z, moment_ref)

    put_moments(moment_ref, stats_ref)
    pick_payloads(send_hot_ref, z_ref, to_c, to_d)
    put_near(device_ref, to_c, to_d, near_ref, 0)


def scale_of(stats_ref, gain_ref, shift_ref, layer, vertex_total):
    both = jnp.sum(stats_ref[...], axis=0) / vertex_total
    centre = both[0:1, :]
    spread = both[1:2, :] - jnp.square(centre)
    factor = gain_ref[layer:layer + 1, :] / jnp.sqrt(spread + norm_eps)
    return centre, factor, shift_ref[layer:layer + 1, :]


def normal(rows, terms):
    centre, factor, shift = terms
    return jnp.maximum((rows.astype(jnp.float32) - centre) * factor + shift, 0.0)


def second_kernel(device_total, device_ref, hot_in, a, c, d, mixed_ref, stats_in_ref,
                  gain_ref, shift_ref, dense_in, weight_ref, z_ref, stats_ref,
                  got_ref, columns_ref, moment_ref, recv_hot_ref, dense_ref, arrived):
    layer = 1
    count = a.shape[0] // 2
    height = z_ref.shape[0]
    halo = 4 * count
    blocks = (height + halo) // EDGE
    size = dense_ref.shape[2]
    load_hot = pltpu.make_async_copy(hot_in, recv_hot_ref, arrived.at[height // size])
    load_hot.start()

    def load_dense(m):
        return pltpu.make_async_copy(
            dense_in.at[pl.ds(0, blocks), pl.ds(pl.multiple_of(m * size, size), size), :],
            dense_ref.at[m],
            arrived.at[m],
        )

    for m in range(height // size):
        load_dense(m).start()
    terms = scale_of(stats_in_ref, gain_ref, shift_ref, 0, device_total * height)
    device = device_ref[0]
    near_side = (device > 0) & (device < device_total - 1)
    far_side = (device > 1) & (device < device_total - 2)
    present = (1.0, near_side.astype(jnp.float32), 1.0, far_side.astype(jnp.float32))
    for n, piece in enumerate(received(a, c, d)):
        got_ref[pl.ds(n * count, count), :] = (
            normal(piece, terms) * present[n]
        ).astype(jnp.bfloat16)
    for part in range(8):
        rows = pl.ds(part * (height // 8), height // 8)
        columns_ref[rows, :] = normal(mixed_ref[rows, :], terms).astype(jnp.bfloat16)
    load_hot.wait()
    columns_ref[pl.ds(height, halo), :] = jnp.dot(
        recv_hot_ref[...], got_ref[...], preferred_element_type=jnp.float32
    ).astype(jnp.bfloat16)
    moment_ref[...] = jnp.zeros_like(moment_ref)

    @pl.loop(0, height // size)
    def _(m):
        load_dense(m).wait()
        start = pl.multiple_of(m * size, size)
        agg = jnp.dot(
            jnp.concatenate([dense_ref[m, c] for c in range(blocks)], axis=1),
            columns_ref[...],
            preferred_element_type=jnp.float32,
        )
        z = jnp.dot(
            agg.astype(jnp.bfloat16), weight_ref[layer], preferred_element_type=jnp.float32
        ).astype(jnp.bfloat16)
        z_ref[pl.ds(start, size), :] = z
        add_moments(z, moment_ref)

    put_moments(moment_ref, stats_ref)


def last_kernel(vertex_total, mixed_ref, stats_in_ref, gain_ref, shift_ref, out_ref):
    terms = scale_of(stats_in_ref, gain_ref, shift_ref, 1, vertex_total)
    out_ref[...] = normal(mixed_ref[...], terms).astype(jnp.bfloat16)


VMEM = pl.BlockSpec(memory_space=pltpu.VMEM)
SMEM = pl.BlockSpec(memory_space=pltpu.SMEM)
HBM = pl.BlockSpec(memory_space=pltpu.HBM)


def from_peers(stats, axes):
    return lax.all_to_all(stats, axes, 0, 0, tiled=True)


def shards(features, tile_values, tile_blocks, tile_count, send_rows, recv_index,
           layer_weight, norm_gain, norm_shift):
    height, channels = features.shape
    neighbours, count = send_rows.shape[1:]
    halo = neighbours * count
    row_count = height // EDGE
    column_count = (height + halo) // EDGE
    device = lax.axis_index(PARTS)
    total = lax.axis_size(PARTS)
    vertex_total = height * total
    peers = lax.axis_size(PLANE)
    bf16, f32 = jnp.bfloat16, jnp.float32
    struct = jax.ShapeDtypeStruct
    piece = struct((count, channels), bf16)
    payload = struct((2 * count, channels), bf16)
    stats_type = struct((peers, 2, channels), f32)
    mixed = struct((height, channels), bf16)

    place = device.reshape(1)

    def on_chip(value):
        return pltpu.with_memory_space_constraint(value, pltpu.VMEM)

    def in_hbm(value):
        return pltpu.with_memory_space_constraint(value, pltpu.HBM)

    *sent, near, send_hot, order, rows = pl.pallas_call(
        functools.partial(gather_kernel, row_count, column_count),
        out_shape=[payload] * 2 + [
            piece,
            pltpu.VMEM((halo, height), bf16),
            struct((4, tile_blocks.shape[0]), jnp.int32),
            pltpu.VMEM((height, channels), bf16),
        ],
        in_specs=[SMEM, SMEM, HBM, HBM, HBM],
        out_specs=[VMEM] * 6,
        scratch_shapes=[
            pltpu.VMEM((neighbours, count), jnp.int32),
            pltpu.VMEM((2, tile_blocks.shape[0]), jnp.int32),
            pltpu.VMEM((halo // EDGE, EDGE), jnp.int32),
            pltpu.SemaphoreType.DMA((3,)),
        ],
        compiler_params=pltpu.CompilerParams(vmem_limit_bytes=16 * MIB),
        cost_estimate=pl.CostEstimate(
            flops=2 * halo * height * channels, bytes_accessed=2 * MIB, transcendentals=0),
    )(place, tile_count, in_hbm(send_rows[0]), in_hbm(tile_blocks.T), in_hbm(features))
    got = chip_swaps(*sent)

    dense, recv_hot, built = pl.pallas_call(
        functools.partial(build_kernel, count),
        out_shape=[
            pltpu.VMEM((column_count + 1, height, EDGE), bf16),
            pltpu.VMEM((halo, halo), bf16),
            struct((halo // EDGE, EDGE), jnp.int32),
        ],
        in_specs=[SMEM, SMEM, SMEM, HBM, HBM],
        out_specs=[VMEM] * 3,
        scratch_shapes=[
            pltpu.VMEM(tile_values.shape, bf16),
            pltpu.VMEM(recv_index.shape, jnp.int32),
            pltpu.SemaphoreType.DMA((2,)),
        ],
        compiler_params=pltpu.CompilerParams(vmem_limit_bytes=16 * MIB),
        cost_estimate=pl.CostEstimate(
            flops=4 * height * height * channels, bytes_accessed=24 * MIB, transcendentals=0),
    )(place, order, tile_count, in_hbm(recv_index), in_hbm(tile_values))

    relay_call = pl.pallas_call(
        relay_kernel,
        out_shape=payload,
        in_specs=[VMEM, SMEM] + [VMEM] * 3,
        out_specs=VMEM,
        compiler_params=pltpu.CompilerParams(vmem_limit_bytes=4 * MIB),
    )
    relay = relay_call(built, place, near, *got)
    got_core = core_swap(relay)

    own = pl.pallas_call(
        own_kernel,
        out_shape=pltpu.VMEM((height, channels), f32),
        in_specs=[VMEM] * 3,
        out_specs=VMEM,
        compiler_params=pltpu.CompilerParams(vmem_limit_bytes=8 * MIB),
        cost_estimate=pl.CostEstimate(
            flops=2 * height * height * channels, bytes_accessed=8 * MIB, transcendentals=0),
    )(relay, on_chip(dense), on_chip(rows))

    z, stats, *sent, near = pl.pallas_call(
        first_kernel,
        out_shape=[pltpu.VMEM(mixed.shape, bf16), stats_type] + [payload] * 2 + [piece],
        in_specs=[SMEM] + [VMEM] * 8,
        out_specs=[VMEM] * 5,
        scratch_shapes=[
            pltpu.VMEM((halo, channels), bf16),
            pltpu.VMEM((halo, channels), bf16),
            pltpu.VMEM((16, channels), f32),
        ],
        compiler_params=pltpu.CompilerParams(vmem_limit_bytes=12 * MIB),
        cost_estimate=pl.CostEstimate(
            flops=2 * height * halo * channels, bytes_accessed=16 * MIB, transcendentals=0),
    )(place, on_chip(recv_hot), got_core, *got, on_chip(dense), on_chip(own), layer_weight, on_chip(send_hot))
    got = chip_swaps(*sent)
    stats = from_peers(stats, PLANE)
    column_stats = struct((lax.axis_size(COLUMN), 2, channels), f32)
    total_call = pl.pallas_call(
        put_total,
        out_shape=column_stats,
        in_specs=[VMEM],
        out_specs=VMEM,
        compiler_params=pltpu.CompilerParams(vmem_limit_bytes=MIB),
    )
    stats = from_peers(total_call(stats), COLUMN)
    relay = relay_call(built, place, near, *got)
    got_core = core_swap(relay)

    chunk = 512
    z, stats = pl.pallas_call(
        functools.partial(second_kernel, total),
        out_shape=[pltpu.VMEM(mixed.shape, bf16), stats_type],
        in_specs=[SMEM, HBM] + [VMEM] * 7 + [HBM, VMEM],
        out_specs=[VMEM] * 2,
        scratch_shapes=[
            pltpu.VMEM((halo, channels), bf16),
            pltpu.VMEM((height + halo, channels), bf16),
            pltpu.VMEM((16, channels), f32),
            pltpu.VMEM((halo, halo), bf16),
            pltpu.VMEM((height // chunk, column_count, chunk, EDGE), bf16),
            pltpu.SemaphoreType.DMA((height // chunk + 1,)),
        ],
        compiler_params=pltpu.CompilerParams(vmem_limit_bytes=28 * MIB),
        cost_estimate=pl.CostEstimate(
            flops=2 * height * (height + halo) * channels, bytes_accessed=16 * MIB,
            transcendentals=0),
    )(place, in_hbm(recv_hot), got_core, *got, on_chip(z), stats, norm_gain, norm_shift,
      in_hbm(dense), layer_weight)
    stats = from_peers(stats, PLANE)
    stats = from_peers(total_call(stats), COLUMN)

    return pl.pallas_call(
        functools.partial(last_kernel, vertex_total),
        out_shape=mixed,
        in_specs=[VMEM] * 4,
        out_specs=VMEM,
        compiler_params=pltpu.CompilerParams(vmem_limit_bytes=16 * MIB),
    )(on_chip(z), stats, norm_gain, norm_shift)


def solution(mesh):
    finer = Mesh(mesh.devices.reshape(4, 4, 8, 2), PARTS)
    placed = (
        P(PARTS, None),
        P(PARTS, None, None),
        P(PARTS, None),
        P(PARTS),
        P(PARTS, None, None),
        P(PARTS, None),
        P(),
        P(),
        P(),
    )
    return jax.shard_map(
        shards, mesh=finer, in_specs=placed, out_specs=P(PARTS, None), check_vma=False
    )
```

```python
import functools

import jax
import jax.numpy as jnp
from jax import lax
from jax.experimental import pallas as pl
from jax.experimental.pallas import tpu as pltpu
from jax.sharding import Mesh
from jax.sharding import PartitionSpec as P


PARTS = ("parts_0", "parts_1", "parts_2", "parts_3")
PLANE = PARTS[:2]
COLUMN = PARTS[2:]
norm_eps = 1e-05
EDGE = 128
MIB = 1 << 20


def swap(value, first, stride, total):
    pairs = []
    for q in range(total - stride):
        if first(q):
            pairs += [(q, q + stride), (q + stride, q)]
    return lax.ppermute(value, PARTS, pairs)


def chip_swaps(to_c, to_d):
    total = lax.axis_size(PARTS)
    return (
        swap(to_c, lambda q: q % 4 < 2, 2, total),
        swap(to_d, lambda q: q % 4 >= 2, 2, total),
    )


def core_swap(value):
    return swap(value, lambda q: q % 2 == 0, 1, lax.axis_size(PARTS))


def fill_one_hot(index_ref, one_hot_ref, groups):
    columns = one_hot_ref.shape[1]
    lanes = lax.broadcasted_iota(jnp.int32, (EDGE, EDGE), 1)
    for group in groups:
        row = jnp.broadcast_to(index_ref[pl.ds(group, 1), :], (EDGE, EDGE))
        away = row.T - lanes
        for block in range(columns // EDGE):
            one_hot_ref[pl.ds(group * EDGE, EDGE), pl.ds(block * EDGE, EDGE)] = jnp.where(
                away == block * EDGE, 1.0, 0.0
            ).astype(jnp.bfloat16)


def pick_piece(one_hot_ref, rows_ref, piece_ref, first, at, count):
    piece_ref[pl.ds(at, count), :] = jnp.dot(
        one_hot_ref[pl.ds(first, count), :], rows_ref[...], preferred_element_type=jnp.float32
    ).astype(jnp.bfloat16)


def pick_payloads(one_hot_ref, rows_ref, to_c, to_d):
    size = to_c.shape[0]
    pick_piece(one_hot_ref, rows_ref, to_c, 0, 0, size)
    pick_piece(one_hot_ref, rows_ref, to_d, size, 0, size)


def spread(row):
    n = row.shape[1]
    return jnp.broadcast_to(row, (n, n)).T


def put_tile_order(blocks_ref, live_count, row_count, column_count, order_ref):
    tiles = blocks_ref.shape[1]
    number = lax.broadcasted_iota(jnp.int32, (1, tiles), 1)
    live = number < live_count
    row = jnp.where(live, blocks_ref[0:1, :], 0)
    column = jnp.where(live, blocks_ref[1:2, :], column_count)
    cell = column * row_count + row
    key = cell * tiles + number
    down = lax.broadcasted_iota(jnp.int32, (tiles, tiles), 0)
    cells_down = spread(cell)
    keys_down = cells_down * tiles + down
    rank = jnp.sum((keys_down < key).astype(jnp.int32), axis=0, keepdims=True)
    same = (cells_down == cell) & (down < number)
    keep = jnp.sum(same.astype(jnp.int32), axis=0, keepdims=True) > 0
    packed = (cell * 2 + keep.astype(jnp.int32)) * tiles + number
    hit = spread(rank) == number
    packed = jnp.sum(jnp.where(hit, spread(packed), 0), axis=0, keepdims=True)
    cell = packed // (2 * tiles)
    order_ref[0:1, :] = packed % tiles
    order_ref[1:2, :] = cell % row_count
    order_ref[2:3, :] = cell // row_count
    order_ref[3:4, :] = (packed // tiles) % 2


def put_zeros(dense_ref, first, last):
    size = 256
    zeros = jnp.zeros((size, dense_ref.shape[2]), dense_ref.dtype)

    @pl.loop(first, last)
    def _(c):
        for at in range(0, dense_ref.shape[1], size):
            dense_ref[c, pl.ds(at, size), :] = zeros


def gather_kernel(row_count, column_count, zeroed, loaded,
                  device_ref, live_ref, send_in, blocks_in, features_ref, tiles_in,
                  to_c, to_d, near_ref, one_hot_ref, order_ref, rows_ref, dense_ref, tiles_ref,
                  send_ref, blocks_ref, index_ref, arrived):
    load_send = pltpu.make_async_copy(send_in, send_ref, arrived.at[0])
    load_blocks = pltpu.make_async_copy(blocks_in, blocks_ref, arrived.at[1])
    load = pltpu.make_async_copy(features_ref, rows_ref, arrived.at[2])
    part = pl.ds(0, loaded)
    load_tiles = pltpu.make_async_copy(tiles_in.at[part], tiles_ref.at[part], arrived.at[3])
    load_send.start()
    load_blocks.start()
    load.start()
    load_tiles.start()
    put_zeros(dense_ref, 0, zeroed)
    load_send.wait()
    even_chip = device_ref[0] % 4 < 2
    count = send_ref.shape[1]
    per_piece = count // EDGE
    for part in range(per_piece):
        n0, n1, n2, n3 = (send_ref[n:n + 1, part * EDGE:(part + 1) * EDGE] for n in range(4))
        lists = (
            jnp.where(even_chip, n2, n3),
            jnp.where(even_chip, n0, n1),
            jnp.where(even_chip, n3, n2),
            jnp.where(even_chip, n1, n0),
        )
        for n, chosen in enumerate(lists):
            at = n * per_piece + part
            index_ref[at:at + 1, :] = chosen
    fill_one_hot(index_ref, one_hot_ref, range(2 * per_piece))
    load_blocks.wait()
    put_tile_order(blocks_ref, live_ref[0], row_count, column_count, order_ref)
    load.wait()
    pick_piece(one_hot_ref, rows_ref, to_c, 0, 0, count)
    fill_one_hot(index_ref, one_hot_ref, range(2 * per_piece, 3 * per_piece))
    pick_piece(one_hot_ref, rows_ref, to_c, count, count, count)
    fill_one_hot(index_ref, one_hot_ref, range(3 * per_piece, 4 * per_piece))
    pick_piece(one_hot_ref, rows_ref, to_d, 2 * count, 0, count)
    pick_piece(one_hot_ref, rows_ref, to_d, 3 * count, count, count)
    put_near(device_ref, to_c, to_d, near_ref, 0)
    load_tiles.wait()


def put_near(device_ref, from_c, from_d, out_ref, at):
    count = from_c.shape[0] // 2
    first = (device_ref[0] % 4 < 2) == (device_ref[0] % 2 == 0)

    @pl.when(first)
    def _():
        out_ref[at:at + count, :] = from_c[count:2 * count, :]

    @pl.when(jnp.logical_not(first))
    def _():
        out_ref[at:at + count, :] = from_d[count:2 * count, :]


def relay_kernel(after_ref, device_ref, near_ref, got_c, got_d, out_ref):
    del after_ref
    count = near_ref.shape[0]
    out_ref[0:count, :] = near_ref[...]
    put_near(device_ref, got_c, got_d, out_ref, count)


def put_total(parts_ref, out_ref):
    both = jnp.sum(parts_ref[...], axis=0)
    for n in range(out_ref.shape[0]):
        out_ref[n] = both


def adjacency_block(dense_ref, first, last, start, size):
    return jnp.concatenate(
        [dense_ref[c, pl.ds(start, size), :] for c in range(first, last)], axis=1
    )


def build_kernel(count, zeroed, loaded,
                 device_ref, order_ref, live_ref, recv_in, tiles_in, _dense, _tiles,
                 dense_ref, held_ref, recv_hot_ref, index_ref, recv_ref, arrived):
    part = pl.ds(loaded, held_ref.shape[0] - loaded)
    load_recv = pltpu.make_async_copy(recv_in, recv_ref, arrived.at[0])
    load = pltpu.make_async_copy(tiles_in.at[part], held_ref.at[part], arrived.at[1])
    load_recv.start()
    load.start()
    unroll = 8
    put_zeros(dense_ref, zeroed, dense_ref.shape[0])

    near = jnp.where(device_ref[0] % 2 == 0, count, 0)
    far = jnp.where(device_ref[0] % 4 < 2, count, 0)
    load_recv.wait()
    for group in range(index_ref.shape[0]):
        rows = recv_ref[0:1, group * EDGE:(group + 1) * EDGE]
        index_ref[group:group + 1, :] = rows ^ jnp.where(rows < 2 * count, near, far)
    fill_one_hot(index_ref, recv_hot_ref, range(index_ref.shape[0]))
    load.wait()

    def step(turn, total):
        for u in range(unroll):
            k = turn * unroll + u
            tile = held_ref[order_ref[0, k]].astype(jnp.float32)
            total = total * order_ref[3, k].astype(jnp.float32) + tile
            start = pl.multiple_of(order_ref[1, k] * EDGE, EDGE)
            dense_ref[order_ref[2, k], pl.ds(start, EDGE), :] = total.astype(jnp.bfloat16)
        return total

    lax.fori_loop(
        0, (live_ref[0] + unroll - 1) // unroll, step, jnp.zeros((EDGE, EDGE), jnp.float32)
    )


def own_kernel(after_ref, dense_ref, rows_ref, own_ref):
    del after_ref
    height = own_ref.shape[0]
    own_blocks = height // EDGE
    size = 512

    @pl.loop(0, height // size)
    def _(m):
        start = pl.multiple_of(m * size, size)
        own_ref[pl.ds(start, size), :] = jnp.dot(
            adjacency_block(dense_ref, 0, own_blocks, start, size),
            rows_ref[...],
            preferred_element_type=jnp.float32,
        )


def add_moments(z, moment_ref):
    wide = z.astype(jnp.float32)
    moment_ref[0:8, :] += jnp.sum(wide.reshape(-1, 8, wide.shape[1]), axis=0)
    moment_ref[8:16, :] += jnp.sum(jnp.square(wide).reshape(-1, 8, wide.shape[1]), axis=0)


def put_moments(moment_ref, out_ref):
    both = jnp.concatenate(
        [
            jnp.sum(moment_ref[0:8, :], axis=0, keepdims=True),
            jnp.sum(moment_ref[8:16, :], axis=0, keepdims=True),
        ],
        axis=0,
    )
    for n in range(out_ref.shape[0]):
        out_ref[n] = both


def received(a, c, d):
    count = a.shape[0] // 2
    return a[0:count, :], a[count:2 * count, :], c[0:count, :], d[0:count, :]


def first_kernel(device_ref, recv_hot_ref, a, c, d, dense_ref, own_ref, weight_ref, send_hot_ref,
                 z_ref, stats_ref, to_c, to_d, near_ref, dense_out,
                 halo_ref, got_ref, moment_ref, left):
    layer = 0
    store = pltpu.make_async_copy(dense_ref, dense_out, left)
    store.start()
    count = a.shape[0] // 2
    for n, piece in enumerate(received(a, c, d)):
        got_ref[pl.ds(n * count, count), :] = piece
    halo_ref[...] = jnp.dot(
        recv_hot_ref[...], got_ref[...], preferred_element_type=jnp.float32
    ).astype(jnp.bfloat16)
    moment_ref[...] = jnp.zeros_like(moment_ref)
    height = z_ref.shape[0]
    own_blocks, halo_blocks = height // EDGE, halo_ref.shape[0] // EDGE
    size = 512

    @pl.loop(0, height // size)
    def _(m):
        start = pl.multiple_of(m * size, size)
        agg = own_ref[pl.ds(start, size), :] + jnp.dot(
            adjacency_block(dense_ref, own_blocks, own_blocks + halo_blocks, start, size),
            halo_ref[...],
            preferred_element_type=jnp.float32,
        )
        z = jnp.dot(
            agg.astype(jnp.bfloat16), weight_ref[layer], preferred_element_type=jnp.float32
        ).astype(jnp.bfloat16)
        z_ref[pl.ds(start, size), :] = z
        add_moments(z, moment_ref)

    put_moments(moment_ref, stats_ref)
    pick_payloads(send_hot_ref, z_ref, to_c, to_d)
    put_near(device_ref, to_c, to_d, near_ref, 0)
    store.wait()


def scale_of(stats_ref, gain_ref, shift_ref, layer, vertex_total):
    both = jnp.sum(stats_ref[...], axis=0) / vertex_total
    centre = both[0:1, :]
    spread = both[1:2, :] - jnp.square(centre)
    factor = gain_ref[layer:layer + 1, :] / jnp.sqrt(spread + norm_eps)
    return centre, factor, shift_ref[layer:layer + 1, :]


def normal(rows, terms):
    centre, factor, shift = terms
    return jnp.maximum((rows.astype(jnp.float32) - centre) * factor + shift, 0.0)


def second_kernel(device_total, device_ref, index_ref, a, c, d, mixed_ref, stats_in_ref,
                  gain_ref, shift_ref, dense_in, weight_ref, z_ref, stats_ref,
                  got_ref, columns_ref, moment_ref, recv_hot_ref, dense_ref, arrived):
    layer = 1
    count = a.shape[0] // 2
    height = z_ref.shape[0]
    halo = 4 * count
    blocks = (height + halo) // EDGE
    size = dense_ref.shape[2]

    def load_dense(m):
        return pltpu.make_async_copy(
            dense_in.at[pl.ds(0, blocks), pl.ds(pl.multiple_of(m * size, size), size), :],
            dense_ref.at[m],
            arrived.at[m],
        )

    for m in range(height // size):
        load_dense(m).start()
    terms = scale_of(stats_in_ref, gain_ref, shift_ref, 0, device_total * height)
    device = device_ref[0]
    near_side = (device > 0) & (device < device_total - 1)
    far_side = (device > 1) & (device < device_total - 2)
    present = (1.0, near_side.astype(jnp.float32), 1.0, far_side.astype(jnp.float32))
    for n, piece in enumerate(received(a, c, d)):
        got_ref[pl.ds(n * count, count), :] = (
            normal(piece, terms) * present[n]
        ).astype(jnp.bfloat16)
    for part in range(8):
        rows = pl.ds(part * (height // 8), height // 8)
        columns_ref[rows, :] = normal(mixed_ref[rows, :], terms).astype(jnp.bfloat16)
    fill_one_hot(index_ref, recv_hot_ref, range(index_ref.shape[0]))
    columns_ref[pl.ds(height, halo), :] = jnp.dot(
        recv_hot_ref[...], got_ref[...], preferred_element_type=jnp.float32
    ).astype(jnp.bfloat16)
    moment_ref[...] = jnp.zeros_like(moment_ref)

    @pl.loop(0, height // size)
    def _(m):
        load_dense(m).wait()
        start = pl.multiple_of(m * size, size)
        agg = jnp.dot(
            jnp.concatenate([dense_ref[m, c] for c in range(blocks)], axis=1),
            columns_ref[...],
            preferred_element_type=jnp.float32,
        )
        z = jnp.dot(
            agg.astype(jnp.bfloat16), weight_ref[layer], preferred_element_type=jnp.float32
        ).astype(jnp.bfloat16)
        z_ref[pl.ds(start, size), :] = z
        add_moments(z, moment_ref)

    put_moments(moment_ref, stats_ref)


def last_kernel(vertex_total, mixed_ref, stats_in_ref, gain_ref, shift_ref, out_ref):
    terms = scale_of(stats_in_ref, gain_ref, shift_ref, 1, vertex_total)
    out_ref[...] = normal(mixed_ref[...], terms).astype(jnp.bfloat16)


VMEM = pl.BlockSpec(memory_space=pltpu.VMEM)
SMEM = pl.BlockSpec(memory_space=pltpu.SMEM)
HBM = pl.BlockSpec(memory_space=pltpu.HBM)


def from_peers(stats, axes):
    return lax.all_to_all(stats, axes, 0, 0, tiled=True)


def shards(features, tile_values, tile_blocks, tile_count, send_rows, recv_index,
           layer_weight, norm_gain, norm_shift):
    height, channels = features.shape
    neighbours, count = send_rows.shape[1:]
    halo = neighbours * count
    row_count = height // EDGE
    column_count = (height + halo) // EDGE
    device = lax.axis_index(PARTS)
    total = lax.axis_size(PARTS)
    vertex_total = height * total
    peers = lax.axis_size(PLANE)
    bf16, f32 = jnp.bfloat16, jnp.float32
    struct = jax.ShapeDtypeStruct
    piece = struct((count, channels), bf16)
    payload = struct((2 * count, channels), bf16)
    stats_type = struct((peers, 2, channels), f32)
    mixed = struct((height, channels), bf16)

    place = device.reshape(1)

    def on_chip(value):
        return pltpu.with_memory_space_constraint(value, pltpu.VMEM)

    def in_hbm(value):
        return pltpu.with_memory_space_constraint(value, pltpu.HBM)

    zeroed, loaded = column_count // 2, tile_values.shape[0] * 5 // 8
    dense_type = pltpu.VMEM((column_count + 1, height, EDGE), bf16)
    tiles_type = pltpu.VMEM(tile_values.shape, bf16)
    *sent, near, send_hot, order, rows, dense, tiles = pl.pallas_call(
        functools.partial(gather_kernel, row_count, column_count, zeroed, loaded),
        out_shape=[payload] * 2 + [
            piece,
            pltpu.VMEM((halo, height), bf16),
            struct((4, tile_blocks.shape[0]), jnp.int32),
            pltpu.VMEM((height, channels), bf16),
            dense_type,
            tiles_type,
        ],
        in_specs=[SMEM, SMEM, HBM, HBM, HBM, HBM],
        out_specs=[VMEM] * 8,
        scratch_shapes=[
            pltpu.VMEM((neighbours, count), jnp.int32),
            pltpu.VMEM((2, tile_blocks.shape[0]), jnp.int32),
            pltpu.VMEM((halo // EDGE, EDGE), jnp.int32),
            pltpu.SemaphoreType.DMA((4,)),
        ],
        compiler_params=pltpu.CompilerParams(vmem_limit_bytes=16 * MIB),
        cost_estimate=pl.CostEstimate(
            flops=2 * halo * height * channels, bytes_accessed=2 * MIB, transcendentals=0),
    )(place, tile_count, in_hbm(send_rows[0]), in_hbm(tile_blocks.T), in_hbm(features),
      in_hbm(tile_values))
    got = chip_swaps(*sent)

    dense, _, recv_hot, built = pl.pallas_call(
        functools.partial(build_kernel, count, zeroed, loaded),
        out_shape=[
            dense_type,
            tiles_type,
            pltpu.VMEM((halo, halo), bf16),
            struct((halo // EDGE, EDGE), jnp.int32),
        ],
        in_specs=[SMEM, SMEM, SMEM, HBM, HBM, VMEM, VMEM],
        out_specs=[VMEM] * 4,
        input_output_aliases={5: 0, 6: 1},
        scratch_shapes=[
            pltpu.VMEM(recv_index.shape, jnp.int32),
            pltpu.SemaphoreType.DMA((2,)),
        ],
        compiler_params=pltpu.CompilerParams(vmem_limit_bytes=8 * MIB),
        cost_estimate=pl.CostEstimate(
            flops=4 * height * height * channels, bytes_accessed=24 * MIB, transcendentals=0),
    )(place, order, tile_count, in_hbm(recv_index), in_hbm(tile_values), on_chip(dense),
      on_chip(tiles))

    relay_call = pl.pallas_call(
        relay_kernel,
        out_shape=payload,
        in_specs=[VMEM, SMEM] + [VMEM] * 3,
        out_specs=VMEM,
        compiler_params=pltpu.CompilerParams(vmem_limit_bytes=4 * MIB),
    )
    relay = relay_call(built, place, near, *got)
    got_core = core_swap(relay)

    own = pl.pallas_call(
        own_kernel,
        out_shape=pltpu.VMEM((height, channels), f32),
        in_specs=[VMEM] * 3,
        out_specs=VMEM,
        compiler_params=pltpu.CompilerParams(vmem_limit_bytes=8 * MIB),
        cost_estimate=pl.CostEstimate(
            flops=2 * height * height * channels, bytes_accessed=8 * MIB, transcendentals=0),
    )(relay, on_chip(dense), on_chip(rows))

    z, stats, *sent, near, dense_out = pl.pallas_call(
        first_kernel,
        out_shape=[pltpu.VMEM(mixed.shape, bf16), pltpu.VMEM(stats_type.shape, f32)]
        + [payload] * 2 + [piece, pltpu.HBM(dense_type.shape, bf16)],
        in_specs=[SMEM] + [VMEM] * 8,
        out_specs=[VMEM] * 5 + [HBM],
        scratch_shapes=[
            pltpu.VMEM((halo, channels), bf16),
            pltpu.VMEM((halo, channels), bf16),
            pltpu.VMEM((16, channels), f32),
            pltpu.SemaphoreType.DMA,
        ],
        compiler_params=pltpu.CompilerParams(vmem_limit_bytes=12 * MIB),
        cost_estimate=pl.CostEstimate(
            flops=2 * height * halo * channels, bytes_accessed=16 * MIB, transcendentals=0),
    )(place, on_chip(recv_hot), got_core, *got, on_chip(dense), on_chip(own), layer_weight, on_chip(send_hot))
    got = chip_swaps(*sent)
    stats = from_peers(stats, PLANE)
    column_stats = struct((lax.axis_size(COLUMN), 2, channels), f32)
    total_call = pl.pallas_call(
        put_total,
        out_shape=pltpu.VMEM(column_stats.shape, f32),
        in_specs=[VMEM],
        out_specs=VMEM,
        compiler_params=pltpu.CompilerParams(vmem_limit_bytes=MIB),
    )
    stats = from_peers(total_call(stats), COLUMN)
    relay = relay_call(built, place, near, *got)
    got_core = core_swap(relay)

    chunk = 512
    z, stats = pl.pallas_call(
        functools.partial(second_kernel, total),
        out_shape=[pltpu.VMEM(mixed.shape, bf16), stats_type],
        in_specs=[SMEM] + [VMEM] * 8 + [HBM, VMEM],
        out_specs=[VMEM] * 2,
        scratch_shapes=[
            pltpu.VMEM((halo, channels), bf16),
            pltpu.VMEM((height + halo, channels), bf16),
            pltpu.VMEM((16, channels), f32),
            pltpu.VMEM((halo, halo), bf16),
            pltpu.VMEM((height // chunk, column_count, chunk, EDGE), bf16),
            pltpu.SemaphoreType.DMA((height // chunk,)),
        ],
        compiler_params=pltpu.CompilerParams(vmem_limit_bytes=28 * MIB),
        cost_estimate=pl.CostEstimate(
            flops=2 * height * (height + halo) * channels, bytes_accessed=16 * MIB,
            transcendentals=0),
    )(place, built, got_core, *got, on_chip(z), stats, norm_gain, norm_shift,
      in_hbm(dense_out), layer_weight)
    stats = from_peers(stats, PLANE)
    stats = from_peers(total_call(stats), COLUMN)

    return pl.pallas_call(
        functools.partial(last_kernel, vertex_total),
        out_shape=mixed,
        in_specs=[VMEM] * 4,
        out_specs=VMEM,
        compiler_params=pltpu.CompilerParams(vmem_limit_bytes=16 * MIB),
    )(on_chip(z), stats, norm_gain, norm_shift)


def solution(mesh):
    finer = Mesh(mesh.devices.reshape(4, 4, 8, 2), PARTS)
    placed = (
        P(PARTS, None),
        P(PARTS, None, None),
        P(PARTS, None),
        P(PARTS),
        P(PARTS, None, None),
        P(PARTS, None),
        P(),
        P(),
        P(),
    )
    return jax.shard_map(
        shards, mesh=finer, in_specs=placed, out_specs=P(PARTS, None), check_vma=False
    )
```

```python
import functools

import jax
import jax.numpy as jnp
from jax import lax
from jax.experimental import pallas as pl
from jax.experimental.pallas import tpu as pltpu
from jax.sharding import Mesh
from jax.sharding import PartitionSpec as P


PARTS = ("parts_0", "parts_1", "parts_2", "parts_3")
PLANE = PARTS[:2]
COLUMN = PARTS[2:]
norm_eps = 1e-05
EDGE = 128
MIB = 1 << 20


def swap(value, first, stride, total):
    pairs = []
    for q in range(total - stride):
        if first(q):
            pairs += [(q, q + stride), (q + stride, q)]
    return lax.ppermute(value, PARTS, pairs)


def chip_swaps(to_c, to_d):
    total = lax.axis_size(PARTS)
    got_d = swap(to_d, lambda q: q % 4 >= 2, 2, total)
    got_c = swap(to_c, lambda q: q % 4 < 2, 2, total)
    return got_c, got_d


def core_swap(value):
    return swap(value, lambda q: q % 2 == 0, 1, lax.axis_size(PARTS))


def fill_one_hot(index_ref, one_hot_ref, groups):
    columns = one_hot_ref.shape[1]
    lanes = lax.broadcasted_iota(jnp.int32, (EDGE, EDGE), 1)
    for group in groups:
        row = jnp.broadcast_to(index_ref[pl.ds(group, 1), :], (EDGE, EDGE))
        away = row.T - lanes
        for block in range(columns // EDGE):
            one_hot_ref[pl.ds(group * EDGE, EDGE), pl.ds(block * EDGE, EDGE)] = jnp.where(
                away == block * EDGE, 1.0, 0.0
            ).astype(jnp.bfloat16)


def pick_piece(one_hot_ref, rows_ref, piece_ref, first, at, count):
    piece_ref[pl.ds(at, count), :] = jnp.dot(
        one_hot_ref[pl.ds(first, count), :], rows_ref[...], preferred_element_type=jnp.float32
    ).astype(jnp.bfloat16)


def pick_payloads(one_hot_ref, rows_ref, to_c, to_d):
    size = to_c.shape[0]
    pick_piece(one_hot_ref, rows_ref, to_c, 0, 0, size)
    pick_piece(one_hot_ref, rows_ref, to_d, size, 0, size)


def spread(row):
    n = row.shape[1]
    return jnp.broadcast_to(row, (n, n)).T


def put_tile_order(blocks_ref, live_count, row_count, column_count, order_ref):
    tiles = blocks_ref.shape[1]
    number = lax.broadcasted_iota(jnp.int32, (1, tiles), 1)
    live = number < live_count
    row = jnp.where(live, blocks_ref[0:1, :], 0)
    column = jnp.where(live, blocks_ref[1:2, :], column_count)
    cell = column * row_count + row
    key = cell * tiles + number
    down = lax.broadcasted_iota(jnp.int32, (tiles, tiles), 0)
    cells_down = spread(cell)
    keys_down = cells_down * tiles + down
    rank = jnp.sum((keys_down < key).astype(jnp.int32), axis=0, keepdims=True)
    same = (cells_down == cell) & (down < number)
    keep = jnp.sum(same.astype(jnp.int32), axis=0, keepdims=True) > 0
    packed = (cell * 2 + keep.astype(jnp.int32)) * tiles + number
    hit = spread(rank) == number
    packed = jnp.sum(jnp.where(hit, spread(packed), 0), axis=0, keepdims=True)
    cell = packed // (2 * tiles)
    order_ref[0:1, :] = packed % tiles
    order_ref[1:2, :] = cell % row_count
    order_ref[2:3, :] = cell // row_count
    order_ref[3:4, :] = (packed // tiles) % 2


def put_zeros(dense_ref, first, last):
    size = 256
    zeros = jnp.zeros((size, dense_ref.shape[2]), dense_ref.dtype)

    @pl.loop(first, last)
    def _(c):
        for at in range(0, dense_ref.shape[1], size):
            dense_ref[c, pl.ds(at, size), :] = zeros


def gather_kernel(row_count, column_count, zeroed, loaded,
                  device_ref, live_ref, send_in, blocks_in, features_ref, tiles_in,
                  to_c, to_d, near_ref, one_hot_ref, order_ref, rows_ref, dense_ref, tiles_ref,
                  send_ref, blocks_ref, index_ref, arrived):
    load_send = pltpu.make_async_copy(send_in, send_ref, arrived.at[0])
    load_blocks = pltpu.make_async_copy(blocks_in, blocks_ref, arrived.at[1])
    load = pltpu.make_async_copy(features_ref, rows_ref, arrived.at[2])
    part = pl.ds(0, loaded)
    load_tiles = pltpu.make_async_copy(tiles_in.at[part], tiles_ref.at[part], arrived.at[3])
    load_send.start()
    load_blocks.start()
    load.start()
    load_tiles.start()
    put_zeros(dense_ref, 0, zeroed)
    load_send.wait()
    even_chip = device_ref[0] % 4 < 2
    count = send_ref.shape[1]
    per_piece = count // EDGE
    for part in range(per_piece):
        n0, n1, n2, n3 = (send_ref[n:n + 1, part * EDGE:(part + 1) * EDGE] for n in range(4))
        lists = (
            jnp.where(even_chip, n2, n3),
            jnp.where(even_chip, n0, n1),
            jnp.where(even_chip, n3, n2),
            jnp.where(even_chip, n1, n0),
        )
        for n, chosen in enumerate(lists):
            at = n * per_piece + part
            index_ref[at:at + 1, :] = chosen
    fill_one_hot(index_ref, one_hot_ref, range(2 * per_piece))
    load_blocks.wait()
    put_tile_order(blocks_ref, live_ref[0], row_count, column_count, order_ref)
    load.wait()
    pick_piece(one_hot_ref, rows_ref, to_c, 0, 0, count)
    fill_one_hot(index_ref, one_hot_ref, range(2 * per_piece, 3 * per_piece))
    pick_piece(one_hot_ref, rows_ref, to_c, count, count, count)
    fill_one_hot(index_ref, one_hot_ref, range(3 * per_piece, 4 * per_piece))
    pick_piece(one_hot_ref, rows_ref, to_d, 2 * count, 0, count)
    pick_piece(one_hot_ref, rows_ref, to_d, 3 * count, count, count)
    put_near(device_ref, to_c, to_d, near_ref, 0)
    load_tiles.wait()


def put_near(device_ref, from_c, from_d, out_ref, at):
    count = from_c.shape[0] // 2
    first = (device_ref[0] % 4 < 2) == (device_ref[0] % 2 == 0)

    @pl.when(first)
    def _():
        out_ref[at:at + count, :] = from_c[count:2 * count, :]

    @pl.when(jnp.logical_not(first))
    def _():
        out_ref[at:at + count, :] = from_d[count:2 * count, :]


def relay_kernel(after_ref, device_ref, near_ref, got_c, got_d, out_ref):
    del after_ref
    count = near_ref.shape[0]
    out_ref[0:count, :] = near_ref[...]
    put_near(device_ref, got_c, got_d, out_ref, count)


def put_total(parts_ref, out_ref):
    both = jnp.sum(parts_ref[...], axis=0)
    for n in range(out_ref.shape[0]):
        out_ref[n] = both


def adjacency_block(dense_ref, first, last, start, size):
    return jnp.concatenate(
        [dense_ref[c, pl.ds(start, size), :] for c in range(first, last)], axis=1
    )


def build_kernel(count, zeroed, loaded,
                 device_ref, order_ref, live_ref, recv_in, tiles_in, _dense, _tiles,
                 dense_ref, held_ref, recv_hot_ref, index_ref, recv_ref, arrived):
    part = pl.ds(loaded, held_ref.shape[0] - loaded)
    load_recv = pltpu.make_async_copy(recv_in, recv_ref, arrived.at[0])
    load = pltpu.make_async_copy(tiles_in.at[part], held_ref.at[part], arrived.at[1])
    load_recv.start()
    load.start()
    unroll = 8
    put_zeros(dense_ref, zeroed, dense_ref.shape[0])

    near = jnp.where(device_ref[0] % 2 == 0, count, 0)
    far = jnp.where(device_ref[0] % 4 < 2, count, 0)
    load_recv.wait()
    for group in range(index_ref.shape[0]):
        rows = recv_ref[0:1, group * EDGE:(group + 1) * EDGE]
        index_ref[group:group + 1, :] = rows ^ jnp.where(rows < 2 * count, near, far)
    fill_one_hot(index_ref, recv_hot_ref, range(index_ref.shape[0]))
    load.wait()

    def step(turn, total):
        for u in range(unroll):
            k = turn * unroll + u
            tile = held_ref[order_ref[0, k]].astype(jnp.float32)
            total = total * order_ref[3, k].astype(jnp.float32) + tile
            start = pl.multiple_of(order_ref[1, k] * EDGE, EDGE)
            dense_ref[order_ref[2, k], pl.ds(start, EDGE), :] = total.astype(jnp.bfloat16)
        return total

    lax.fori_loop(
        0, (live_ref[0] + unroll - 1) // unroll, step, jnp.zeros((EDGE, EDGE), jnp.float32)
    )


def own_kernel(dense_ref, rows_ref, own_ref, dense_out, left):
    store = pltpu.make_async_copy(
        dense_ref.at[pl.ds(0, dense_out.shape[0])], dense_out, left
    )
    store.start()
    height = own_ref.shape[0]
    own_blocks = height // EDGE
    size = 512
    for start in range(0, height, size):
        own_ref[pl.ds(start, size), :] = jnp.dot(
            adjacency_block(dense_ref, 0, own_blocks, start, size),
            rows_ref[...],
            preferred_element_type=jnp.float32,
        )
    store.wait()


def add_moments(z, moment_ref):
    wide = z.astype(jnp.float32)
    moment_ref[0:8, :] += jnp.sum(wide.reshape(-1, 8, wide.shape[1]), axis=0)
    moment_ref[8:16, :] += jnp.sum(jnp.square(wide).reshape(-1, 8, wide.shape[1]), axis=0)


def put_moments(moment_ref, out_ref):
    both = jnp.concatenate(
        [
            jnp.sum(moment_ref[0:8, :], axis=0, keepdims=True),
            jnp.sum(moment_ref[8:16, :], axis=0, keepdims=True),
        ],
        axis=0,
    )
    for n in range(out_ref.shape[0]):
        out_ref[n] = both


def received(a, c, d):
    count = a.shape[0] // 2
    return a[0:count, :], a[count:2 * count, :], c[0:count, :], d[0:count, :]


def first_kernel(device_ref, recv_hot_ref, a, c, d, dense_ref, own_ref, weight_ref, send_hot_ref,
                 z_ref, stats_ref, to_c, to_d, near_ref, dense_out,
                 halo_ref, got_ref, moment_ref, left):
    layer = 0
    count = a.shape[0] // 2
    written = own_ref.shape[0] // EDGE + 4 * count // EDGE - dense_out.shape[0]
    store = pltpu.make_async_copy(
        dense_ref.at[pl.ds(written, dense_out.shape[0])], dense_out, left
    )
    store.start()
    for n, piece in enumerate(received(a, c, d)):
        got_ref[pl.ds(n * count, count), :] = piece
    halo_ref[...] = jnp.dot(
        recv_hot_ref[...], got_ref[...], preferred_element_type=jnp.float32
    ).astype(jnp.bfloat16)
    moment_ref[...] = jnp.zeros_like(moment_ref)
    height = z_ref.shape[0]
    own_blocks, halo_blocks = height // EDGE, halo_ref.shape[0] // EDGE
    size = 512

    for start in range(0, height, size):
        agg = own_ref[pl.ds(start, size), :] + jnp.dot(
            adjacency_block(dense_ref, own_blocks, own_blocks + halo_blocks, start, size),
            halo_ref[...],
            preferred_element_type=jnp.float32,
        )
        z = jnp.dot(
            agg.astype(jnp.bfloat16), weight_ref[layer], preferred_element_type=jnp.float32
        ).astype(jnp.bfloat16)
        z_ref[pl.ds(start, size), :] = z
        add_moments(z, moment_ref)

    put_moments(moment_ref, stats_ref)
    pick_payloads(send_hot_ref, z_ref, to_c, to_d)
    put_near(device_ref, to_c, to_d, near_ref, 0)
    store.wait()


def scale_of(stats_ref, gain_ref, shift_ref, layer, vertex_total):
    both = jnp.sum(stats_ref[...], axis=0) / vertex_total
    centre = both[0:1, :]
    spread = both[1:2, :] - jnp.square(centre)
    factor = gain_ref[layer:layer + 1, :] / jnp.sqrt(spread + norm_eps)
    return centre, factor, shift_ref[layer:layer + 1, :]


def normal(rows, terms):
    centre, factor, shift = terms
    return jnp.maximum((rows.astype(jnp.float32) - centre) * factor + shift, 0.0)


def second_kernel(device_total, device_ref, index_ref, a, c, d, mixed_ref, stats_in_ref,
                  gain_ref, shift_ref, dense_a, dense_b, weight_ref, z_ref, stats_ref,
                  got_ref, columns_ref, moment_ref, recv_hot_ref, dense_ref, arrived):
    layer = 1
    count = a.shape[0] // 2
    height = z_ref.shape[0]
    halo = 4 * count
    blocks = (height + halo) // EDGE
    size = dense_ref.shape[2]

    loads = []
    for m in range(height // size):
        at = 0
        for n, part in enumerate((dense_a, dense_b)):
            load = pltpu.make_async_copy(
                part.at[:, pl.ds(m * size, size), :],
                dense_ref.at[m, pl.ds(at, part.shape[0])],
                arrived.at[m, n],
            )
            load.start()
            loads.append(load)
            at += part.shape[0]
    terms = scale_of(stats_in_ref, gain_ref, shift_ref, 0, device_total * height)
    device = device_ref[0]
    near_side = (device > 0) & (device < device_total - 1)
    far_side = (device > 1) & (device < device_total - 2)
    present = (1.0, near_side.astype(jnp.float32), 1.0, far_side.astype(jnp.float32))
    for n, piece in enumerate(received(a, c, d)):
        got_ref[pl.ds(n * count, count), :] = (
            normal(piece, terms) * present[n]
        ).astype(jnp.bfloat16)
    for part in range(8):
        rows = pl.ds(part * (height // 8), height // 8)
        columns_ref[rows, :] = normal(mixed_ref[rows, :], terms).astype(jnp.bfloat16)
    fill_one_hot(index_ref, recv_hot_ref, range(index_ref.shape[0]))
    columns_ref[pl.ds(height, halo), :] = jnp.dot(
        recv_hot_ref[...], got_ref[...], preferred_element_type=jnp.float32
    ).astype(jnp.bfloat16)
    moment_ref[...] = jnp.zeros_like(moment_ref)

    for m in range(height // size):
        loads[2 * m].wait()
        loads[2 * m + 1].wait()
        start = m * size
        agg = jnp.dot(
            jnp.concatenate([dense_ref[m, c] for c in range(blocks)], axis=1),
            columns_ref[...],
            preferred_element_type=jnp.float32,
        )
        z = jnp.dot(
            agg.astype(jnp.bfloat16), weight_ref[layer], preferred_element_type=jnp.float32
        ).astype(jnp.bfloat16)
        z_ref[pl.ds(start, size), :] = z
        add_moments(z, moment_ref)

    put_moments(moment_ref, stats_ref)


def last_kernel(vertex_total, mixed_ref, stats_in_ref, gain_ref, shift_ref, out_ref):
    terms = scale_of(stats_in_ref, gain_ref, shift_ref, 1, vertex_total)
    out_ref[...] = normal(mixed_ref[...], terms).astype(jnp.bfloat16)


VMEM = pl.BlockSpec(memory_space=pltpu.VMEM)
SMEM = pl.BlockSpec(memory_space=pltpu.SMEM)
HBM = pl.BlockSpec(memory_space=pltpu.HBM)


def from_peers(stats, axes):
    return lax.all_to_all(stats, axes, 0, 0, tiled=True)


def shards(features, tile_values, tile_blocks, tile_count, send_rows, recv_index,
           layer_weight, norm_gain, norm_shift):
    height, channels = features.shape
    neighbours, count = send_rows.shape[1:]
    halo = neighbours * count
    row_count = height // EDGE
    column_count = (height + halo) // EDGE
    device = lax.axis_index(PARTS)
    total = lax.axis_size(PARTS)
    vertex_total = height * total
    peers = lax.axis_size(PLANE)
    bf16, f32 = jnp.bfloat16, jnp.float32
    struct = jax.ShapeDtypeStruct
    piece = struct((count, channels), bf16)
    payload = struct((2 * count, channels), bf16)
    stats_type = struct((peers, 2, channels), f32)
    mixed = struct((height, channels), bf16)

    place = device.reshape(1)

    def on_chip(value):
        return pltpu.with_memory_space_constraint(value, pltpu.VMEM)

    def in_hbm(value):
        return pltpu.with_memory_space_constraint(value, pltpu.HBM)

    zeroed, loaded = column_count // 2, tile_values.shape[0] * 5 // 8
    dense_type = pltpu.VMEM((column_count + 1, height, EDGE), bf16)
    tiles_type = pltpu.VMEM(tile_values.shape, bf16)
    *sent, near, send_hot, order, rows, dense, tiles = pl.pallas_call(
        functools.partial(gather_kernel, row_count, column_count, zeroed, loaded),
        out_shape=[payload] * 2 + [
            piece,
            pltpu.VMEM((halo, height), bf16),
            struct((4, tile_blocks.shape[0]), jnp.int32),
            pltpu.VMEM((height, channels), bf16),
            dense_type,
            tiles_type,
        ],
        in_specs=[SMEM, SMEM, HBM, HBM, HBM, HBM],
        out_specs=[VMEM] * 8,
        scratch_shapes=[
            pltpu.VMEM((neighbours, count), jnp.int32),
            pltpu.VMEM((2, tile_blocks.shape[0]), jnp.int32),
            pltpu.VMEM((halo // EDGE, EDGE), jnp.int32),
            pltpu.SemaphoreType.DMA((4,)),
        ],
        compiler_params=pltpu.CompilerParams(vmem_limit_bytes=16 * MIB),
        cost_estimate=pl.CostEstimate(
            flops=2 * halo * height * channels, bytes_accessed=2 * MIB, transcendentals=0),
    )(place, tile_count, in_hbm(send_rows[0]), in_hbm(tile_blocks.T), in_hbm(features),
      in_hbm(tile_values))
    got = chip_swaps(*sent)

    dense, _, recv_hot, built = pl.pallas_call(
        functools.partial(build_kernel, count, zeroed, loaded),
        out_shape=[
            dense_type,
            tiles_type,
            pltpu.VMEM((halo, halo), bf16),
            struct((halo // EDGE, EDGE), jnp.int32),
        ],
        in_specs=[SMEM, SMEM, SMEM, HBM, HBM, VMEM, VMEM],
        out_specs=[VMEM] * 4,
        input_output_aliases={5: 0, 6: 1},
        scratch_shapes=[
            pltpu.VMEM(recv_index.shape, jnp.int32),
            pltpu.SemaphoreType.DMA((2,)),
        ],
        compiler_params=pltpu.CompilerParams(vmem_limit_bytes=8 * MIB),
        cost_estimate=pl.CostEstimate(
            flops=4 * height * height * channels, bytes_accessed=24 * MIB, transcendentals=0),
    )(place, order, tile_count, in_hbm(recv_index), in_hbm(tile_values), on_chip(dense),
      on_chip(tiles))

    early = column_count // 3
    own, dense_a = pl.pallas_call(
        own_kernel,
        out_shape=[
            pltpu.VMEM((height, channels), f32),
            pltpu.HBM((early, height, EDGE), bf16),
        ],
        in_specs=[VMEM] * 2,
        out_specs=[VMEM, HBM],
        scratch_shapes=[pltpu.SemaphoreType.DMA],
        compiler_params=pltpu.CompilerParams(vmem_limit_bytes=8 * MIB),
        cost_estimate=pl.CostEstimate(
            flops=2 * height * height * channels, bytes_accessed=8 * MIB, transcendentals=0),
    )(on_chip(dense), on_chip(rows))

    relay_call = pl.pallas_call(
        relay_kernel,
        out_shape=payload,
        in_specs=[VMEM, SMEM] + [VMEM] * 3,
        out_specs=VMEM,
        compiler_params=pltpu.CompilerParams(vmem_limit_bytes=4 * MIB),
    )
    relay = relay_call(own, place, near, *got)
    got_core = core_swap(relay)

    z, stats, *sent, near, dense_b = pl.pallas_call(
        first_kernel,
        out_shape=[pltpu.VMEM(mixed.shape, bf16), pltpu.VMEM(stats_type.shape, f32)]
        + [payload] * 2 + [piece, pltpu.HBM((column_count - early, height, EDGE), bf16)],
        in_specs=[SMEM] + [VMEM] * 8,
        out_specs=[VMEM] * 5 + [HBM],
        scratch_shapes=[
            pltpu.VMEM((halo, channels), bf16),
            pltpu.VMEM((halo, channels), bf16),
            pltpu.VMEM((16, channels), f32),
            pltpu.SemaphoreType.DMA,
        ],
        compiler_params=pltpu.CompilerParams(vmem_limit_bytes=12 * MIB),
        cost_estimate=pl.CostEstimate(
            flops=2 * height * halo * channels, bytes_accessed=16 * MIB, transcendentals=0),
    )(place, on_chip(recv_hot), got_core, *got, on_chip(dense), on_chip(own), layer_weight, on_chip(send_hot))
    got = chip_swaps(*sent)
    stats = from_peers(stats, PLANE)
    column_stats = struct((lax.axis_size(COLUMN), 2, channels), f32)
    total_call = pl.pallas_call(
        put_total,
        out_shape=pltpu.VMEM(column_stats.shape, f32),
        in_specs=[VMEM],
        out_specs=VMEM,
        compiler_params=pltpu.CompilerParams(vmem_limit_bytes=MIB),
    )
    stats = from_peers(total_call(stats), COLUMN)
    relay = relay_call(built, place, near, *got)
    got_core = core_swap(relay)

    chunk = 512
    z, stats = pl.pallas_call(
        functools.partial(second_kernel, total),
        out_shape=[pltpu.VMEM(mixed.shape, bf16), stats_type],
        in_specs=[SMEM] + [VMEM] * 8 + [HBM, HBM, VMEM],
        out_specs=[VMEM] * 2,
        scratch_shapes=[
            pltpu.VMEM((halo, channels), bf16),
            pltpu.VMEM((height + halo, channels), bf16),
            pltpu.VMEM((16, channels), f32),
            pltpu.VMEM((halo, halo), bf16),
            pltpu.VMEM((height // chunk, column_count, chunk, EDGE), bf16),
            pltpu.SemaphoreType.DMA((height // chunk, 2)),
        ],
        compiler_params=pltpu.CompilerParams(vmem_limit_bytes=28 * MIB),
        cost_estimate=pl.CostEstimate(
            flops=2 * height * (height + halo) * channels, bytes_accessed=16 * MIB,
            transcendentals=0),
    )(place, built, got_core, *got, on_chip(z), stats, norm_gain, norm_shift,
      in_hbm(dense_a), in_hbm(dense_b), layer_weight)
    stats = from_peers(stats, PLANE)
    stats = from_peers(total_call(stats), COLUMN)

    return pl.pallas_call(
        functools.partial(last_kernel, vertex_total),
        out_shape=mixed,
        in_specs=[VMEM] * 4,
        out_specs=VMEM,
        compiler_params=pltpu.CompilerParams(vmem_limit_bytes=16 * MIB),
    )(on_chip(z), stats, norm_gain, norm_shift)


def solution(mesh):
    finer = Mesh(mesh.devices.reshape(4, 4, 8, 2), PARTS)
    placed = (
        P(PARTS, None),
        P(PARTS, None, None),
        P(PARTS, None),
        P(PARTS),
        P(PARTS, None, None),
        P(PARTS, None),
        P(),
        P(),
        P(),
    )
    return jax.shard_map(
        shards, mesh=finer, in_specs=placed, out_specs=P(PARTS, None), check_vma=False
    )
```

```python
import functools

import jax
import jax.numpy as jnp
from jax import lax
from jax.experimental import pallas as pl
from jax.experimental.pallas import tpu as pltpu
from jax.sharding import Mesh
from jax.sharding import PartitionSpec as P


PARTS = ("parts_0", "parts_1", "parts_2", "parts_3")
PLANE = PARTS[:2]
COLUMN = PARTS[2:]
norm_eps = 1e-05
EDGE = 128
MIB = 1 << 20


def swap(value, first, stride, total):
    pairs = []
    for q in range(total - stride):
        if first(q):
            pairs += [(q, q + stride), (q + stride, q)]
    return lax.ppermute(value, PARTS, pairs)


def chip_swaps(to_c, to_d):
    total = lax.axis_size(PARTS)
    got_d = swap(to_d, lambda q: q % 4 >= 2, 2, total)
    got_c = swap(to_c, lambda q: q % 4 < 2, 2, total)
    return got_c, got_d


def core_swap(value):
    return swap(value, lambda q: q % 2 == 0, 1, lax.axis_size(PARTS))


def direct_swaps(a, b, c, d):
    total = lax.axis_size(PARTS)
    d = swap(d, lambda q: q % 4 >= 2, 2, total)
    b = swap(b, lambda q: q % 2 == 1, 1, total)
    c = swap(c, lambda q: q % 4 < 2, 2, total)
    a = swap(a, lambda q: q % 2 == 0, 1, total)
    return a, b, c, d


def fill_one_hot(index_ref, one_hot_ref, groups):
    columns = one_hot_ref.shape[1]
    lanes = lax.broadcasted_iota(jnp.int32, (EDGE, EDGE), 1)
    for group in groups:
        row = jnp.broadcast_to(index_ref[pl.ds(group, 1), :], (EDGE, EDGE))
        away = row.T - lanes
        for block in range(columns // EDGE):
            one_hot_ref[pl.ds(group * EDGE, EDGE), pl.ds(block * EDGE, EDGE)] = jnp.where(
                away == block * EDGE, 1.0, 0.0
            ).astype(jnp.bfloat16)


def pick_piece(one_hot_ref, rows_ref, piece_ref, first, at, count):
    piece_ref[pl.ds(at, count), :] = jnp.dot(
        one_hot_ref[pl.ds(first, count), :], rows_ref[...], preferred_element_type=jnp.float32
    ).astype(jnp.bfloat16)


def pick_payloads(one_hot_ref, rows_ref, to_c, to_d):
    size = to_c.shape[0]
    pick_piece(one_hot_ref, rows_ref, to_c, 0, 0, size)
    pick_piece(one_hot_ref, rows_ref, to_d, size, 0, size)


def spread(row):
    n = row.shape[1]
    return jnp.broadcast_to(row, (n, n)).T


def put_tile_order(blocks_ref, live_count, row_count, column_count, order_ref):
    tiles = blocks_ref.shape[1]
    number = lax.broadcasted_iota(jnp.int32, (1, tiles), 1)
    live = number < live_count
    row = jnp.where(live, blocks_ref[0:1, :], 0)
    column = jnp.where(live, blocks_ref[1:2, :], column_count)
    cell = column * row_count + row
    key = cell * tiles + number
    down = lax.broadcasted_iota(jnp.int32, (tiles, tiles), 0)
    cells_down = spread(cell)
    keys_down = cells_down * tiles + down
    rank = jnp.sum((keys_down < key).astype(jnp.int32), axis=0, keepdims=True)
    same = (cells_down == cell) & (down < number)
    keep = jnp.sum(same.astype(jnp.int32), axis=0, keepdims=True) > 0
    packed = (cell * 2 + keep.astype(jnp.int32)) * tiles + number
    hit = spread(rank) == number
    packed = jnp.sum(jnp.where(hit, spread(packed), 0), axis=0, keepdims=True)
    cell = packed // (2 * tiles)
    order_ref[0:1, :] = packed % tiles
    order_ref[1:2, :] = cell % row_count
    order_ref[2:3, :] = cell // row_count
    order_ref[3:4, :] = (packed // tiles) % 2


def put_zeros(dense_ref, first, last):
    size = 256
    zeros = jnp.zeros((size, dense_ref.shape[2]), dense_ref.dtype)

    @pl.loop(first, last)
    def _(c):
        for at in range(0, dense_ref.shape[1], size):
            dense_ref[c, pl.ds(at, size), :] = zeros


def gather_kernel(row_count, column_count, zeroed, loaded,
                  device_ref, live_ref, send_in, blocks_in, features_ref, tiles_in,
                  a, b, c, d, one_hot_ref, order_ref, rows_ref, dense_ref, tiles_ref,
                  send_ref, blocks_ref, index_ref, arrived):
    load_send = pltpu.make_async_copy(send_in, send_ref, arrived.at[0])
    load_blocks = pltpu.make_async_copy(blocks_in, blocks_ref, arrived.at[1])
    load = pltpu.make_async_copy(features_ref, rows_ref, arrived.at[2])
    part = pl.ds(0, loaded)
    load_tiles = pltpu.make_async_copy(tiles_in.at[part], tiles_ref.at[part], arrived.at[3])
    load_send.start()
    load_blocks.start()
    load.start()
    load_tiles.start()
    put_zeros(dense_ref, 0, zeroed)
    load_send.wait()
    even_chip = device_ref[0] % 4 < 2
    count = send_ref.shape[1]
    per_piece = count // EDGE
    for part in range(per_piece):
        n0, n1, n2, n3 = (send_ref[n:n + 1, part * EDGE:(part + 1) * EDGE] for n in range(4))
        lists = (
            jnp.where(even_chip, n2, n3),
            jnp.where(even_chip, n0, n1),
            jnp.where(even_chip, n3, n2),
            jnp.where(even_chip, n1, n0),
        )
        for n, chosen in enumerate(lists):
            at = n * per_piece + part
            index_ref[at:at + 1, :] = chosen
    fill_one_hot(index_ref, one_hot_ref, range(2 * per_piece))
    load_blocks.wait()
    put_tile_order(blocks_ref, live_ref[0], row_count, column_count, order_ref)
    load.wait()
    first = even_chip == (device_ref[0] % 2 == 0)
    near_core = pl.multiple_of(jnp.where(first, count, 3 * count), EDGE)
    near_chip = pl.multiple_of(jnp.where(first, 3 * count, count), EDGE)
    pick_piece(one_hot_ref, rows_ref, c, 0, 0, count)
    fill_one_hot(index_ref, one_hot_ref, range(2 * per_piece, 3 * per_piece))
    pick_piece(one_hot_ref, rows_ref, d, 2 * count, 0, count)
    fill_one_hot(index_ref, one_hot_ref, range(3 * per_piece, 4 * per_piece))
    pick_piece(one_hot_ref, rows_ref, b, near_chip, 0, count)
    pick_piece(one_hot_ref, rows_ref, a, near_core, 0, count)
    load_tiles.wait()


def put_near(device_ref, from_c, from_d, out_ref, at):
    count = from_c.shape[0] // 2
    first = (device_ref[0] % 4 < 2) == (device_ref[0] % 2 == 0)

    @pl.when(first)
    def _():
        out_ref[at:at + count, :] = from_c[count:2 * count, :]

    @pl.when(jnp.logical_not(first))
    def _():
        out_ref[at:at + count, :] = from_d[count:2 * count, :]


def relay_kernel(after_ref, device_ref, near_ref, got_c, got_d, out_ref):
    del after_ref
    count = near_ref.shape[0]
    out_ref[0:count, :] = near_ref[...]
    put_near(device_ref, got_c, got_d, out_ref, count)


def put_total(parts_ref, out_ref):
    both = jnp.sum(parts_ref[...], axis=0)
    for n in range(out_ref.shape[0]):
        out_ref[n] = both


def adjacency_block(dense_ref, first, last, start, size):
    return jnp.concatenate(
        [dense_ref[c, pl.ds(start, size), :] for c in range(first, last)], axis=1
    )


def build_kernel(count, zeroed, loaded,
                 device_ref, order_ref, live_ref, recv_in, tiles_in, _dense, _tiles,
                 dense_ref, held_ref, recv_hot_ref, index_ref, recv_ref, arrived):
    part = pl.ds(loaded, held_ref.shape[0] - loaded)
    load_recv = pltpu.make_async_copy(recv_in, recv_ref, arrived.at[0])
    load = pltpu.make_async_copy(tiles_in.at[part], held_ref.at[part], arrived.at[1])
    load_recv.start()
    load.start()
    unroll = 8
    put_zeros(dense_ref, zeroed, dense_ref.shape[0])

    near = jnp.where(device_ref[0] % 2 == 0, count, 0)
    far = jnp.where(device_ref[0] % 4 < 2, count, 0)
    load_recv.wait()
    for group in range(index_ref.shape[0]):
        rows = recv_ref[0:1, group * EDGE:(group + 1) * EDGE]
        index_ref[group:group + 1, :] = rows ^ jnp.where(rows < 2 * count, near, far)
    fill_one_hot(index_ref, recv_hot_ref, range(index_ref.shape[0]))
    load.wait()

    def step(turn, total):
        for u in range(unroll):
            k = turn * unroll + u
            tile = held_ref[order_ref[0, k]].astype(jnp.float32)
            total = total * order_ref[3, k].astype(jnp.float32) + tile
            start = pl.multiple_of(order_ref[1, k] * EDGE, EDGE)
            dense_ref[order_ref[2, k], pl.ds(start, EDGE), :] = total.astype(jnp.bfloat16)
        return total

    lax.fori_loop(
        0, (live_ref[0] + unroll - 1) // unroll, step, jnp.zeros((EDGE, EDGE), jnp.float32)
    )


def own_kernel(dense_ref, rows_ref, own_ref, dense_out, left):
    store = pltpu.make_async_copy(
        dense_ref.at[pl.ds(0, dense_out.shape[0])], dense_out, left
    )
    store.start()
    height = own_ref.shape[0]
    own_blocks = height // EDGE
    size = 512
    for start in range(0, height, size):
        own_ref[pl.ds(start, size), :] = jnp.dot(
            adjacency_block(dense_ref, 0, own_blocks, start, size),
            rows_ref[...],
            preferred_element_type=jnp.float32,
        )
    store.wait()


def add_moments(z, moment_ref):
    wide = z.astype(jnp.float32)
    moment_ref[0:8, :] += jnp.sum(wide.reshape(-1, 8, wide.shape[1]), axis=0)
    moment_ref[8:16, :] += jnp.sum(jnp.square(wide).reshape(-1, 8, wide.shape[1]), axis=0)


def put_moments(moment_ref, out_ref):
    both = jnp.concatenate(
        [
            jnp.sum(moment_ref[0:8, :], axis=0, keepdims=True),
            jnp.sum(moment_ref[8:16, :], axis=0, keepdims=True),
        ],
        axis=0,
    )
    for n in range(out_ref.shape[0]):
        out_ref[n] = both


def received(a, c, d):
    count = a.shape[0] // 2
    return a[0:count, :], a[count:2 * count, :], c[0:count, :], d[0:count, :]


def first_kernel(device_ref, recv_hot_ref, a, b, c, d, dense_ref, own_ref, weight_ref, send_hot_ref,
                 z_ref, stats_ref, to_c, to_d, near_ref, dense_out,
                 halo_ref, got_ref, moment_ref, left):
    layer = 0
    count = a.shape[0]
    written = own_ref.shape[0] // EDGE + 4 * count // EDGE - dense_out.shape[0]
    store = pltpu.make_async_copy(
        dense_ref.at[pl.ds(written, dense_out.shape[0])], dense_out, left
    )
    store.start()
    for n, piece in enumerate((a, b, c, d)):
        got_ref[pl.ds(n * count, count), :] = piece[...]
    halo_ref[...] = jnp.dot(
        recv_hot_ref[...], got_ref[...], preferred_element_type=jnp.float32
    ).astype(jnp.bfloat16)
    moment_ref[...] = jnp.zeros_like(moment_ref)
    height = z_ref.shape[0]
    own_blocks, halo_blocks = height // EDGE, halo_ref.shape[0] // EDGE
    size = 512

    @pl.loop(0, height // size)
    def _(m):
        start = pl.multiple_of(m * size, size)
        agg = own_ref[pl.ds(start, size), :] + jnp.dot(
            adjacency_block(dense_ref, own_blocks, own_blocks + halo_blocks, start, size),
            halo_ref[...],
            preferred_element_type=jnp.float32,
        )
        z = jnp.dot(
            agg.astype(jnp.bfloat16), weight_ref[layer], preferred_element_type=jnp.float32
        ).astype(jnp.bfloat16)
        z_ref[pl.ds(start, size), :] = z
        add_moments(z, moment_ref)

    put_moments(moment_ref, stats_ref)
    pick_payloads(send_hot_ref, z_ref, to_c, to_d)
    put_near(device_ref, to_c, to_d, near_ref, 0)
    store.wait()


def scale_of(stats_ref, gain_ref, shift_ref, layer, vertex_total):
    both = jnp.sum(stats_ref[...], axis=0) / vertex_total
    centre = both[0:1, :]
    spread = both[1:2, :] - jnp.square(centre)
    factor = gain_ref[layer:layer + 1, :] / jnp.sqrt(spread + norm_eps)
    return centre, factor, shift_ref[layer:layer + 1, :]


def normal(rows, terms):
    centre, factor, shift = terms
    return jnp.maximum((rows.astype(jnp.float32) - centre) * factor + shift, 0.0)


def second_kernel(device_total, device_ref, index_ref, a, c, d, mixed_ref, stats_in_ref,
                  gain_ref, shift_ref, dense_a, dense_b, weight_ref, z_ref, stats_ref,
                  got_ref, columns_ref, moment_ref, recv_hot_ref, dense_ref, arrived):
    layer = 1
    count = a.shape[0] // 2
    height = z_ref.shape[0]
    halo = 4 * count
    blocks = (height + halo) // EDGE
    size = dense_ref.shape[2]


    def loads(m):
        rows, at, found = pl.ds(pl.multiple_of(m * size, size), size), 0, []
        for n, part in enumerate((dense_a, dense_b)):
            found.append(pltpu.make_async_copy(
                part.at[:, rows, :], dense_ref.at[m, pl.ds(at, part.shape[0])], arrived.at[m, n]
            ))
            at += part.shape[0]
        return found

    for m in range(height // size):
        for load in loads(m):
            load.start()
    terms = scale_of(stats_in_ref, gain_ref, shift_ref, 0, device_total * height)
    device = device_ref[0]
    near_side = (device > 0) & (device < device_total - 1)
    far_side = (device > 1) & (device < device_total - 2)
    present = (1.0, near_side.astype(jnp.float32), 1.0, far_side.astype(jnp.float32))
    for n, piece in enumerate(received(a, c, d)):
        got_ref[pl.ds(n * count, count), :] = (
            normal(piece, terms) * present[n]
        ).astype(jnp.bfloat16)
    for part in range(8):
        rows = pl.ds(part * (height // 8), height // 8)
        columns_ref[rows, :] = normal(mixed_ref[rows, :], terms).astype(jnp.bfloat16)
    fill_one_hot(index_ref, recv_hot_ref, range(index_ref.shape[0]))
    columns_ref[pl.ds(height, halo), :] = jnp.dot(
        recv_hot_ref[...], got_ref[...], preferred_element_type=jnp.float32
    ).astype(jnp.bfloat16)
    moment_ref[...] = jnp.zeros_like(moment_ref)

    @pl.loop(0, height // size)
    def _(m):
        for load in loads(m):
            load.wait()
        start = pl.multiple_of(m * size, size)
        agg = jnp.dot(
            jnp.concatenate([dense_ref[m, c] for c in range(blocks)], axis=1),
            columns_ref[...],
            preferred_element_type=jnp.float32,
        )
        z = jnp.dot(
            agg.astype(jnp.bfloat16), weight_ref[layer], preferred_element_type=jnp.float32
        ).astype(jnp.bfloat16)
        z_ref[pl.ds(start, size), :] = z
        add_moments(z, moment_ref)

    put_moments(moment_ref, stats_ref)


def last_kernel(vertex_total, mixed_ref, stats_in_ref, gain_ref, shift_ref, out_ref):
    terms = scale_of(stats_in_ref, gain_ref, shift_ref, 1, vertex_total)
    out_ref[...] = normal(mixed_ref[...], terms).astype(jnp.bfloat16)


VMEM = pl.BlockSpec(memory_space=pltpu.VMEM)
SMEM = pl.BlockSpec(memory_space=pltpu.SMEM)
HBM = pl.BlockSpec(memory_space=pltpu.HBM)


def from_peers(stats, axes):
    return lax.all_to_all(stats, axes, 0, 0, tiled=True)


def shards(features, tile_values, tile_blocks, tile_count, send_rows, recv_index,
           layer_weight, norm_gain, norm_shift):
    height, channels = features.shape
    neighbours, count = send_rows.shape[1:]
    halo = neighbours * count
    row_count = height // EDGE
    column_count = (height + halo) // EDGE
    device = lax.axis_index(PARTS)
    total = lax.axis_size(PARTS)
    vertex_total = height * total
    peers = lax.axis_size(PLANE)
    bf16, f32 = jnp.bfloat16, jnp.float32
    struct = jax.ShapeDtypeStruct
    piece = struct((count, channels), bf16)
    payload = struct((2 * count, channels), bf16)
    stats_type = struct((peers, 2, channels), f32)
    mixed = struct((height, channels), bf16)

    place = device.reshape(1)

    def on_chip(value):
        return pltpu.with_memory_space_constraint(value, pltpu.VMEM)

    def in_hbm(value):
        return pltpu.with_memory_space_constraint(value, pltpu.HBM)

    zeroed, loaded = column_count // 2, tile_values.shape[0] * 5 // 8
    dense_type = pltpu.VMEM((column_count + 1, height, EDGE), bf16)
    tiles_type = pltpu.VMEM(tile_values.shape, bf16)
    *pieces, send_hot, order, rows, dense, tiles = pl.pallas_call(
        functools.partial(gather_kernel, row_count, column_count, zeroed, loaded),
        out_shape=[piece] * 4 + [
            pltpu.VMEM((halo, height), bf16),
            struct((4, tile_blocks.shape[0]), jnp.int32),
            pltpu.VMEM((height, channels), bf16),
            dense_type,
            tiles_type,
        ],
        in_specs=[SMEM, SMEM, HBM, HBM, HBM, HBM],
        out_specs=[VMEM] * 9,
        scratch_shapes=[
            pltpu.VMEM((neighbours, count), jnp.int32),
            pltpu.VMEM((2, tile_blocks.shape[0]), jnp.int32),
            pltpu.VMEM((halo // EDGE, EDGE), jnp.int32),
            pltpu.SemaphoreType.DMA((4,)),
        ],
        compiler_params=pltpu.CompilerParams(vmem_limit_bytes=16 * MIB),
        cost_estimate=pl.CostEstimate(
            flops=2 * halo * height * channels, bytes_accessed=2 * MIB, transcendentals=0),
    )(place, tile_count, in_hbm(send_rows[0]), in_hbm(tile_blocks.T), in_hbm(features),
      in_hbm(tile_values))
    got = direct_swaps(*pieces)

    dense, _, recv_hot, built = pl.pallas_call(
        functools.partial(build_kernel, count, zeroed, loaded),
        out_shape=[
            dense_type,
            tiles_type,
            pltpu.VMEM((halo, halo), bf16),
            struct((halo // EDGE, EDGE), jnp.int32),
        ],
        in_specs=[SMEM, SMEM, SMEM, HBM, HBM, VMEM, VMEM],
        out_specs=[VMEM] * 4,
        input_output_aliases={5: 0, 6: 1},
        scratch_shapes=[
            pltpu.VMEM(recv_index.shape, jnp.int32),
            pltpu.SemaphoreType.DMA((2,)),
        ],
        compiler_params=pltpu.CompilerParams(vmem_limit_bytes=8 * MIB),
        cost_estimate=pl.CostEstimate(
            flops=4 * height * height * channels, bytes_accessed=24 * MIB, transcendentals=0),
    )(place, order, tile_count, in_hbm(recv_index), in_hbm(tile_values), on_chip(dense),
      on_chip(tiles))

    early = column_count // 3
    own, dense_a = pl.pallas_call(
        own_kernel,
        out_shape=[
            pltpu.VMEM((height, channels), f32),
            pltpu.HBM((early, height, EDGE), bf16),
        ],
        in_specs=[VMEM] * 2,
        out_specs=[VMEM, HBM],
        scratch_shapes=[pltpu.SemaphoreType.DMA],
        compiler_params=pltpu.CompilerParams(vmem_limit_bytes=8 * MIB),
        cost_estimate=pl.CostEstimate(
            flops=2 * height * height * channels, bytes_accessed=8 * MIB, transcendentals=0),
    )(on_chip(dense), on_chip(rows))

    relay_call = pl.pallas_call(
        relay_kernel,
        out_shape=payload,
        in_specs=[VMEM, SMEM] + [VMEM] * 3,
        out_specs=VMEM,
        compiler_params=pltpu.CompilerParams(vmem_limit_bytes=4 * MIB),
    )

    z, stats, *sent, near, dense_b = pl.pallas_call(
        first_kernel,
        out_shape=[pltpu.VMEM(mixed.shape, bf16), pltpu.VMEM(stats_type.shape, f32)]
        + [payload] * 2 + [piece, pltpu.HBM((column_count - early, height, EDGE), bf16)],
        in_specs=[SMEM] + [VMEM] * 9,
        out_specs=[VMEM] * 5 + [HBM],
        scratch_shapes=[
            pltpu.VMEM((halo, channels), bf16),
            pltpu.VMEM((halo, channels), bf16),
            pltpu.VMEM((16, channels), f32),
            pltpu.SemaphoreType.DMA,
        ],
        compiler_params=pltpu.CompilerParams(vmem_limit_bytes=12 * MIB),
        cost_estimate=pl.CostEstimate(
            flops=2 * height * halo * channels, bytes_accessed=16 * MIB, transcendentals=0),
    )(place, on_chip(recv_hot), *got, on_chip(dense), on_chip(own), layer_weight, on_chip(send_hot))
    got = chip_swaps(*sent)
    stats = from_peers(stats, PLANE)
    column_stats = struct((lax.axis_size(COLUMN), 2, channels), f32)
    total_call = pl.pallas_call(
        put_total,
        out_shape=pltpu.VMEM(column_stats.shape, f32),
        in_specs=[VMEM],
        out_specs=VMEM,
        compiler_params=pltpu.CompilerParams(vmem_limit_bytes=MIB),
    )
    stats = from_peers(total_call(stats), COLUMN)
    relay = relay_call(built, place, near, *got)
    got_core = core_swap(relay)

    chunk = 512
    z, stats = pl.pallas_call(
        functools.partial(second_kernel, total),
        out_shape=[pltpu.VMEM(mixed.shape, bf16), stats_type],
        in_specs=[SMEM] + [VMEM] * 8 + [HBM, HBM, VMEM],
        out_specs=[VMEM] * 2,
        scratch_shapes=[
            pltpu.VMEM((halo, channels), bf16),
            pltpu.VMEM((height + halo, channels), bf16),
            pltpu.VMEM((16, channels), f32),
            pltpu.VMEM((halo, halo), bf16),
            pltpu.VMEM((height // chunk, column_count, chunk, EDGE), bf16),
            pltpu.SemaphoreType.DMA((height // chunk, 2)),
        ],
        compiler_params=pltpu.CompilerParams(vmem_limit_bytes=28 * MIB),
        cost_estimate=pl.CostEstimate(
            flops=2 * height * (height + halo) * channels, bytes_accessed=16 * MIB,
            transcendentals=0),
    )(place, built, got_core, *got, on_chip(z), stats, norm_gain, norm_shift,
      in_hbm(dense_a), in_hbm(dense_b), layer_weight)
    stats = from_peers(stats, PLANE)
    stats = from_peers(total_call(stats), COLUMN)

    return pl.pallas_call(
        functools.partial(last_kernel, vertex_total),
        out_shape=mixed,
        in_specs=[VMEM] * 4,
        out_specs=VMEM,
        compiler_params=pltpu.CompilerParams(vmem_limit_bytes=16 * MIB),
    )(on_chip(z), stats, norm_gain, norm_shift)


def solution(mesh):
    finer = Mesh(mesh.devices.reshape(4, 4, 8, 2), PARTS)
    placed = (
        P(PARTS, None),
        P(PARTS, None, None),
        P(PARTS, None),
        P(PARTS),
        P(PARTS, None, None),
        P(PARTS, None),
        P(),
        P(),
        P(),
    )
    return jax.shard_map(
        shards, mesh=finer, in_specs=placed, out_specs=P(PARTS, None), check_vma=False
    )
```

```python
import functools

import jax
import jax.numpy as jnp
from jax import lax
from jax.experimental import pallas as pl
from jax.experimental.pallas import tpu as pltpu
from jax.sharding import Mesh
from jax.sharding import PartitionSpec as P


PARTS = ("parts_0", "parts_1", "parts_2", "parts_3")
PLANE = PARTS[:2]
COLUMN = PARTS[2:]
norm_eps = 1e-05
EDGE = 128
MIB = 1 << 20


def swap(value, first, stride, total):
    pairs = []
    for q in range(total - stride):
        if first(q):
            pairs += [(q, q + stride), (q + stride, q)]
    return lax.ppermute(value, PARTS, pairs)


def chip_swaps(to_c, to_d):
    total = lax.axis_size(PARTS)
    got_d = swap(to_d, lambda q: q % 4 >= 2, 2, total)
    got_c = swap(to_c, lambda q: q % 4 < 2, 2, total)
    return got_c, got_d


def core_swap(value):
    return swap(value, lambda q: q % 2 == 0, 1, lax.axis_size(PARTS))


def fill_one_hot(index_ref, one_hot_ref, groups):
    columns = one_hot_ref.shape[1]
    lanes = lax.broadcasted_iota(jnp.int32, (EDGE, EDGE), 1)
    for group in groups:
        row = jnp.broadcast_to(index_ref[pl.ds(group, 1), :], (EDGE, EDGE))
        away = row.T - lanes
        for block in range(columns // EDGE):
            one_hot_ref[pl.ds(group * EDGE, EDGE), pl.ds(block * EDGE, EDGE)] = jnp.where(
                away == block * EDGE, 1.0, 0.0
            ).astype(jnp.bfloat16)


def pick_piece(one_hot_ref, rows_ref, piece_ref, first, at, count):
    piece_ref[pl.ds(at, count), :] = jnp.dot(
        one_hot_ref[pl.ds(first, count), :], rows_ref[...], preferred_element_type=jnp.float32
    ).astype(jnp.bfloat16)


def pick_payloads(one_hot_ref, rows_ref, to_c, to_d):
    size = to_c.shape[0]
    pick_piece(one_hot_ref, rows_ref, to_c, 0, 0, size)
    pick_piece(one_hot_ref, rows_ref, to_d, size, 0, size)


def spread(row):
    n = row.shape[1]
    return jnp.broadcast_to(row, (n, n)).T


def put_tile_order(blocks_ref, live_count, row_count, column_count, order_ref):
    tiles = blocks_ref.shape[1]
    number = lax.broadcasted_iota(jnp.int32, (1, tiles), 1)
    live = number < live_count
    row = jnp.where(live, blocks_ref[0:1, :], 0)
    column = jnp.where(live, blocks_ref[1:2, :], column_count)
    cell = column * row_count + row
    key = cell * tiles + number
    down = lax.broadcasted_iota(jnp.int32, (tiles, tiles), 0)
    cells_down = spread(cell)
    keys_down = cells_down * tiles + down
    rank = jnp.sum((keys_down < key).astype(jnp.int32), axis=0, keepdims=True)
    same = (cells_down == cell) & (down < number)
    keep = jnp.sum(same.astype(jnp.int32), axis=0, keepdims=True) > 0
    packed = (cell * 2 + keep.astype(jnp.int32)) * tiles + number
    hit = spread(rank) == number
    packed = jnp.sum(jnp.where(hit, spread(packed), 0), axis=0, keepdims=True)
    cell = packed // (2 * tiles)
    order_ref[0:1, :] = packed % tiles
    order_ref[1:2, :] = cell % row_count
    order_ref[2:3, :] = cell // row_count
    order_ref[3:4, :] = (packed // tiles) % 2


def put_zeros(dense_ref, first, last):
    size = 256
    zeros = jnp.zeros((size, dense_ref.shape[2]), dense_ref.dtype)

    @pl.loop(first, last)
    def _(c):
        for at in range(0, dense_ref.shape[1], size):
            dense_ref[c, pl.ds(at, size), :] = zeros


def gather_kernel(row_count, column_count, zeroed, loaded,
                  device_ref, live_ref, send_in, blocks_in, features_ref, tiles_in,
                  to_c, to_d, near_ref, one_hot_ref, order_ref, rows_ref, dense_ref, tiles_ref,
                  send_ref, blocks_ref, index_ref, arrived):
    load_send = pltpu.make_async_copy(send_in, send_ref, arrived.at[0])
    load_blocks = pltpu.make_async_copy(blocks_in, blocks_ref, arrived.at[1])
    load = pltpu.make_async_copy(features_ref, rows_ref, arrived.at[2])
    part = pl.ds(0, loaded)
    load_tiles = pltpu.make_async_copy(tiles_in.at[part], tiles_ref.at[part], arrived.at[3])
    load_send.start()
    load_blocks.start()
    load.start()
    load_tiles.start()
    put_zeros(dense_ref, 0, zeroed)
    load_send.wait()
    even_chip = device_ref[0] % 4 < 2
    count = send_ref.shape[1]
    per_piece = count // EDGE
    for part in range(per_piece):
        n0, n1, n2, n3 = (send_ref[n:n + 1, part * EDGE:(part + 1) * EDGE] for n in range(4))
        lists = (
            jnp.where(even_chip, n2, n3),
            jnp.where(even_chip, n0, n1),
            jnp.where(even_chip, n3, n2),
            jnp.where(even_chip, n1, n0),
        )
        for n, chosen in enumerate(lists):
            at = n * per_piece + part
            index_ref[at:at + 1, :] = chosen
    fill_one_hot(index_ref, one_hot_ref, range(2 * per_piece))
    load_blocks.wait()
    put_tile_order(blocks_ref, live_ref[0], row_count, column_count, order_ref)
    load.wait()
    pick_piece(one_hot_ref, rows_ref, to_c, 0, 0, count)
    fill_one_hot(index_ref, one_hot_ref, range(2 * per_piece, 3 * per_piece))
    pick_piece(one_hot_ref, rows_ref, to_c, count, count, count)
    fill_one_hot(index_ref, one_hot_ref, range(3 * per_piece, 4 * per_piece))
    pick_piece(one_hot_ref, rows_ref, to_d, 2 * count, 0, count)
    pick_piece(one_hot_ref, rows_ref, to_d, 3 * count, count, count)
    put_near(device_ref, to_c, to_d, near_ref, 0)
    load_tiles.wait()


def put_near(device_ref, from_c, from_d, out_ref, at):
    count = from_c.shape[0] // 2
    first = (device_ref[0] % 4 < 2) == (device_ref[0] % 2 == 0)

    @pl.when(first)
    def _():
        out_ref[at:at + count, :] = from_c[count:2 * count, :]

    @pl.when(jnp.logical_not(first))
    def _():
        out_ref[at:at + count, :] = from_d[count:2 * count, :]


def relay_kernel(after_ref, device_ref, near_ref, got_c, got_d, out_ref):
    del after_ref
    count = near_ref.shape[0]
    out_ref[0:count, :] = near_ref[...]
    put_near(device_ref, got_c, got_d, out_ref, count)


def put_total(parts_ref, out_ref):
    both = jnp.sum(parts_ref[...], axis=0)
    for n in range(out_ref.shape[0]):
        out_ref[n] = both


def adjacency_block(dense_ref, first, last, start, size):
    return jnp.concatenate(
        [dense_ref[c, pl.ds(start, size), :] for c in range(first, last)], axis=1
    )


def build_kernel(count, zeroed, loaded,
                 device_ref, order_ref, live_ref, recv_in, tiles_in, _dense, _tiles,
                 dense_ref, held_ref, recv_hot_ref, index_ref, recv_ref, arrived):
    part = pl.ds(loaded, held_ref.shape[0] - loaded)
    load_recv = pltpu.make_async_copy(recv_in, recv_ref, arrived.at[0])
    load = pltpu.make_async_copy(tiles_in.at[part], held_ref.at[part], arrived.at[1])
    load_recv.start()
    load.start()
    unroll = 8
    put_zeros(dense_ref, zeroed, dense_ref.shape[0])

    near = jnp.where(device_ref[0] % 2 == 0, count, 0)
    far = jnp.where(device_ref[0] % 4 < 2, count, 0)
    load_recv.wait()
    for group in range(index_ref.shape[0]):
        rows = recv_ref[0:1, group * EDGE:(group + 1) * EDGE]
        index_ref[group:group + 1, :] = rows ^ jnp.where(rows < 2 * count, near, far)
    fill_one_hot(index_ref, recv_hot_ref, range(index_ref.shape[0]))
    load.wait()

    def step(turn, total):
        for u in range(unroll):
            k = turn * unroll + u
            tile = held_ref[order_ref[0, k]].astype(jnp.float32)
            total = total * order_ref[3, k].astype(jnp.float32) + tile
            start = pl.multiple_of(order_ref[1, k] * EDGE, EDGE)
            dense_ref[order_ref[2, k], pl.ds(start, EDGE), :] = total.astype(jnp.bfloat16)
        return total

    lax.fori_loop(
        0, (live_ref[0] + unroll - 1) // unroll, step, jnp.zeros((EDGE, EDGE), jnp.float32)
    )


def own_kernel(dense_ref, rows_ref, own_ref, dense_out, left):
    store = pltpu.make_async_copy(
        dense_ref.at[pl.ds(0, dense_out.shape[0])], dense_out, left
    )
    store.start()
    height = own_ref.shape[0]
    own_blocks = height // EDGE
    size = 512
    for start in range(0, height, size):
        own_ref[pl.ds(start, size), :] = jnp.dot(
            adjacency_block(dense_ref, 0, own_blocks, start, size),
            rows_ref[...],
            preferred_element_type=jnp.float32,
        )
    store.wait()


def add_moments(z, moment_ref):
    wide = z.astype(jnp.float32)
    moment_ref[0:8, :] += jnp.sum(wide.reshape(-1, 8, wide.shape[1]), axis=0)
    moment_ref[8:16, :] += jnp.sum(jnp.square(wide).reshape(-1, 8, wide.shape[1]), axis=0)


def put_moments(moment_ref, out_ref):
    both = jnp.concatenate(
        [
            jnp.sum(moment_ref[0:8, :], axis=0, keepdims=True),
            jnp.sum(moment_ref[8:16, :], axis=0, keepdims=True),
        ],
        axis=0,
    )
    for n in range(out_ref.shape[0]):
        out_ref[n] = both


def received(a, c, d):
    count = a.shape[0] // 2
    return a[0:count, :], a[count:2 * count, :], c[0:count, :], d[0:count, :]


def first_kernel(device_ref, recv_hot_ref, a, c, d, dense_ref, own_ref, weight_ref, send_hot_ref,
                 z_ref, stats_ref, to_c, to_d, near_ref, dense_out,
                 halo_ref, got_ref, moment_ref, left):
    layer = 0
    count = a.shape[0] // 2
    written = own_ref.shape[0] // EDGE + 4 * count // EDGE - dense_out.shape[0]
    store = pltpu.make_async_copy(
        dense_ref.at[pl.ds(written, dense_out.shape[0])], dense_out, left
    )
    store.start()
    for n, piece in enumerate(received(a, c, d)):
        got_ref[pl.ds(n * count, count), :] = piece
    halo_ref[...] = jnp.dot(
        recv_hot_ref[...], got_ref[...], preferred_element_type=jnp.float32
    ).astype(jnp.bfloat16)
    moment_ref[...] = jnp.zeros_like(moment_ref)
    height = z_ref.shape[0]
    own_blocks, halo_blocks = height // EDGE, halo_ref.shape[0] // EDGE
    size = 512

    @pl.loop(0, height // size)
    def _(m):
        start = pl.multiple_of(m * size, size)
        agg = own_ref[pl.ds(start, size), :] + jnp.dot(
            adjacency_block(dense_ref, own_blocks, own_blocks + halo_blocks, start, size),
            halo_ref[...],
            preferred_element_type=jnp.float32,
        )
        z = jnp.dot(
            agg.astype(jnp.bfloat16), weight_ref[layer], preferred_element_type=jnp.float32
        ).astype(jnp.bfloat16)
        z_ref[pl.ds(start, size), :] = z
        add_moments(z, moment_ref)

    put_moments(moment_ref, stats_ref)
    pick_payloads(send_hot_ref, z_ref, to_c, to_d)
    put_near(device_ref, to_c, to_d, near_ref, 0)
    store.wait()


def scale_of(stats_ref, gain_ref, shift_ref, layer, vertex_total):
    both = jnp.sum(stats_ref[...], axis=0) / vertex_total
    centre = both[0:1, :]
    spread = both[1:2, :] - jnp.square(centre)
    factor = gain_ref[layer:layer + 1, :] / jnp.sqrt(spread + norm_eps)
    return centre, factor, shift_ref[layer:layer + 1, :]


def normal(rows, terms):
    centre, factor, shift = terms
    return jnp.maximum((rows.astype(jnp.float32) - centre) * factor + shift, 0.0)


def second_kernel(device_total, device_ref, index_ref, a, c, d, mixed_ref, stats_in_ref,
                  gain_ref, shift_ref, dense_a, dense_b, weight_ref, z_ref, stats_ref,
                  got_ref, columns_ref, moment_ref, recv_hot_ref, dense_ref, arrived):
    layer = 1
    count = a.shape[0] // 2
    height = z_ref.shape[0]
    halo = 4 * count
    blocks = (height + halo) // EDGE
    size = dense_ref.shape[2]


    def loads(m):
        rows, at, found = pl.ds(pl.multiple_of(m * size, size), size), 0, []
        for n, part in enumerate((dense_a, dense_b)):
            found.append(pltpu.make_async_copy(
                part.at[:, rows, :], dense_ref.at[m, pl.ds(at, part.shape[0])], arrived.at[m, n]
            ))
            at += part.shape[0]
        return found

    for m in range(height // size):
        for load in loads(m):
            load.start()
    terms = scale_of(stats_in_ref, gain_ref, shift_ref, 0, device_total * height)
    device = device_ref[0]
    near_side = (device > 0) & (device < device_total - 1)
    far_side = (device > 1) & (device < device_total - 2)
    present = (1.0, near_side.astype(jnp.float32), 1.0, far_side.astype(jnp.float32))
    for n, piece in enumerate(received(a, c, d)):
        got_ref[pl.ds(n * count, count), :] = (
            normal(piece, terms) * present[n]
        ).astype(jnp.bfloat16)
    for part in range(8):
        rows = pl.ds(part * (height // 8), height // 8)
        columns_ref[rows, :] = normal(mixed_ref[rows, :], terms).astype(jnp.bfloat16)
    fill_one_hot(index_ref, recv_hot_ref, range(index_ref.shape[0]))
    columns_ref[pl.ds(height, halo), :] = jnp.dot(
        recv_hot_ref[...], got_ref[...], preferred_element_type=jnp.float32
    ).astype(jnp.bfloat16)
    moment_ref[...] = jnp.zeros_like(moment_ref)

    @pl.loop(0, height // size)
    def _(m):
        for load in loads(m):
            load.wait()
        start = pl.multiple_of(m * size, size)
        agg = jnp.dot(
            jnp.concatenate([dense_ref[m, c] for c in range(blocks)], axis=1),
            columns_ref[...],
            preferred_element_type=jnp.float32,
        )
        z = jnp.dot(
            agg.astype(jnp.bfloat16), weight_ref[layer], preferred_element_type=jnp.float32
        ).astype(jnp.bfloat16)
        z_ref[pl.ds(start, size), :] = z
        add_moments(z, moment_ref)

    put_moments(moment_ref, stats_ref)


def last_kernel(vertex_total, mixed_ref, stats_in_ref, gain_ref, shift_ref, out_ref):
    terms = scale_of(stats_in_ref, gain_ref, shift_ref, 1, vertex_total)
    out_ref[...] = normal(mixed_ref[...], terms).astype(jnp.bfloat16)


VMEM = pl.BlockSpec(memory_space=pltpu.VMEM)
SMEM = pl.BlockSpec(memory_space=pltpu.SMEM)
HBM = pl.BlockSpec(memory_space=pltpu.HBM)


def from_peers(stats, axes):
    return lax.all_to_all(stats, axes, 0, 0, tiled=True)


def shards(features, tile_values, tile_blocks, tile_count, send_rows, recv_index,
           layer_weight, norm_gain, norm_shift):
    height, channels = features.shape
    neighbours, count = send_rows.shape[1:]
    halo = neighbours * count
    row_count = height // EDGE
    column_count = (height + halo) // EDGE
    device = lax.axis_index(PARTS)
    total = lax.axis_size(PARTS)
    vertex_total = height * total
    peers = lax.axis_size(PLANE)
    bf16, f32 = jnp.bfloat16, jnp.float32
    struct = jax.ShapeDtypeStruct
    piece = struct((count, channels), bf16)
    payload = struct((2 * count, channels), bf16)
    stats_type = struct((peers, 2, channels), f32)
    mixed = struct((height, channels), bf16)

    place = device.reshape(1)

    def on_chip(value):
        return pltpu.with_memory_space_constraint(value, pltpu.VMEM)

    def in_hbm(value):
        return pltpu.with_memory_space_constraint(value, pltpu.HBM)

    zeroed, loaded = column_count // 2, tile_values.shape[0] * 5 // 8
    dense_type = pltpu.VMEM((column_count + 1, height, EDGE), bf16)
    tiles_type = pltpu.VMEM(tile_values.shape, bf16)
    *sent, near, send_hot, order, rows, dense, tiles = pl.pallas_call(
        functools.partial(gather_kernel, row_count, column_count, zeroed, loaded),
        out_shape=[payload] * 2 + [
            piece,
            pltpu.VMEM((halo, height), bf16),
            struct((4, tile_blocks.shape[0]), jnp.int32),
            pltpu.VMEM((height, channels), bf16),
            dense_type,
            tiles_type,
        ],
        in_specs=[SMEM, SMEM, HBM, HBM, HBM, HBM],
        out_specs=[VMEM] * 8,
        scratch_shapes=[
            pltpu.VMEM((neighbours, count), jnp.int32),
            pltpu.VMEM((2, tile_blocks.shape[0]), jnp.int32),
            pltpu.VMEM((halo // EDGE, EDGE), jnp.int32),
            pltpu.SemaphoreType.DMA((4,)),
        ],
        compiler_params=pltpu.CompilerParams(vmem_limit_bytes=16 * MIB),
        cost_estimate=pl.CostEstimate(
            flops=2 * halo * height * channels, bytes_accessed=2 * MIB, transcendentals=0),
    )(place, tile_count, in_hbm(send_rows[0]), in_hbm(tile_blocks.T), in_hbm(features),
      in_hbm(tile_values))
    got = chip_swaps(*sent)

    dense, _, recv_hot, built = pl.pallas_call(
        functools.partial(build_kernel, count, zeroed, loaded),
        out_shape=[
            dense_type,
            tiles_type,
            pltpu.VMEM((halo, halo), bf16),
            struct((halo // EDGE, EDGE), jnp.int32),
        ],
        in_specs=[SMEM, SMEM, SMEM, HBM, HBM, VMEM, VMEM],
        out_specs=[VMEM] * 4,
        input_output_aliases={5: 0, 6: 1},
        scratch_shapes=[
            pltpu.VMEM(recv_index.shape, jnp.int32),
            pltpu.SemaphoreType.DMA((2,)),
        ],
        compiler_params=pltpu.CompilerParams(vmem_limit_bytes=8 * MIB),
        cost_estimate=pl.CostEstimate(
            flops=4 * height * height * channels, bytes_accessed=24 * MIB, transcendentals=0),
    )(place, order, tile_count, in_hbm(recv_index), in_hbm(tile_values), on_chip(dense),
      on_chip(tiles))

    early = column_count // 3
    own, dense_a = pl.pallas_call(
        own_kernel,
        out_shape=[
            pltpu.VMEM((height, channels), f32),
            pltpu.HBM((early, height, EDGE), bf16),
        ],
        in_specs=[VMEM] * 2,
        out_specs=[VMEM, HBM],
        scratch_shapes=[pltpu.SemaphoreType.DMA],
        compiler_params=pltpu.CompilerParams(vmem_limit_bytes=8 * MIB),
        cost_estimate=pl.CostEstimate(
            flops=2 * height * height * channels, bytes_accessed=8 * MIB, transcendentals=0),
    )(on_chip(dense), on_chip(rows))

    relay_call = pl.pallas_call(
        relay_kernel,
        out_shape=payload,
        in_specs=[VMEM, SMEM] + [VMEM] * 3,
        out_specs=VMEM,
        compiler_params=pltpu.CompilerParams(vmem_limit_bytes=4 * MIB),
    )
    relay = relay_call(own, place, near, *got)
    got_core = core_swap(relay)

    z, stats, *sent, near, dense_b = pl.pallas_call(
        first_kernel,
        out_shape=[pltpu.VMEM(mixed.shape, bf16), pltpu.VMEM(stats_type.shape, f32)]
        + [payload] * 2 + [piece, pltpu.HBM((column_count - early, height, EDGE), bf16)],
        in_specs=[SMEM] + [VMEM] * 8,
        out_specs=[VMEM] * 5 + [HBM],
        scratch_shapes=[
            pltpu.VMEM((halo, channels), bf16),
            pltpu.VMEM((halo, channels), bf16),
            pltpu.VMEM((16, channels), f32),
            pltpu.SemaphoreType.DMA,
        ],
        compiler_params=pltpu.CompilerParams(vmem_limit_bytes=12 * MIB),
        cost_estimate=pl.CostEstimate(
            flops=2 * height * halo * channels, bytes_accessed=16 * MIB, transcendentals=0),
    )(place, on_chip(recv_hot), got_core, *got, on_chip(dense), on_chip(own), layer_weight, on_chip(send_hot))
    got = chip_swaps(*sent)
    stats = from_peers(stats, PLANE)
    column_stats = struct((lax.axis_size(COLUMN), 2, channels), f32)
    total_call = pl.pallas_call(
        put_total,
        out_shape=pltpu.VMEM(column_stats.shape, f32),
        in_specs=[VMEM],
        out_specs=VMEM,
        compiler_params=pltpu.CompilerParams(vmem_limit_bytes=MIB),
    )
    stats = from_peers(total_call(stats), COLUMN)
    relay = relay_call(built, place, near, *got)
    got_core = core_swap(relay)

    chunk = 512
    z, stats = pl.pallas_call(
        functools.partial(second_kernel, total),
        out_shape=[pltpu.VMEM(mixed.shape, bf16), stats_type],
        in_specs=[SMEM] + [VMEM] * 8 + [HBM, HBM, VMEM],
        out_specs=[VMEM] * 2,
        scratch_shapes=[
            pltpu.VMEM((halo, channels), bf16),
            pltpu.VMEM((height + halo, channels), bf16),
            pltpu.VMEM((16, channels), f32),
            pltpu.VMEM((halo, halo), bf16),
            pltpu.VMEM((height // chunk, column_count, chunk, EDGE), bf16),
            pltpu.SemaphoreType.DMA((height // chunk, 2)),
        ],
        compiler_params=pltpu.CompilerParams(vmem_limit_bytes=28 * MIB),
        cost_estimate=pl.CostEstimate(
            flops=2 * height * (height + halo) * channels, bytes_accessed=16 * MIB,
            transcendentals=0),
    )(place, built, got_core, *got, on_chip(z), stats, norm_gain, norm_shift,
      in_hbm(dense_a), in_hbm(dense_b), layer_weight)
    stats = from_peers(stats, PLANE)
    stats = from_peers(total_call(stats), COLUMN)

    return pl.pallas_call(
        functools.partial(last_kernel, vertex_total),
        out_shape=mixed,
        in_specs=[VMEM] * 4,
        out_specs=VMEM,
        compiler_params=pltpu.CompilerParams(vmem_limit_bytes=16 * MIB),
    )(on_chip(z), stats, norm_gain, norm_shift)


def solution(mesh):
    finer = Mesh(mesh.devices.reshape(4, 4, 8, 2), PARTS)
    placed = (
        P(PARTS, None),
        P(PARTS, None, None),
        P(PARTS, None),
        P(PARTS),
        P(PARTS, None, None),
        P(PARTS, None),
        P(),
        P(),
        P(),
    )
    return jax.shard_map(
        shards, mesh=finer, in_specs=placed, out_specs=P(PARTS, None), check_vma=False
    )
```

```python
import functools

import jax
import jax.numpy as jnp
from jax import lax
from jax.experimental import pallas as pl
from jax.experimental.pallas import tpu as pltpu
from jax.sharding import Mesh
from jax.sharding import PartitionSpec as P


PARTS = ("parts_0", "parts_1", "parts_2", "parts_3")
PLANE = PARTS[:2]
COLUMN = PARTS[2:]
norm_eps = 1e-05
EDGE = 128
MIB = 1 << 20


def swap(value, first, stride, total):
    pairs = []
    for q in range(total - stride):
        if first(q):
            pairs += [(q, q + stride), (q + stride, q)]
    return lax.ppermute(value, PARTS, pairs)


def chip_swaps(to_c, to_d):
    total = lax.axis_size(PARTS)
    got_d = swap(to_d, lambda q: q % 4 >= 2, 2, total)
    got_c = swap(to_c, lambda q: q % 4 < 2, 2, total)
    return got_c, got_d


def core_swap(value):
    return swap(value, lambda q: q % 2 == 0, 1, lax.axis_size(PARTS))


def fill_one_hot(index_ref, one_hot_ref, groups):
    columns = one_hot_ref.shape[1]
    lanes = lax.broadcasted_iota(jnp.int32, (EDGE, EDGE), 1)
    for group in groups:
        row = jnp.broadcast_to(index_ref[pl.ds(group, 1), :], (EDGE, EDGE))
        away = row.T - lanes
        for block in range(columns // EDGE):
            one_hot_ref[pl.ds(group * EDGE, EDGE), pl.ds(block * EDGE, EDGE)] = jnp.where(
                away == block * EDGE, 1.0, 0.0
            ).astype(jnp.bfloat16)


def pick_piece(one_hot_ref, rows_ref, piece_ref, first, at, count):
    piece_ref[pl.ds(at, count), :] = jnp.dot(
        one_hot_ref[pl.ds(first, count), :], rows_ref[...], preferred_element_type=jnp.float32
    ).astype(jnp.bfloat16)


def spread(row):
    n = row.shape[1]
    return jnp.broadcast_to(row, (n, n)).T


def put_tile_order(blocks_ref, live_count, row_count, column_count, order_ref):
    tiles = blocks_ref.shape[1]
    number = lax.broadcasted_iota(jnp.int32, (1, tiles), 1)
    live = number < live_count
    row = jnp.where(live, blocks_ref[0:1, :], 0)
    column = jnp.where(live, blocks_ref[1:2, :], column_count)
    cell = column * row_count + row
    key = cell * tiles + number
    down = lax.broadcasted_iota(jnp.int32, (tiles, tiles), 0)
    cells_down = spread(cell)
    keys_down = cells_down * tiles + down
    rank = jnp.sum((keys_down < key).astype(jnp.int32), axis=0, keepdims=True)
    same = (cells_down == cell) & (down < number)
    keep = jnp.sum(same.astype(jnp.int32), axis=0, keepdims=True) > 0
    packed = (cell * 2 + keep.astype(jnp.int32)) * tiles + number
    hit = spread(rank) == number
    packed = jnp.sum(jnp.where(hit, spread(packed), 0), axis=0, keepdims=True)
    cell = packed // (2 * tiles)
    order_ref[0:1, :] = packed % tiles
    order_ref[1:2, :] = cell % row_count
    order_ref[2:3, :] = cell // row_count
    order_ref[3:4, :] = (packed // tiles) % 2


def put_zeros(dense_ref, first, last):
    size = 256
    zeros = jnp.zeros((size, dense_ref.shape[2]), dense_ref.dtype)

    @pl.loop(first, last)
    def _(c):
        for at in range(0, dense_ref.shape[1], size):
            dense_ref[c, pl.ds(at, size), :] = zeros


def gather_kernel(row_count, column_count, zeroed, loaded,
                  device_ref, live_ref, send_in, blocks_in, features_ref, tiles_in,
                  to_c, to_d, near_ref, one_hot_ref, order_ref, rows_ref, dense_ref, tiles_ref,
                  send_ref, blocks_ref, index_ref, arrived):
    load_send = pltpu.make_async_copy(send_in, send_ref, arrived.at[0])
    load_blocks = pltpu.make_async_copy(blocks_in, blocks_ref, arrived.at[1])
    load = pltpu.make_async_copy(features_ref, rows_ref, arrived.at[2])
    part = pl.ds(0, loaded)
    load_tiles = pltpu.make_async_copy(tiles_in.at[part], tiles_ref.at[part], arrived.at[3])
    load_send.start()
    load_blocks.start()
    load.start()
    load_tiles.start()
    put_zeros(dense_ref, 0, zeroed)
    load_send.wait()
    even_chip = device_ref[0] % 4 < 2
    count = send_ref.shape[1]
    per_piece = count // EDGE
    for part in range(per_piece):
        n0, n1, n2, n3 = (send_ref[n:n + 1, part * EDGE:(part + 1) * EDGE] for n in range(4))
        lists = (
            jnp.where(even_chip, n2, n3),
            jnp.where(even_chip, n0, n1),
            jnp.where(even_chip, n3, n2),
            jnp.where(even_chip, n1, n0),
        )
        for n, chosen in enumerate(lists):
            at = n * per_piece + part
            index_ref[at:at + 1, :] = chosen
    fill_one_hot(index_ref, one_hot_ref, range(2 * per_piece))
    load_blocks.wait()
    put_tile_order(blocks_ref, live_ref[0], row_count, column_count, order_ref)
    load.wait()
    pick_piece(one_hot_ref, rows_ref, to_c, 0, 0, count)
    fill_one_hot(index_ref, one_hot_ref, range(2 * per_piece, 3 * per_piece))
    pick_piece(one_hot_ref, rows_ref, to_c, count, count, count)
    fill_one_hot(index_ref, one_hot_ref, range(3 * per_piece, 4 * per_piece))
    pick_piece(one_hot_ref, rows_ref, to_d, 2 * count, 0, count)
    pick_piece(one_hot_ref, rows_ref, to_d, 3 * count, count, count)
    put_near(device_ref, to_c, to_d, near_ref, 0)
    load_tiles.wait()


def put_near(device_ref, from_c, from_d, out_ref, at):
    count = from_c.shape[0] // 2
    first = (device_ref[0] % 4 < 2) == (device_ref[0] % 2 == 0)

    @pl.when(first)
    def _():
        out_ref[at:at + count, :] = from_c[count:2 * count, :]

    @pl.when(jnp.logical_not(first))
    def _():
        out_ref[at:at + count, :] = from_d[count:2 * count, :]


def relay_kernel(after_ref, device_ref, near_ref, got_c, got_d, out_ref):
    del after_ref
    count = near_ref.shape[0]
    out_ref[0:count, :] = near_ref[...]
    put_near(device_ref, got_c, got_d, out_ref, count)


def put_total(parts_ref, out_ref):
    both = jnp.sum(parts_ref[...], axis=0)
    for n in range(out_ref.shape[0]):
        out_ref[n] = both


def adjacency_block(dense_ref, first, last, start, size):
    return jnp.concatenate(
        [dense_ref[c, pl.ds(start, size), :] for c in range(first, last)], axis=1
    )


def build_kernel(count, zeroed, loaded,
                 device_ref, order_ref, live_ref, recv_in, tiles_in, _dense, _tiles,
                 dense_ref, held_ref, recv_hot_ref, index_ref, recv_ref, arrived):
    part = pl.ds(loaded, held_ref.shape[0] - loaded)
    load_recv = pltpu.make_async_copy(recv_in, recv_ref, arrived.at[0])
    load = pltpu.make_async_copy(tiles_in.at[part], held_ref.at[part], arrived.at[1])
    load_recv.start()
    load.start()
    unroll = 8
    put_zeros(dense_ref, zeroed, dense_ref.shape[0])

    near = jnp.where(device_ref[0] % 2 == 0, count, 0)
    far = jnp.where(device_ref[0] % 4 < 2, count, 0)
    load_recv.wait()
    for group in range(index_ref.shape[0]):
        rows = recv_ref[0:1, group * EDGE:(group + 1) * EDGE]
        index_ref[group:group + 1, :] = rows ^ jnp.where(rows < 2 * count, near, far)
    fill_one_hot(index_ref, recv_hot_ref, range(index_ref.shape[0]))
    load.wait()

    def step(turn, total):
        for u in range(unroll):
            k = turn * unroll + u
            tile = held_ref[order_ref[0, k]].astype(jnp.float32)
            total = total * order_ref[3, k].astype(jnp.float32) + tile
            start = pl.multiple_of(order_ref[1, k] * EDGE, EDGE)
            dense_ref[order_ref[2, k], pl.ds(start, EDGE), :] = total.astype(jnp.bfloat16)
        return total

    lax.fori_loop(
        0, (live_ref[0] + unroll - 1) // unroll, step, jnp.zeros((EDGE, EDGE), jnp.float32)
    )


def own_kernel(dense_ref, rows_ref, own_ref, dense_out, left):
    store = pltpu.make_async_copy(
        dense_ref.at[pl.ds(0, dense_out.shape[0])], dense_out, left
    )
    store.start()
    height = own_ref.shape[0]
    own_blocks = height // EDGE
    size = 512
    for start in range(0, height, size):
        own_ref[pl.ds(start, size), :] = jnp.dot(
            adjacency_block(dense_ref, 0, own_blocks, start, size),
            rows_ref[...],
            preferred_element_type=jnp.float32,
        )
    store.wait()


def add_moments(z, moment_ref):
    wide = z.astype(jnp.float32)
    moment_ref[0:8, :] += jnp.sum(wide.reshape(-1, 8, wide.shape[1]), axis=0)
    moment_ref[8:16, :] += jnp.sum(jnp.square(wide).reshape(-1, 8, wide.shape[1]), axis=0)


def put_moments(moment_ref, out_ref):
    both = jnp.concatenate(
        [
            jnp.sum(moment_ref[0:8, :], axis=0, keepdims=True),
            jnp.sum(moment_ref[8:16, :], axis=0, keepdims=True),
        ],
        axis=0,
    )
    for n in range(out_ref.shape[0]):
        out_ref[n] = both


def received(a, c, d):
    count = a.shape[0] // 2
    return a[0:count, :], a[count:2 * count, :], c[0:count, :], d[0:count, :]


def first_kernel(device_ref, recv_hot_ref, a, c, d, dense_ref, own_ref, weight_ref, send_hot_ref,
                 z_ref, stats_out, to_c, to_d, near_ref, dense_out,
                 halo_ref, got_ref, moment_ref, stats_ref, left):
    layer = 0
    count = a.shape[0] // 2
    written = own_ref.shape[0] // EDGE + 4 * count // EDGE - dense_out.shape[0]
    store = pltpu.make_async_copy(
        dense_ref.at[pl.ds(written, dense_out.shape[0])], dense_out, left.at[0]
    )
    store.start()
    for n, piece in enumerate(received(a, c, d)):
        got_ref[pl.ds(n * count, count), :] = piece
    halo_ref[...] = jnp.dot(
        recv_hot_ref[...], got_ref[...], preferred_element_type=jnp.float32
    ).astype(jnp.bfloat16)
    moment_ref[...] = jnp.zeros_like(moment_ref)
    height = z_ref.shape[0]
    own_blocks, halo_blocks = height // EDGE, halo_ref.shape[0] // EDGE
    size = 512

    @pl.loop(0, height // size)
    def _(m):
        start = pl.multiple_of(m * size, size)
        agg = own_ref[pl.ds(start, size), :] + jnp.dot(
            adjacency_block(dense_ref, own_blocks, own_blocks + halo_blocks, start, size),
            halo_ref[...],
            preferred_element_type=jnp.float32,
        )
        z = jnp.dot(
            agg.astype(jnp.bfloat16), weight_ref[layer], preferred_element_type=jnp.float32
        ).astype(jnp.bfloat16)
        z_ref[pl.ds(start, size), :] = z
        add_moments(z, moment_ref)

    put_moments(moment_ref, stats_ref)
    size = to_c.shape[0]
    pick_piece(send_hot_ref, z_ref, to_c, 0, 0, size)
    store_stats = pltpu.make_async_copy(stats_ref, stats_out, left.at[1])
    store_stats.start()
    pick_piece(send_hot_ref, z_ref, to_d, size, 0, size)
    put_near(device_ref, to_c, to_d, near_ref, 0)
    store.wait()
    store_stats.wait()


def scale_of(stats_ref, gain_ref, shift_ref, layer, vertex_total):
    both = jnp.sum(stats_ref[...], axis=0) / vertex_total
    centre = both[0:1, :]
    spread = both[1:2, :] - jnp.square(centre)
    factor = gain_ref[layer:layer + 1, :] / jnp.sqrt(spread + norm_eps)
    return centre, factor, shift_ref[layer:layer + 1, :]


def normal(rows, terms):
    centre, factor, shift = terms
    return jnp.maximum((rows.astype(jnp.float32) - centre) * factor + shift, 0.0)


def second_kernel(device_total, device_ref, index_ref, a, c, d, mixed_ref, stats_in_ref,
                  gain_ref, shift_ref, dense_a, dense_b, weight_ref, z_ref, stats_ref,
                  got_ref, columns_ref, moment_ref, recv_hot_ref, dense_ref, arrived):
    layer = 1
    count = a.shape[0] // 2
    height = z_ref.shape[0]
    halo = 4 * count
    blocks = (height + halo) // EDGE
    size = dense_ref.shape[2]


    def loads(m):
        rows, at, found = pl.ds(pl.multiple_of(m * size, size), size), 0, []
        for n, part in enumerate((dense_a, dense_b)):
            found.append(pltpu.make_async_copy(
                part.at[:, rows, :], dense_ref.at[m, pl.ds(at, part.shape[0])], arrived.at[m, n]
            ))
            at += part.shape[0]
        return found

    for m in range(height // size):
        for load in loads(m):
            load.start()
    terms = scale_of(stats_in_ref, gain_ref, shift_ref, 0, device_total * height)
    device = device_ref[0]
    near_side = (device > 0) & (device < device_total - 1)
    far_side = (device > 1) & (device < device_total - 2)
    present = (1.0, near_side.astype(jnp.float32), 1.0, far_side.astype(jnp.float32))
    for n, piece in enumerate(received(a, c, d)):
        got_ref[pl.ds(n * count, count), :] = (
            normal(piece, terms) * present[n]
        ).astype(jnp.bfloat16)
    for part in range(8):
        rows = pl.ds(part * (height // 8), height // 8)
        columns_ref[rows, :] = normal(mixed_ref[rows, :], terms).astype(jnp.bfloat16)
    fill_one_hot(index_ref, recv_hot_ref, range(index_ref.shape[0]))
    columns_ref[pl.ds(height, halo), :] = jnp.dot(
        recv_hot_ref[...], got_ref[...], preferred_element_type=jnp.float32
    ).astype(jnp.bfloat16)
    moment_ref[...] = jnp.zeros_like(moment_ref)

    @pl.loop(0, height // size)
    def _(m):
        for load in loads(m):
            load.wait()
        start = pl.multiple_of(m * size, size)
        agg = jnp.dot(
            jnp.concatenate([dense_ref[m, c] for c in range(blocks)], axis=1),
            columns_ref[...],
            preferred_element_type=jnp.float32,
        )
        z = jnp.dot(
            agg.astype(jnp.bfloat16), weight_ref[layer], preferred_element_type=jnp.float32
        ).astype(jnp.bfloat16)
        z_ref[pl.ds(start, size), :] = z
        add_moments(z, moment_ref)

    put_moments(moment_ref, stats_ref)


def last_kernel(vertex_total, mixed_ref, stats_in_ref, gain_ref, shift_ref, out_ref):
    terms = scale_of(stats_in_ref, gain_ref, shift_ref, 1, vertex_total)
    out_ref[...] = normal(mixed_ref[...], terms).astype(jnp.bfloat16)


VMEM = pl.BlockSpec(memory_space=pltpu.VMEM)
SMEM = pl.BlockSpec(memory_space=pltpu.SMEM)
HBM = pl.BlockSpec(memory_space=pltpu.HBM)


def from_peers(stats, axes):
    return lax.all_to_all(stats, axes, 0, 0, tiled=True)


def shards(features, tile_values, tile_blocks, tile_count, send_rows, recv_index,
           layer_weight, norm_gain, norm_shift):
    height, channels = features.shape
    neighbours, count = send_rows.shape[1:]
    halo = neighbours * count
    row_count = height // EDGE
    column_count = (height + halo) // EDGE
    device = lax.axis_index(PARTS)
    total = lax.axis_size(PARTS)
    vertex_total = height * total
    peers = lax.axis_size(PLANE)
    bf16, f32 = jnp.bfloat16, jnp.float32
    struct = jax.ShapeDtypeStruct
    piece = struct((count, channels), bf16)
    payload = struct((2 * count, channels), bf16)
    stats_type = struct((peers, 2, channels), f32)
    mixed = struct((height, channels), bf16)

    place = device.reshape(1)

    def on_chip(value):
        return pltpu.with_memory_space_constraint(value, pltpu.VMEM)

    def in_hbm(value):
        return pltpu.with_memory_space_constraint(value, pltpu.HBM)

    zeroed, loaded = column_count // 2, tile_values.shape[0] * 5 // 8
    dense_type = pltpu.VMEM((column_count + 1, height, EDGE), bf16)
    tiles_type = pltpu.VMEM(tile_values.shape, bf16)
    *sent, near, send_hot, order, rows, dense, tiles = pl.pallas_call(
        functools.partial(gather_kernel, row_count, column_count, zeroed, loaded),
        out_shape=[payload] * 2 + [
            piece,
            pltpu.VMEM((halo, height), bf16),
            struct((4, tile_blocks.shape[0]), jnp.int32),
            pltpu.VMEM((height, channels), bf16),
            dense_type,
            tiles_type,
        ],
        in_specs=[SMEM, SMEM, HBM, HBM, HBM, HBM],
        out_specs=[VMEM] * 8,
        scratch_shapes=[
            pltpu.VMEM((neighbours, count), jnp.int32),
            pltpu.VMEM((2, tile_blocks.shape[0]), jnp.int32),
            pltpu.VMEM((halo // EDGE, EDGE), jnp.int32),
            pltpu.SemaphoreType.DMA((4,)),
        ],
        compiler_params=pltpu.CompilerParams(vmem_limit_bytes=16 * MIB),
        cost_estimate=pl.CostEstimate(
            flops=2 * halo * height * channels, bytes_accessed=2 * MIB, transcendentals=0),
    )(place, tile_count, in_hbm(send_rows[0]), in_hbm(tile_blocks.T), in_hbm(features),
      in_hbm(tile_values))
    got = chip_swaps(*sent)

    dense, _, recv_hot, built = pl.pallas_call(
        functools.partial(build_kernel, count, zeroed, loaded),
        out_shape=[
            dense_type,
            tiles_type,
            pltpu.VMEM((halo, halo), bf16),
            struct((halo // EDGE, EDGE), jnp.int32),
        ],
        in_specs=[SMEM, SMEM, SMEM, HBM, HBM, VMEM, VMEM],
        out_specs=[VMEM] * 4,
        input_output_aliases={5: 0, 6: 1},
        scratch_shapes=[
            pltpu.VMEM(recv_index.shape, jnp.int32),
            pltpu.SemaphoreType.DMA((2,)),
        ],
        compiler_params=pltpu.CompilerParams(vmem_limit_bytes=8 * MIB),
        cost_estimate=pl.CostEstimate(
            flops=4 * height * height * channels, bytes_accessed=24 * MIB, transcendentals=0),
    )(place, order, tile_count, in_hbm(recv_index), in_hbm(tile_values), on_chip(dense),
      on_chip(tiles))

    early = column_count // 3
    own, dense_a = pl.pallas_call(
        own_kernel,
        out_shape=[
            pltpu.VMEM((height, channels), f32),
            pltpu.HBM((early, height, EDGE), bf16),
        ],
        in_specs=[VMEM] * 2,
        out_specs=[VMEM, HBM],
        scratch_shapes=[pltpu.SemaphoreType.DMA],
        compiler_params=pltpu.CompilerParams(vmem_limit_bytes=8 * MIB),
        cost_estimate=pl.CostEstimate(
            flops=2 * height * height * channels, bytes_accessed=8 * MIB, transcendentals=0),
    )(on_chip(dense), on_chip(rows))

    relay_call = pl.pallas_call(
        relay_kernel,
        out_shape=payload,
        in_specs=[VMEM, SMEM] + [VMEM] * 3,
        out_specs=VMEM,
        compiler_params=pltpu.CompilerParams(vmem_limit_bytes=4 * MIB),
    )
    relay = relay_call(own, place, near, *got)
    got_core = core_swap(relay)

    z, stats, *sent, near, dense_b = pl.pallas_call(
        first_kernel,
        out_shape=[pltpu.VMEM(mixed.shape, bf16), pltpu.HBM(stats_type.shape, f32)]
        + [payload] * 2 + [piece, pltpu.HBM((column_count - early, height, EDGE), bf16)],
        in_specs=[SMEM] + [VMEM] * 8,
        out_specs=[VMEM, HBM] + [VMEM] * 3 + [HBM],
        scratch_shapes=[
            pltpu.VMEM((halo, channels), bf16),
            pltpu.VMEM((halo, channels), bf16),
            pltpu.VMEM((16, channels), f32),
            pltpu.VMEM(stats_type.shape, f32),
            pltpu.SemaphoreType.DMA((2,)),
        ],
        compiler_params=pltpu.CompilerParams(vmem_limit_bytes=12 * MIB),
        cost_estimate=pl.CostEstimate(
            flops=2 * height * halo * channels, bytes_accessed=16 * MIB, transcendentals=0),
    )(place, on_chip(recv_hot), got_core, *got, on_chip(dense), on_chip(own), layer_weight, on_chip(send_hot))
    got = chip_swaps(*sent)
    stats = from_peers(stats, PLANE)
    column_stats = struct((lax.axis_size(COLUMN), 2, channels), f32)
    total_call = pl.pallas_call(
        put_total,
        out_shape=pltpu.VMEM(column_stats.shape, f32),
        in_specs=[VMEM],
        out_specs=VMEM,
        compiler_params=pltpu.CompilerParams(vmem_limit_bytes=MIB),
    )
    stats = from_peers(total_call(stats), COLUMN)
    relay = relay_call(built, place, near, *got)
    got_core = core_swap(relay)

    chunk = 512
    z, stats = pl.pallas_call(
        functools.partial(second_kernel, total),
        out_shape=[pltpu.VMEM(mixed.shape, bf16), stats_type],
        in_specs=[SMEM] + [VMEM] * 8 + [HBM, HBM, VMEM],
        out_specs=[VMEM] * 2,
        scratch_shapes=[
            pltpu.VMEM((halo, channels), bf16),
            pltpu.VMEM((height + halo, channels), bf16),
            pltpu.VMEM((16, channels), f32),
            pltpu.VMEM((halo, halo), bf16),
            pltpu.VMEM((height // chunk, column_count, chunk, EDGE), bf16),
            pltpu.SemaphoreType.DMA((height // chunk, 2)),
        ],
        compiler_params=pltpu.CompilerParams(vmem_limit_bytes=28 * MIB),
        cost_estimate=pl.CostEstimate(
            flops=2 * height * (height + halo) * channels, bytes_accessed=16 * MIB,
            transcendentals=0),
    )(place, built, got_core, *got, on_chip(z), stats, norm_gain, norm_shift,
      in_hbm(dense_a), in_hbm(dense_b), layer_weight)
    stats = from_peers(stats, PLANE)
    stats = from_peers(total_call(stats), COLUMN)

    return pl.pallas_call(
        functools.partial(last_kernel, vertex_total),
        out_shape=mixed,
        in_specs=[VMEM] * 4,
        out_specs=VMEM,
        compiler_params=pltpu.CompilerParams(vmem_limit_bytes=16 * MIB),
    )(on_chip(z), stats, norm_gain, norm_shift)


def solution(mesh):
    finer = Mesh(mesh.devices.reshape(4, 4, 8, 2), PARTS)
    placed = (
        P(PARTS, None),
        P(PARTS, None, None),
        P(PARTS, None),
        P(PARTS),
        P(PARTS, None, None),
        P(PARTS, None),
        P(),
        P(),
        P(),
    )
    return jax.shard_map(
        shards, mesh=finer, in_specs=placed, out_specs=P(PARTS, None), check_vma=False
    )
```

```python
import functools

import jax
import jax.numpy as jnp
from jax import lax
from jax.experimental import pallas as pl
from jax.experimental.pallas import tpu as pltpu
from jax.sharding import Mesh
from jax.sharding import PartitionSpec as P


PARTS = ("parts_0", "parts_1", "parts_2", "parts_3")
PLANE = PARTS[:2]
COLUMN = PARTS[2:]
norm_eps = 1e-05
EDGE = 128
MIB = 1 << 20


def swap(value, first, stride, total):
    pairs = []
    for q in range(total - stride):
        if first(q):
            pairs += [(q, q + stride), (q + stride, q)]
    return lax.ppermute(value, PARTS, pairs)


def chip_swaps(to_c, to_d):
    total = lax.axis_size(PARTS)
    got_d = swap(to_d, lambda q: q % 4 >= 2, 2, total)
    got_c = swap(to_c, lambda q: q % 4 < 2, 2, total)
    return got_c, got_d


def core_swap(value):
    return swap(value, lambda q: q % 2 == 0, 1, lax.axis_size(PARTS))


def fill_one_hot(index_ref, one_hot_ref, groups):
    columns = one_hot_ref.shape[1]
    lanes = lax.broadcasted_iota(jnp.int32, (EDGE, EDGE), 1)
    for group in groups:
        row = jnp.broadcast_to(index_ref[pl.ds(group, 1), :], (EDGE, EDGE))
        away = row.T - lanes
        for block in range(columns // EDGE):
            one_hot_ref[pl.ds(group * EDGE, EDGE), pl.ds(block * EDGE, EDGE)] = jnp.where(
                away == block * EDGE, 1.0, 0.0
            ).astype(jnp.bfloat16)


def pick_piece(one_hot_ref, rows_ref, piece_ref, first, at, count):
    piece_ref[pl.ds(at, count), :] = jnp.dot(
        one_hot_ref[pl.ds(first, count), :], rows_ref[...], preferred_element_type=jnp.float32
    ).astype(jnp.bfloat16)


def spread(row):
    n = row.shape[1]
    return jnp.broadcast_to(row, (n, n)).T


def put_tile_order(blocks_ref, live_count, row_count, column_count, order_ref):
    tiles = blocks_ref.shape[1]
    number = lax.broadcasted_iota(jnp.int32, (1, tiles), 1)
    live = number < live_count
    row = jnp.where(live, blocks_ref[0:1, :], 0)
    column = jnp.where(live, blocks_ref[1:2, :], column_count)
    cell = column * row_count + row
    key = cell * tiles + number
    down = lax.broadcasted_iota(jnp.int32, (tiles, tiles), 0)
    cells_down = spread(cell)
    keys_down = cells_down * tiles + down
    rank = jnp.sum((keys_down < key).astype(jnp.int32), axis=0, keepdims=True)
    same = (cells_down == cell) & (down < number)
    keep = jnp.sum(same.astype(jnp.int32), axis=0, keepdims=True) > 0
    packed = (cell * 2 + keep.astype(jnp.int32)) * tiles + number
    hit = spread(rank) == number
    packed = jnp.sum(jnp.where(hit, spread(packed), 0), axis=0, keepdims=True)
    cell = packed // (2 * tiles)
    order_ref[0:1, :] = packed % tiles
    order_ref[1:2, :] = cell % row_count
    order_ref[2:3, :] = cell // row_count
    order_ref[3:4, :] = (packed // tiles) % 2


def put_zeros(dense_ref, first, last):
    size = 256
    zeros = jnp.zeros((size, dense_ref.shape[2]), dense_ref.dtype)

    @pl.loop(first, last)
    def _(c):
        for at in range(0, dense_ref.shape[1], size):
            dense_ref[c, pl.ds(at, size), :] = zeros


def gather_kernel(row_count, column_count, zeroed, loaded,
                  device_ref, live_ref, send_in, blocks_in, features_ref, tiles_in,
                  to_c, to_d, near_ref, one_hot_ref, order_ref, rows_ref, dense_ref, tiles_ref,
                  send_ref, blocks_ref, index_ref, arrived):
    load_send = pltpu.make_async_copy(send_in, send_ref, arrived.at[0])
    load_blocks = pltpu.make_async_copy(blocks_in, blocks_ref, arrived.at[1])
    load = pltpu.make_async_copy(features_ref, rows_ref, arrived.at[2])
    part = pl.ds(0, loaded)
    load_tiles = pltpu.make_async_copy(tiles_in.at[part], tiles_ref.at[part], arrived.at[3])
    load_send.start()
    load_blocks.start()
    load.start()
    load_tiles.start()
    put_zeros(dense_ref, 0, zeroed)
    load_send.wait()
    even_chip = device_ref[0] % 4 < 2
    count = send_ref.shape[1]
    per_piece = count // EDGE
    for part in range(per_piece):
        n0, n1, n2, n3 = (send_ref[n:n + 1, part * EDGE:(part + 1) * EDGE] for n in range(4))
        lists = (
            jnp.where(even_chip, n2, n3),
            jnp.where(even_chip, n0, n1),
            jnp.where(even_chip, n3, n2),
            jnp.where(even_chip, n1, n0),
        )
        for n, chosen in enumerate(lists):
            at = n * per_piece + part
            index_ref[at:at + 1, :] = chosen
    fill_one_hot(index_ref, one_hot_ref, range(2 * per_piece))
    load_blocks.wait()
    put_tile_order(blocks_ref, live_ref[0], row_count, column_count, order_ref)
    load.wait()
    pick_piece(one_hot_ref, rows_ref, to_c, 0, 0, count)
    fill_one_hot(index_ref, one_hot_ref, range(2 * per_piece, 3 * per_piece))
    pick_piece(one_hot_ref, rows_ref, to_c, count, count, count)
    fill_one_hot(index_ref, one_hot_ref, range(3 * per_piece, 4 * per_piece))
    pick_piece(one_hot_ref, rows_ref, to_d, 2 * count, 0, count)
    pick_piece(one_hot_ref, rows_ref, to_d, 3 * count, count, count)
    put_near(device_ref, to_c, to_d, near_ref, 0)
    load_tiles.wait()


def put_near(device_ref, from_c, from_d, out_ref, at):
    count = from_c.shape[0] // 2
    first = (device_ref[0] % 4 < 2) == (device_ref[0] % 2 == 0)

    @pl.when(first)
    def _():
        out_ref[at:at + count, :] = from_c[count:2 * count, :]

    @pl.when(jnp.logical_not(first))
    def _():
        out_ref[at:at + count, :] = from_d[count:2 * count, :]


def relay_kernel(after_ref, device_ref, near_ref, got_c, got_d, out_ref):
    del after_ref
    count = near_ref.shape[0]
    out_ref[0:count, :] = near_ref[...]
    put_near(device_ref, got_c, got_d, out_ref, count)


def put_total(parts_ref, out_ref):
    both = jnp.sum(parts_ref[...], axis=0)
    for n in range(out_ref.shape[0]):
        out_ref[n] = both


def adjacency_block(dense_ref, first, last, start, size):
    return jnp.concatenate(
        [dense_ref[c, pl.ds(start, size), :] for c in range(first, last)], axis=1
    )


def build_kernel(count, zeroed, loaded,
                 device_ref, order_ref, live_ref, recv_in, tiles_in, _dense, _tiles,
                 dense_ref, held_ref, recv_hot_ref, index_ref, recv_ref, arrived):
    part = pl.ds(loaded, held_ref.shape[0] - loaded)
    load_recv = pltpu.make_async_copy(recv_in, recv_ref, arrived.at[0])
    load = pltpu.make_async_copy(tiles_in.at[part], held_ref.at[part], arrived.at[1])
    load_recv.start()
    load.start()
    unroll = 8
    put_zeros(dense_ref, zeroed, dense_ref.shape[0])

    near = jnp.where(device_ref[0] % 2 == 0, count, 0)
    far = jnp.where(device_ref[0] % 4 < 2, count, 0)
    load_recv.wait()
    for group in range(index_ref.shape[0]):
        rows = recv_ref[0:1, group * EDGE:(group + 1) * EDGE]
        index_ref[group:group + 1, :] = rows ^ jnp.where(rows < 2 * count, near, far)
    fill_one_hot(index_ref, recv_hot_ref, range(index_ref.shape[0]))
    load.wait()

    def step(turn, total):
        for u in range(unroll):
            k = turn * unroll + u
            tile = held_ref[order_ref[0, k]].astype(jnp.float32)
            total = total * order_ref[3, k].astype(jnp.float32) + tile
            start = pl.multiple_of(order_ref[1, k] * EDGE, EDGE)
            dense_ref[order_ref[2, k], pl.ds(start, EDGE), :] = total.astype(jnp.bfloat16)
        return total

    lax.fori_loop(
        0, (live_ref[0] + unroll - 1) // unroll, step, jnp.zeros((EDGE, EDGE), jnp.float32)
    )


def put_own(dense_ref, rows_ref, own_ref, first, last):
    own_blocks = own_ref.shape[0] // EDGE
    size = 512
    for start in range(first, last, size):
        own_ref[pl.ds(start, size), :] = jnp.dot(
            adjacency_block(dense_ref, 0, own_blocks, start, size),
            rows_ref[...],
            preferred_element_type=jnp.float32,
        )


def own_upper_kernel(dense_ref, rows_ref, own_ref, dense_out, left):
    store = pltpu.make_async_copy(
        dense_ref.at[pl.ds(0, dense_out.shape[0])], dense_out, left
    )
    store.start()
    put_own(dense_ref, rows_ref, own_ref, 0, own_ref.shape[0] // 2)
    store.wait()


def own_lower_kernel(after_ref, _own, dense_ref, rows_ref, own_ref):
    del after_ref
    height = own_ref.shape[0]
    put_own(dense_ref, rows_ref, own_ref, height // 2, height)


def add_moments(z, moment_ref):
    wide = z.astype(jnp.float32)
    moment_ref[0:8, :] += jnp.sum(wide.reshape(-1, 8, wide.shape[1]), axis=0)
    moment_ref[8:16, :] += jnp.sum(jnp.square(wide).reshape(-1, 8, wide.shape[1]), axis=0)


def put_moments(moment_ref, out_ref):
    both = jnp.concatenate(
        [
            jnp.sum(moment_ref[0:8, :], axis=0, keepdims=True),
            jnp.sum(moment_ref[8:16, :], axis=0, keepdims=True),
        ],
        axis=0,
    )
    for n in range(out_ref.shape[0]):
        out_ref[n] = both


def received(a, c, d):
    count = a.shape[0] // 2
    return a[0:count, :], a[count:2 * count, :], c[0:count, :], d[0:count, :]


def first_kernel(device_ref, recv_hot_ref, a, c, d, dense_ref, own_ref, weight_ref, send_hot_ref,
                 z_ref, stats_out, to_c, to_d, near_ref, dense_out,
                 halo_ref, got_ref, moment_ref, stats_ref, left):
    layer = 0
    count = a.shape[0] // 2
    written = own_ref.shape[0] // EDGE + 4 * count // EDGE - dense_out.shape[0]
    store = pltpu.make_async_copy(
        dense_ref.at[pl.ds(written, dense_out.shape[0])], dense_out, left.at[0]
    )
    store.start()
    for n, piece in enumerate(received(a, c, d)):
        got_ref[pl.ds(n * count, count), :] = piece
    halo_ref[...] = jnp.dot(
        recv_hot_ref[...], got_ref[...], preferred_element_type=jnp.float32
    ).astype(jnp.bfloat16)
    moment_ref[...] = jnp.zeros_like(moment_ref)
    height = z_ref.shape[0]
    own_blocks, halo_blocks = height // EDGE, halo_ref.shape[0] // EDGE
    size = 512

    @pl.loop(0, height // size)
    def _(m):
        start = pl.multiple_of(m * size, size)
        agg = own_ref[pl.ds(start, size), :] + jnp.dot(
            adjacency_block(dense_ref, own_blocks, own_blocks + halo_blocks, start, size),
            halo_ref[...],
            preferred_element_type=jnp.float32,
        )
        z = jnp.dot(
            agg.astype(jnp.bfloat16), weight_ref[layer], preferred_element_type=jnp.float32
        ).astype(jnp.bfloat16)
        z_ref[pl.ds(start, size), :] = z
        add_moments(z, moment_ref)

    put_moments(moment_ref, stats_ref)
    size = to_c.shape[0]
    pick_piece(send_hot_ref, z_ref, to_c, 0, 0, size)
    store_stats = pltpu.make_async_copy(stats_ref, stats_out, left.at[1])
    store_stats.start()
    pick_piece(send_hot_ref, z_ref, to_d, size, 0, size)
    put_near(device_ref, to_c, to_d, near_ref, 0)
    store.wait()
    store_stats.wait()


def scale_of(stats_ref, gain_ref, shift_ref, layer, vertex_total):
    both = jnp.sum(stats_ref[...], axis=0) / vertex_total
    centre = both[0:1, :]
    spread = both[1:2, :] - jnp.square(centre)
    factor = gain_ref[layer:layer + 1, :] / jnp.sqrt(spread + norm_eps)
    return centre, factor, shift_ref[layer:layer + 1, :]


def normal(rows, terms):
    centre, factor, shift = terms
    return jnp.maximum((rows.astype(jnp.float32) - centre) * factor + shift, 0.0)


def second_kernel(device_total, device_ref, index_ref, a, c, d, mixed_ref, stats_in_ref,
                  gain_ref, shift_ref, dense_a, dense_b, weight_ref, z_ref, stats_ref,
                  got_ref, columns_ref, moment_ref, recv_hot_ref, dense_ref, arrived):
    layer = 1
    count = a.shape[0] // 2
    height = z_ref.shape[0]
    halo = 4 * count
    blocks = (height + halo) // EDGE
    size = dense_ref.shape[2]


    def loads(m):
        rows, at, found = pl.ds(pl.multiple_of(m * size, size), size), 0, []
        for n, part in enumerate((dense_a, dense_b)):
            found.append(pltpu.make_async_copy(
                part.at[:, rows, :], dense_ref.at[m, pl.ds(at, part.shape[0])], arrived.at[m, n]
            ))
            at += part.shape[0]
        return found

    for m in range(height // size):
        for load in loads(m):
            load.start()
    terms = scale_of(stats_in_ref, gain_ref, shift_ref, 0, device_total * height)
    device = device_ref[0]
    near_side = (device > 0) & (device < device_total - 1)
    far_side = (device > 1) & (device < device_total - 2)
    present = (1.0, near_side.astype(jnp.float32), 1.0, far_side.astype(jnp.float32))
    for n, piece in enumerate(received(a, c, d)):
        got_ref[pl.ds(n * count, count), :] = (
            normal(piece, terms) * present[n]
        ).astype(jnp.bfloat16)
    for part in range(8):
        rows = pl.ds(part * (height // 8), height // 8)
        columns_ref[rows, :] = normal(mixed_ref[rows, :], terms).astype(jnp.bfloat16)
    fill_one_hot(index_ref, recv_hot_ref, range(index_ref.shape[0]))
    columns_ref[pl.ds(height, halo), :] = jnp.dot(
        recv_hot_ref[...], got_ref[...], preferred_element_type=jnp.float32
    ).astype(jnp.bfloat16)
    moment_ref[...] = jnp.zeros_like(moment_ref)

    @pl.loop(0, height // size)
    def _(m):
        for load in loads(m):
            load.wait()
        start = pl.multiple_of(m * size, size)
        agg = jnp.dot(
            jnp.concatenate([dense_ref[m, c] for c in range(blocks)], axis=1),
            columns_ref[...],
            preferred_element_type=jnp.float32,
        )
        z = jnp.dot(
            agg.astype(jnp.bfloat16), weight_ref[layer], preferred_element_type=jnp.float32
        ).astype(jnp.bfloat16)
        z_ref[pl.ds(start, size), :] = z
        add_moments(z, moment_ref)

    put_moments(moment_ref, stats_ref)


def last_kernel(vertex_total, mixed_ref, stats_in_ref, gain_ref, shift_ref, out_ref):
    terms = scale_of(stats_in_ref, gain_ref, shift_ref, 1, vertex_total)
    out_ref[...] = normal(mixed_ref[...], terms).astype(jnp.bfloat16)


VMEM = pl.BlockSpec(memory_space=pltpu.VMEM)
SMEM = pl.BlockSpec(memory_space=pltpu.SMEM)
HBM = pl.BlockSpec(memory_space=pltpu.HBM)


def from_peers(stats, axes):
    return lax.all_to_all(stats, axes, 0, 0, tiled=True)


def shards(features, tile_values, tile_blocks, tile_count, send_rows, recv_index,
           layer_weight, norm_gain, norm_shift):
    height, channels = features.shape
    neighbours, count = send_rows.shape[1:]
    halo = neighbours * count
    row_count = height // EDGE
    column_count = (height + halo) // EDGE
    device = lax.axis_index(PARTS)
    total = lax.axis_size(PARTS)
    vertex_total = height * total
    peers = lax.axis_size(PLANE)
    bf16, f32 = jnp.bfloat16, jnp.float32
    struct = jax.ShapeDtypeStruct
    piece = struct((count, channels), bf16)
    payload = struct((2 * count, channels), bf16)
    stats_type = struct((peers, 2, channels), f32)
    mixed = struct((height, channels), bf16)

    place = device.reshape(1)

    def on_chip(value):
        return pltpu.with_memory_space_constraint(value, pltpu.VMEM)

    def in_hbm(value):
        return pltpu.with_memory_space_constraint(value, pltpu.HBM)

    zeroed, loaded = column_count // 6, tile_values.shape[0] * 3 // 8
    dense_type = pltpu.VMEM((column_count + 1, height, EDGE), bf16)
    tiles_type = pltpu.VMEM(tile_values.shape, bf16)
    *sent, near, send_hot, order, rows, dense, tiles = pl.pallas_call(
        functools.partial(gather_kernel, row_count, column_count, zeroed, loaded),
        out_shape=[payload] * 2 + [
            piece,
            pltpu.VMEM((halo, height), bf16),
            struct((4, tile_blocks.shape[0]), jnp.int32),
            pltpu.VMEM((height, channels), bf16),
            dense_type,
            tiles_type,
        ],
        in_specs=[SMEM, SMEM, HBM, HBM, HBM, HBM],
        out_specs=[VMEM] * 8,
        scratch_shapes=[
            pltpu.VMEM((neighbours, count), jnp.int32),
            pltpu.VMEM((2, tile_blocks.shape[0]), jnp.int32),
            pltpu.VMEM((halo // EDGE, EDGE), jnp.int32),
            pltpu.SemaphoreType.DMA((4,)),
        ],
        compiler_params=pltpu.CompilerParams(vmem_limit_bytes=16 * MIB),
        cost_estimate=pl.CostEstimate(
            flops=2 * halo * height * channels, bytes_accessed=2 * MIB, transcendentals=0),
    )(place, tile_count, in_hbm(send_rows[0]), in_hbm(tile_blocks.T), in_hbm(features),
      in_hbm(tile_values))
    got = chip_swaps(*sent)

    dense, _, recv_hot, built = pl.pallas_call(
        functools.partial(build_kernel, count, zeroed, loaded),
        out_shape=[
            dense_type,
            tiles_type,
            pltpu.VMEM((halo, halo), bf16),
            struct((halo // EDGE, EDGE), jnp.int32),
        ],
        in_specs=[SMEM, SMEM, SMEM, HBM, HBM, VMEM, VMEM],
        out_specs=[VMEM] * 4,
        input_output_aliases={5: 0, 6: 1},
        scratch_shapes=[
            pltpu.VMEM(recv_index.shape, jnp.int32),
            pltpu.SemaphoreType.DMA((2,)),
        ],
        compiler_params=pltpu.CompilerParams(vmem_limit_bytes=8 * MIB),
        cost_estimate=pl.CostEstimate(
            flops=4 * height * height * channels, bytes_accessed=24 * MIB, transcendentals=0),
    )(place, order, tile_count, in_hbm(recv_index), in_hbm(tile_values), on_chip(dense),
      on_chip(tiles))

    early = column_count // 4
    own, dense_a = pl.pallas_call(
        own_upper_kernel,
        out_shape=[
            pltpu.VMEM((height, channels), f32),
            pltpu.HBM((early, height, EDGE), bf16),
        ],
        in_specs=[VMEM] * 2,
        out_specs=[VMEM, HBM],
        scratch_shapes=[pltpu.SemaphoreType.DMA],
        compiler_params=pltpu.CompilerParams(vmem_limit_bytes=8 * MIB),
        cost_estimate=pl.CostEstimate(
            flops=height * height * channels, bytes_accessed=8 * MIB, transcendentals=0),
    )(on_chip(dense), on_chip(rows))

    relay_call = pl.pallas_call(
        relay_kernel,
        out_shape=payload,
        in_specs=[VMEM, SMEM] + [VMEM] * 3,
        out_specs=VMEM,
        compiler_params=pltpu.CompilerParams(vmem_limit_bytes=4 * MIB),
    )
    relay = relay_call(own, place, near, *got)
    got_core = core_swap(relay)

    own = pl.pallas_call(
        own_lower_kernel,
        out_shape=pltpu.VMEM((height, channels), f32),
        in_specs=[VMEM] * 4,
        out_specs=VMEM,
        input_output_aliases={1: 0},
        compiler_params=pltpu.CompilerParams(vmem_limit_bytes=8 * MIB),
        cost_estimate=pl.CostEstimate(
            flops=height * height * channels, bytes_accessed=8 * MIB, transcendentals=0),
    )(relay, on_chip(own), on_chip(dense), on_chip(rows))

    z, stats, *sent, near, dense_b = pl.pallas_call(
        first_kernel,
        out_shape=[pltpu.VMEM(mixed.shape, bf16), pltpu.HBM(stats_type.shape, f32)]
        + [payload] * 2 + [piece, pltpu.HBM((column_count - early, height, EDGE), bf16)],
        in_specs=[SMEM] + [VMEM] * 8,
        out_specs=[VMEM, HBM] + [VMEM] * 3 + [HBM],
        scratch_shapes=[
            pltpu.VMEM((halo, channels), bf16),
            pltpu.VMEM((halo, channels), bf16),
            pltpu.VMEM((16, channels), f32),
            pltpu.VMEM(stats_type.shape, f32),
            pltpu.SemaphoreType.DMA((2,)),
        ],
        compiler_params=pltpu.CompilerParams(vmem_limit_bytes=12 * MIB),
        cost_estimate=pl.CostEstimate(
            flops=2 * height * halo * channels, bytes_accessed=16 * MIB, transcendentals=0),
    )(place, on_chip(recv_hot), got_core, *got, on_chip(dense), on_chip(own), layer_weight, on_chip(send_hot))
    got = chip_swaps(*sent)
    stats = from_peers(stats, PLANE)
    column_stats = struct((lax.axis_size(COLUMN), 2, channels), f32)
    total_call = pl.pallas_call(
        put_total,
        out_shape=pltpu.VMEM(column_stats.shape, f32),
        in_specs=[VMEM],
        out_specs=VMEM,
        compiler_params=pltpu.CompilerParams(vmem_limit_bytes=MIB),
    )
    stats = from_peers(total_call(stats), COLUMN)
    relay = relay_call(built, place, near, *got)
    got_core = core_swap(relay)

    chunk = 512
    z, stats = pl.pallas_call(
        functools.partial(second_kernel, total),
        out_shape=[pltpu.VMEM(mixed.shape, bf16), stats_type],
        in_specs=[SMEM] + [VMEM] * 8 + [HBM, HBM, VMEM],
        out_specs=[VMEM] * 2,
        scratch_shapes=[
            pltpu.VMEM((halo, channels), bf16),
            pltpu.VMEM((height + halo, channels), bf16),
            pltpu.VMEM((16, channels), f32),
            pltpu.VMEM((halo, halo), bf16),
            pltpu.VMEM((height // chunk, column_count, chunk, EDGE), bf16),
            pltpu.SemaphoreType.DMA((height // chunk, 2)),
        ],
        compiler_params=pltpu.CompilerParams(vmem_limit_bytes=28 * MIB),
        cost_estimate=pl.CostEstimate(
            flops=2 * height * (height + halo) * channels, bytes_accessed=16 * MIB,
            transcendentals=0),
    )(place, built, got_core, *got, on_chip(z), stats, norm_gain, norm_shift,
      in_hbm(dense_a), in_hbm(dense_b), layer_weight)
    stats = from_peers(stats, PLANE)
    stats = from_peers(total_call(stats), COLUMN)

    return pl.pallas_call(
        functools.partial(last_kernel, vertex_total),
        out_shape=mixed,
        in_specs=[VMEM] * 4,
        out_specs=VMEM,
        compiler_params=pltpu.CompilerParams(vmem_limit_bytes=16 * MIB),
    )(on_chip(z), stats, norm_gain, norm_shift)


def solution(mesh):
    finer = Mesh(mesh.devices.reshape(4, 4, 8, 2), PARTS)
    placed = (
        P(PARTS, None),
        P(PARTS, None, None),
        P(PARTS, None),
        P(PARTS),
        P(PARTS, None, None),
        P(PARTS, None),
        P(),
        P(),
        P(),
    )
    return jax.shard_map(
        shards, mesh=finer, in_specs=placed, out_specs=P(PARTS, None), check_vma=False
    )
```

```python
import functools

import jax
import jax.numpy as jnp
from jax import lax
from jax.experimental import pallas as pl
from jax.experimental.pallas import tpu as pltpu
from jax.sharding import Mesh
from jax.sharding import PartitionSpec as P


PARTS = ("parts_0", "parts_1", "parts_2", "parts_3")
PLANE = PARTS[:2]
COLUMN = PARTS[2:]
norm_eps = 1e-05
EDGE = 128
MIB = 1 << 20


def swap(value, first, stride, total):
    pairs = []
    for q in range(total - stride):
        if first(q):
            pairs += [(q, q + stride), (q + stride, q)]
    return lax.ppermute(value, PARTS, pairs)


def chip_swaps(to_c, to_d):
    total = lax.axis_size(PARTS)
    got_d = swap(to_d, lambda q: q % 4 >= 2, 2, total)
    got_c = swap(to_c, lambda q: q % 4 < 2, 2, total)
    return got_c, got_d


def core_swap(value):
    return swap(value, lambda q: q % 2 == 0, 1, lax.axis_size(PARTS))


def fill_one_hot(index_ref, one_hot_ref, groups):
    columns = one_hot_ref.shape[1]
    lanes = lax.broadcasted_iota(jnp.int32, (EDGE, EDGE), 1)
    for group in groups:
        row = jnp.broadcast_to(index_ref[pl.ds(group, 1), :], (EDGE, EDGE))
        away = row.T - lanes
        for block in range(columns // EDGE):
            one_hot_ref[pl.ds(group * EDGE, EDGE), pl.ds(block * EDGE, EDGE)] = jnp.where(
                away == block * EDGE, 1.0, 0.0
            ).astype(jnp.bfloat16)


def pick_piece(one_hot_ref, rows_ref, piece_ref, first, at, count):
    piece_ref[pl.ds(at, count), :] = jnp.dot(
        one_hot_ref[pl.ds(first, count), :], rows_ref[...], preferred_element_type=jnp.float32
    ).astype(jnp.bfloat16)


def spread(row):
    n = row.shape[1]
    return jnp.broadcast_to(row, (n, n)).T


def put_tile_order(blocks_ref, live_count, row_count, column_count, order_ref):
    tiles = blocks_ref.shape[1]
    number = lax.broadcasted_iota(jnp.int32, (1, tiles), 1)
    live = number < live_count
    row = jnp.where(live, blocks_ref[0:1, :], 0)
    column = jnp.where(live, blocks_ref[1:2, :], column_count)
    cell = column * row_count + row
    key = cell * tiles + number
    down = lax.broadcasted_iota(jnp.int32, (tiles, tiles), 0)
    cells_down = spread(cell)
    keys_down = cells_down * tiles + down
    rank = jnp.sum((keys_down < key).astype(jnp.int32), axis=0, keepdims=True)
    same = (cells_down == cell) & (down < number)
    keep = jnp.sum(same.astype(jnp.int32), axis=0, keepdims=True) > 0
    packed = (cell * 2 + keep.astype(jnp.int32)) * tiles + number
    hit = spread(rank) == number
    packed = jnp.sum(jnp.where(hit, spread(packed), 0), axis=0, keepdims=True)
    cell = packed // (2 * tiles)
    order_ref[0:1, :] = packed % tiles
    order_ref[1:2, :] = cell % row_count
    order_ref[2:3, :] = cell // row_count
    order_ref[3:4, :] = (packed // tiles) % 2


def put_zeros(dense_ref, first, last):
    size = 256
    zeros = jnp.zeros((size, dense_ref.shape[2]), dense_ref.dtype)

    @pl.loop(first, last)
    def _(c):
        for at in range(0, dense_ref.shape[1], size):
            dense_ref[c, pl.ds(at, size), :] = zeros


def gather_kernel(row_count, column_count, zeroed, loaded,
                  device_ref, live_ref, send_in, blocks_in, features_ref, tiles_in,
                  to_c, to_d, near_ref, one_hot_ref, order_ref, rows_ref, dense_ref, tiles_ref,
                  send_ref, blocks_ref, index_ref, arrived):
    load_send = pltpu.make_async_copy(send_in, send_ref, arrived.at[0])
    load_blocks = pltpu.make_async_copy(blocks_in, blocks_ref, arrived.at[1])
    load = pltpu.make_async_copy(features_ref, rows_ref, arrived.at[2])
    part = pl.ds(0, loaded)
    load_tiles = pltpu.make_async_copy(tiles_in.at[part], tiles_ref.at[part], arrived.at[3])
    load_send.start()
    load_blocks.start()
    load.start()
    load_tiles.start()
    put_zeros(dense_ref, 0, zeroed)
    load_send.wait()
    even_chip = device_ref[0] % 4 < 2
    count = send_ref.shape[1]
    per_piece = count // EDGE
    for part in range(per_piece):
        n0, n1, n2, n3 = (send_ref[n:n + 1, part * EDGE:(part + 1) * EDGE] for n in range(4))
        lists = (
            jnp.where(even_chip, n2, n3),
            jnp.where(even_chip, n0, n1),
            jnp.where(even_chip, n3, n2),
            jnp.where(even_chip, n1, n0),
        )
        for n, chosen in enumerate(lists):
            at = n * per_piece + part
            index_ref[at:at + 1, :] = chosen
    fill_one_hot(index_ref, one_hot_ref, range(2 * per_piece))
    load_blocks.wait()
    put_tile_order(blocks_ref, live_ref[0], row_count, column_count, order_ref)
    load.wait()
    pick_piece(one_hot_ref, rows_ref, to_c, 0, 0, count)
    fill_one_hot(index_ref, one_hot_ref, range(2 * per_piece, 3 * per_piece))
    pick_piece(one_hot_ref, rows_ref, to_c, count, count, count)
    fill_one_hot(index_ref, one_hot_ref, range(3 * per_piece, 4 * per_piece))
    pick_piece(one_hot_ref, rows_ref, to_d, 2 * count, 0, count)
    pick_piece(one_hot_ref, rows_ref, to_d, 3 * count, count, count)
    put_near(device_ref, to_c, to_d, near_ref, 0)
    load_tiles.wait()


def put_near(device_ref, from_c, from_d, out_ref, at):
    count = from_c.shape[0] // 2
    first = (device_ref[0] % 4 < 2) == (device_ref[0] % 2 == 0)

    @pl.when(first)
    def _():
        out_ref[at:at + count, :] = from_c[count:2 * count, :]

    @pl.when(jnp.logical_not(first))
    def _():
        out_ref[at:at + count, :] = from_d[count:2 * count, :]


def relay_kernel(after_ref, device_ref, near_ref, got_c, got_d, out_ref):
    del after_ref
    count = near_ref.shape[0]
    out_ref[0:count, :] = near_ref[...]
    put_near(device_ref, got_c, got_d, out_ref, count)


def put_total(parts_ref, out_ref):
    both = jnp.sum(parts_ref[...], axis=0)
    for n in range(out_ref.shape[0]):
        out_ref[n] = both


def adjacency_block(dense_ref, first, last, start, size):
    return jnp.concatenate(
        [dense_ref[c, pl.ds(start, size), :] for c in range(first, last)], axis=1
    )


def build_kernel(count, zeroed, loaded,
                 device_ref, order_ref, live_ref, recv_in, tiles_in, _dense, _tiles,
                 dense_ref, held_ref, recv_hot_ref, index_ref, recv_ref, arrived):
    part = pl.ds(loaded, held_ref.shape[0] - loaded)
    load_recv = pltpu.make_async_copy(recv_in, recv_ref, arrived.at[0])
    load = pltpu.make_async_copy(tiles_in.at[part], held_ref.at[part], arrived.at[1])
    load_recv.start()
    load.start()
    unroll = 8
    put_zeros(dense_ref, zeroed, dense_ref.shape[0])

    near = jnp.where(device_ref[0] % 2 == 0, count, 0)
    far = jnp.where(device_ref[0] % 4 < 2, count, 0)
    load_recv.wait()
    for group in range(index_ref.shape[0]):
        rows = recv_ref[0:1, group * EDGE:(group + 1) * EDGE]
        index_ref[group:group + 1, :] = rows ^ jnp.where(rows < 2 * count, near, far)
    fill_one_hot(index_ref, recv_hot_ref, range(index_ref.shape[0]))
    load.wait()

    def step(turn, total):
        for u in range(unroll):
            k = turn * unroll + u
            tile = held_ref[order_ref[0, k]].astype(jnp.float32)
            total = total * order_ref[3, k].astype(jnp.float32) + tile
            start = pl.multiple_of(order_ref[1, k] * EDGE, EDGE)
            dense_ref[order_ref[2, k], pl.ds(start, EDGE), :] = total.astype(jnp.bfloat16)
        return total

    lax.fori_loop(
        0, (live_ref[0] + unroll - 1) // unroll, step, jnp.zeros((EDGE, EDGE), jnp.float32)
    )


def put_own(dense_ref, rows_ref, own_ref, first, last):
    own_blocks = own_ref.shape[0] // EDGE
    size = 512
    for start in range(first, last, size):
        own_ref[pl.ds(start, size), :] = jnp.dot(
            adjacency_block(dense_ref, 0, own_blocks, start, size),
            rows_ref[...],
            preferred_element_type=jnp.float32,
        )


def own_upper_kernel(dense_ref, rows_ref, own_ref, dense_out, left):
    store = pltpu.make_async_copy(
        dense_ref.at[pl.ds(0, dense_out.shape[0])], dense_out, left
    )
    store.start()
    put_own(dense_ref, rows_ref, own_ref, 0, own_ref.shape[0] // 2)
    store.wait()


def own_lower_kernel(after_ref, _own, dense_ref, rows_ref, own_ref):
    del after_ref
    height = own_ref.shape[0]
    put_own(dense_ref, rows_ref, own_ref, height // 2, height)


def add_moments(z, moment_ref):
    wide = z.astype(jnp.float32)
    moment_ref[0:8, :] += jnp.sum(wide.reshape(-1, 8, wide.shape[1]), axis=0)
    moment_ref[8:16, :] += jnp.sum(jnp.square(wide).reshape(-1, 8, wide.shape[1]), axis=0)


def put_moments(moment_ref, out_ref):
    both = jnp.concatenate(
        [
            jnp.sum(moment_ref[0:8, :], axis=0, keepdims=True),
            jnp.sum(moment_ref[8:16, :], axis=0, keepdims=True),
        ],
        axis=0,
    )
    for n in range(out_ref.shape[0]):
        out_ref[n] = both


def received(a, c, d):
    count = a.shape[0] // 2
    return a[0:count, :], a[count:2 * count, :], c[0:count, :], d[0:count, :]


def first_kernel(device_ref, recv_hot_ref, a, c, d, dense_ref, own_ref, weight_ref, send_hot_ref,
                 z_ref, stats_out, to_c, to_d, near_ref, dense_out,
                 halo_ref, got_ref, moment_ref, stats_ref, left):
    layer = 0
    count = a.shape[0] // 2
    written = own_ref.shape[0] // EDGE + 4 * count // EDGE - dense_out.shape[0]
    store = pltpu.make_async_copy(
        dense_ref.at[pl.ds(written, dense_out.shape[0])], dense_out, left.at[0]
    )
    store.start()
    for n, piece in enumerate(received(a, c, d)):
        got_ref[pl.ds(n * count, count), :] = piece
    halo_ref[...] = jnp.dot(
        recv_hot_ref[...], got_ref[...], preferred_element_type=jnp.float32
    ).astype(jnp.bfloat16)
    moment_ref[...] = jnp.zeros_like(moment_ref)
    height = z_ref.shape[0]
    own_blocks, halo_blocks = height // EDGE, halo_ref.shape[0] // EDGE
    size = 512

    @pl.loop(0, height // size)
    def _(m):
        start = pl.multiple_of(m * size, size)
        agg = own_ref[pl.ds(start, size), :] + jnp.dot(
            adjacency_block(dense_ref, own_blocks, own_blocks + halo_blocks, start, size),
            halo_ref[...],
            preferred_element_type=jnp.float32,
        )
        z = jnp.dot(
            agg.astype(jnp.bfloat16), weight_ref[layer], preferred_element_type=jnp.float32
        ).astype(jnp.bfloat16)
        z_ref[pl.ds(start, size), :] = z
        add_moments(z, moment_ref)

    put_moments(moment_ref, stats_ref)
    size = to_c.shape[0]
    pick_piece(send_hot_ref, z_ref, to_c, 0, 0, size)
    store_stats = pltpu.make_async_copy(stats_ref, stats_out, left.at[1])
    store_stats.start()
    pick_piece(send_hot_ref, z_ref, to_d, size, 0, size)
    put_near(device_ref, to_c, to_d, near_ref, 0)
    store.wait()
    store_stats.wait()


def scale_of(stats_ref, gain_ref, shift_ref, layer, vertex_total):
    both = jnp.sum(stats_ref[...], axis=0) / vertex_total
    centre = both[0:1, :]
    spread = both[1:2, :] - jnp.square(centre)
    factor = gain_ref[layer:layer + 1, :] / jnp.sqrt(spread + norm_eps)
    return centre, factor, shift_ref[layer:layer + 1, :]


def normal(rows, terms):
    centre, factor, shift = terms
    return jnp.maximum((rows.astype(jnp.float32) - centre) * factor + shift, 0.0)


def second_kernel(device_total, device_ref, index_ref, a, c, d, mixed_ref, stats_in_ref,
                  gain_ref, shift_ref, dense_a, dense_b, weight_ref, z_ref, stats_ref,
                  got_ref, columns_ref, moment_ref, recv_hot_ref, dense_ref, arrived):
    layer = 1
    count = a.shape[0] // 2
    height = z_ref.shape[0]
    halo = 4 * count
    blocks = (height + halo) // EDGE
    size = dense_ref.shape[2]


    def loads(m):
        rows, at, found = pl.ds(pl.multiple_of(m * size, size), size), 0, []
        for n, part in enumerate((dense_a, dense_b)):
            found.append(pltpu.make_async_copy(
                part.at[:, rows, :], dense_ref.at[m, pl.ds(at, part.shape[0])], arrived.at[m, n]
            ))
            at += part.shape[0]
        return found

    for m in range(height // size):
        for load in loads(m):
            load.start()
    terms = scale_of(stats_in_ref, gain_ref, shift_ref, 0, device_total * height)
    device = device_ref[0]
    near_side = (device > 0) & (device < device_total - 1)
    far_side = (device > 1) & (device < device_total - 2)
    present = (1.0, near_side.astype(jnp.float32), 1.0, far_side.astype(jnp.float32))
    for n, piece in enumerate(received(a, c, d)):
        got_ref[pl.ds(n * count, count), :] = (
            normal(piece, terms) * present[n]
        ).astype(jnp.bfloat16)
    for part in range(8):
        rows = pl.ds(part * (height // 8), height // 8)
        columns_ref[rows, :] = normal(mixed_ref[rows, :], terms).astype(jnp.bfloat16)
    fill_one_hot(index_ref, recv_hot_ref, range(index_ref.shape[0]))
    columns_ref[pl.ds(height, halo), :] = jnp.dot(
        recv_hot_ref[...], got_ref[...], preferred_element_type=jnp.float32
    ).astype(jnp.bfloat16)
    moment_ref[...] = jnp.zeros_like(moment_ref)

    @pl.loop(0, height // size)
    def _(m):
        for load in loads(m):
            load.wait()
        start = pl.multiple_of(m * size, size)
        agg = jnp.dot(
            jnp.concatenate([dense_ref[m, c] for c in range(blocks)], axis=1),
            columns_ref[...],
            preferred_element_type=jnp.float32,
        )
        z = jnp.dot(
            agg.astype(jnp.bfloat16), weight_ref[layer], preferred_element_type=jnp.float32
        ).astype(jnp.bfloat16)
        z_ref[pl.ds(start, size), :] = z
        add_moments(z, moment_ref)

    put_moments(moment_ref, stats_ref)


def last_kernel(vertex_total, mixed_ref, stats_in_ref, gain_ref, shift_ref, out_ref, held_ref, left):
    terms = scale_of(stats_in_ref, gain_ref, shift_ref, 1, vertex_total)
    parts = left.shape[0]
    size = out_ref.shape[0] // parts
    stores = []
    for part in range(parts):
        rows = pl.ds(part * size, size)
        held_ref[rows, :] = normal(mixed_ref[rows, :], terms).astype(jnp.bfloat16)
        stores.append(pltpu.make_async_copy(held_ref.at[rows], out_ref.at[rows], left.at[part]))
        if part:
            stores[part - 1].start()
    stores[-1].start()
    for store in stores:
        store.wait()


VMEM = pl.BlockSpec(memory_space=pltpu.VMEM)
SMEM = pl.BlockSpec(memory_space=pltpu.SMEM)
HBM = pl.BlockSpec(memory_space=pltpu.HBM)


def from_peers(stats, axes):
    return lax.all_to_all(stats, axes, 0, 0, tiled=True)


def shards(features, tile_values, tile_blocks, tile_count, send_rows, recv_index,
           layer_weight, norm_gain, norm_shift):
    height, channels = features.shape
    neighbours, count = send_rows.shape[1:]
    halo = neighbours * count
    row_count = height // EDGE
    column_count = (height + halo) // EDGE
    device = lax.axis_index(PARTS)
    total = lax.axis_size(PARTS)
    vertex_total = height * total
    peers = lax.axis_size(PLANE)
    bf16, f32 = jnp.bfloat16, jnp.float32
    struct = jax.ShapeDtypeStruct
    piece = struct((count, channels), bf16)
    payload = struct((2 * count, channels), bf16)
    stats_type = struct((peers, 2, channels), f32)
    mixed = struct((height, channels), bf16)

    place = device.reshape(1)

    def on_chip(value):
        return pltpu.with_memory_space_constraint(value, pltpu.VMEM)

    def in_hbm(value):
        return pltpu.with_memory_space_constraint(value, pltpu.HBM)

    zeroed, loaded = column_count // 6, tile_values.shape[0] * 3 // 8
    dense_type = pltpu.VMEM((column_count + 1, height, EDGE), bf16)
    tiles_type = pltpu.VMEM(tile_values.shape, bf16)
    *sent, near, send_hot, order, rows, dense, tiles = pl.pallas_call(
        functools.partial(gather_kernel, row_count, column_count, zeroed, loaded),
        out_shape=[payload] * 2 + [
            piece,
            pltpu.VMEM((halo, height), bf16),
            struct((4, tile_blocks.shape[0]), jnp.int32),
            pltpu.VMEM((height, channels), bf16),
            dense_type,
            tiles_type,
        ],
        in_specs=[SMEM, SMEM, HBM, HBM, HBM, HBM],
        out_specs=[VMEM] * 8,
        scratch_shapes=[
            pltpu.VMEM((neighbours, count), jnp.int32),
            pltpu.VMEM((2, tile_blocks.shape[0]), jnp.int32),
            pltpu.VMEM((halo // EDGE, EDGE), jnp.int32),
            pltpu.SemaphoreType.DMA((4,)),
        ],
        compiler_params=pltpu.CompilerParams(vmem_limit_bytes=16 * MIB),
        cost_estimate=pl.CostEstimate(
            flops=2 * halo * height * channels, bytes_accessed=2 * MIB, transcendentals=0),
    )(place, tile_count, in_hbm(send_rows[0]), in_hbm(tile_blocks.T), in_hbm(features),
      in_hbm(tile_values))
    got = chip_swaps(*sent)

    dense, _, recv_hot, built = pl.pallas_call(
        functools.partial(build_kernel, count, zeroed, loaded),
        out_shape=[
            dense_type,
            tiles_type,
            pltpu.VMEM((halo, halo), bf16),
            struct((halo // EDGE, EDGE), jnp.int32),
        ],
        in_specs=[SMEM, SMEM, SMEM, HBM, HBM, VMEM, VMEM],
        out_specs=[VMEM] * 4,
        input_output_aliases={5: 0, 6: 1},
        scratch_shapes=[
            pltpu.VMEM(recv_index.shape, jnp.int32),
            pltpu.SemaphoreType.DMA((2,)),
        ],
        compiler_params=pltpu.CompilerParams(vmem_limit_bytes=8 * MIB),
        cost_estimate=pl.CostEstimate(
            flops=4 * height * height * channels, bytes_accessed=24 * MIB, transcendentals=0),
    )(place, order, tile_count, in_hbm(recv_index), in_hbm(tile_values), on_chip(dense),
      on_chip(tiles))

    early = column_count // 4
    own, dense_a = pl.pallas_call(
        own_upper_kernel,
        out_shape=[
            pltpu.VMEM((height, channels), f32),
            pltpu.HBM((early, height, EDGE), bf16),
        ],
        in_specs=[VMEM] * 2,
        out_specs=[VMEM, HBM],
        scratch_shapes=[pltpu.SemaphoreType.DMA],
        compiler_params=pltpu.CompilerParams(vmem_limit_bytes=8 * MIB),
        cost_estimate=pl.CostEstimate(
            flops=height * height * channels, bytes_accessed=8 * MIB, transcendentals=0),
    )(on_chip(dense), on_chip(rows))

    relay_call = pl.pallas_call(
        relay_kernel,
        out_shape=payload,
        in_specs=[VMEM, SMEM] + [VMEM] * 3,
        out_specs=VMEM,
        compiler_params=pltpu.CompilerParams(vmem_limit_bytes=4 * MIB),
    )
    relay = relay_call(own, place, near, *got)
    got_core = core_swap(relay)

    own = pl.pallas_call(
        own_lower_kernel,
        out_shape=pltpu.VMEM((height, channels), f32),
        in_specs=[VMEM] * 4,
        out_specs=VMEM,
        input_output_aliases={1: 0},
        compiler_params=pltpu.CompilerParams(vmem_limit_bytes=8 * MIB),
        cost_estimate=pl.CostEstimate(
            flops=height * height * channels, bytes_accessed=8 * MIB, transcendentals=0),
    )(relay, on_chip(own), on_chip(dense), on_chip(rows))

    z, stats, *sent, near, dense_b = pl.pallas_call(
        first_kernel,
        out_shape=[pltpu.VMEM(mixed.shape, bf16), pltpu.HBM(stats_type.shape, f32)]
        + [payload] * 2 + [piece, pltpu.HBM((column_count - early, height, EDGE), bf16)],
        in_specs=[SMEM] + [VMEM] * 8,
        out_specs=[VMEM, HBM] + [VMEM] * 3 + [HBM],
        scratch_shapes=[
            pltpu.VMEM((halo, channels), bf16),
            pltpu.VMEM((halo, channels), bf16),
            pltpu.VMEM((16, channels), f32),
            pltpu.VMEM(stats_type.shape, f32),
            pltpu.SemaphoreType.DMA((2,)),
        ],
        compiler_params=pltpu.CompilerParams(vmem_limit_bytes=12 * MIB),
        cost_estimate=pl.CostEstimate(
            flops=2 * height * halo * channels, bytes_accessed=16 * MIB, transcendentals=0),
    )(place, on_chip(recv_hot), got_core, *got, on_chip(dense), on_chip(own), layer_weight, on_chip(send_hot))
    got = chip_swaps(*sent)
    stats = from_peers(stats, PLANE)
    column_stats = struct((lax.axis_size(COLUMN), 2, channels), f32)
    total_call = pl.pallas_call(
        put_total,
        out_shape=pltpu.VMEM(column_stats.shape, f32),
        in_specs=[VMEM],
        out_specs=VMEM,
        compiler_params=pltpu.CompilerParams(vmem_limit_bytes=MIB),
    )
    stats = from_peers(total_call(stats), COLUMN)
    relay = relay_call(built, place, near, *got)
    got_core = core_swap(relay)

    chunk = 512
    z, stats = pl.pallas_call(
        functools.partial(second_kernel, total),
        out_shape=[pltpu.VMEM(mixed.shape, bf16), stats_type],
        in_specs=[SMEM] + [VMEM] * 8 + [HBM, HBM, VMEM],
        out_specs=[VMEM] * 2,
        scratch_shapes=[
            pltpu.VMEM((halo, channels), bf16),
            pltpu.VMEM((height + halo, channels), bf16),
            pltpu.VMEM((16, channels), f32),
            pltpu.VMEM((halo, halo), bf16),
            pltpu.VMEM((height // chunk, column_count, chunk, EDGE), bf16),
            pltpu.SemaphoreType.DMA((height // chunk, 2)),
        ],
        compiler_params=pltpu.CompilerParams(vmem_limit_bytes=28 * MIB),
        cost_estimate=pl.CostEstimate(
            flops=2 * height * (height + halo) * channels, bytes_accessed=16 * MIB,
            transcendentals=0),
    )(place, built, got_core, *got, on_chip(z), stats, norm_gain, norm_shift,
      in_hbm(dense_a), in_hbm(dense_b), layer_weight)
    stats = from_peers(stats, PLANE)
    stats = from_peers(total_call(stats), COLUMN)

    return pl.pallas_call(
        functools.partial(last_kernel, vertex_total),
        out_shape=mixed,
        in_specs=[VMEM] * 4,
        out_specs=HBM,
        scratch_shapes=[pltpu.VMEM(mixed.shape, bf16), pltpu.SemaphoreType.DMA((8,))],
        compiler_params=pltpu.CompilerParams(vmem_limit_bytes=16 * MIB),
    )(on_chip(z), stats, norm_gain, norm_shift)


def solution(mesh):
    finer = Mesh(mesh.devices.reshape(4, 4, 8, 2), PARTS)
    placed = (
        P(PARTS, None),
        P(PARTS, None, None),
        P(PARTS, None),
        P(PARTS),
        P(PARTS, None, None),
        P(PARTS, None),
        P(),
        P(),
        P(),
    )
    return jax.shard_map(
        shards, mesh=finer, in_specs=placed, out_specs=P(PARTS, None), check_vma=False
    )
```
